512 devices in a mesh: gx: 8 (over z), gy: 8 (over y), gz: 8 (over x, core).
Axes of the slice: x: 4, y: 8, z: 8, core: 2. Of those that a mesh axis runs over, the one named last changes fastest.
Arguments:
- right_side: float32 [512, 512, 512], P('gx', 'gy', 'gz'), may hold values from -6 to 6
- guess: float32 [512, 512, 512], P('gx', 'gy', 'gz'), may hold values from -6 to 6
Outputs:
- solution: float32 [512, 512, 512], P('gx', 'gy', 'gz')
- residual: float32 [512, 512, 512], P('gx', 'gy', 'gz')
The draws below stay inside these ranges and needn't reach their ends.
All inputs are finite; a program needn't handle non-finite values.
Results may differ from the reference program's by a relative error of at most 0.0003.
Values sent between devices are 32-bit elements.
A program may use at most 256 MiB of HBM per device.

```python
import jax
import jax.numpy as jnp
from jax import lax

LEVELS = 7
COARSE_SWEEPS = 4
NX = 512
NY = 512
NZ = 512


def level_of(stream_key, dims, split, low, largest):
    def one(axis_at, blocks):
        heights = jax.random.uniform(jax.random.fold_in(jax.random.fold_in(stream_key, 6), axis_at), (blocks,), jnp.float32, low / len(split), largest / len(split))
        return jnp.repeat(jnp.exp(heights), dims[axis_at] // blocks).reshape((-1,) + (1,) * (len(dims) - axis_at - 1))

    loudness = one(*split[0])
    for cut in split[1:]:
        loudness = loudness * one(*cut)
    return loudness


def bell_draw(key, shape, deviation, most, cuts=(), held_as=jnp.bfloat16):
    array = deviation * jax.random.normal(key, shape, jnp.float32)
    if cuts:
        array = array * level_of(key, shape, cuts, -0.22, 0.18)
    return jnp.clip(array, -most, most).astype(held_as)


def setup_inputs(seed: int = 0) -> dict:
    streams_of = jax.random.split(jax.random.key(seed), 3)
    right_side = bell_draw(streams_of[0], (NX, NY, NZ), 1.0, 6.0, ((0, 8), (1, 8), (2, 8)), jnp.float32)
    guess = bell_draw(streams_of[1], (NX, NY, NZ), 1.0, 6.0, ((0, 8), (1, 8), (2, 8)), jnp.float32)
    return dict(right_side=right_side, guess=guess)


def face_total(padded):
    total = padded[2:, 1:-1, 1:-1] + padded[:-2, 1:-1, 1:-1]
    total = total + padded[1:-1, 2:, 1:-1] + padded[1:-1, :-2, 1:-1]
    total = total + padded[1:-1, 1:-1, 2:] + padded[1:-1, 1:-1, :-2]
    return total


def neighbours(field):
    return face_total(jnp.pad(field, 1))


def walls(index, total):
    return (index == 0).astype(jnp.float32) + (index == total - 1).astype(jnp.float32)


def geometry(shape):
    first = lax.iota(jnp.int32, shape[0])[:, None, None]
    second = lax.iota(jnp.int32, shape[1])[None, :, None]
    third = lax.iota(jnp.int32, shape[2])[None, None, :]
    parity = (first + second + third) % 2
    diagonal = 6.0 + walls(first, shape[0]) + walls(second, shape[1]) + walls(third, shape[2])
    return parity == 0, parity == 1, diagonal


def half_sweep(field, source, colour, diagonal, scale):
    updated = (scale * source + neighbours(field)) / diagonal
    return jnp.where(colour, updated, field)


def residual_of(field, source, diagonal, inverse):
    return source - (diagonal * field - neighbours(field)) * inverse


def restrict(remainder):
    shape = remainder.shape
    grouped = remainder.reshape(shape[0] // 2, 2, shape[1] // 2, 2, shape[2] // 2, 2)
    return jnp.sum(grouped, axis=(1, 3, 5)) * 0.125


def odd_pad(field):
    for axis in range(3):
        count = field.shape[axis]
        lowest = -lax.slice_in_dim(field, 0, 1, axis=axis)
        highest = -lax.slice_in_dim(field, count - 1, count, axis=axis)
        field = jnp.concatenate([lowest, field, highest], axis=axis)
    return field


def prolong(padded):
    centre = padded[1:-1, 1:-1, 1:-1]
    below_first = 0.25 * (padded[:-2, 1:-1, 1:-1] - centre)
    above_first = 0.25 * (padded[2:, 1:-1, 1:-1] - centre)
    below_second = 0.25 * (padded[1:-1, :-2, 1:-1] - centre)
    above_second = 0.25 * (padded[1:-1, 2:, 1:-1] - centre)
    below_third = 0.25 * (padded[1:-1, 1:-1, :-2] - centre)
    above_third = 0.25 * (padded[1:-1, 1:-1, 2:] - centre)
    along_first = jnp.stack([below_first, above_first], axis=1)[:, :, :, None, :, None]
    along_second = jnp.stack([below_second, above_second], axis=2)[:, None, :, :, :, None]
    along_third = jnp.stack([below_third, above_third], axis=3)[:, None, :, None, :, :]
    fine = centre[:, None, :, None, :, None] + along_first + along_second + along_third
    shape = centre.shape
    return fine.reshape(2 * shape[0], 2 * shape[1], 2 * shape[2])


def cycle(field, source, level):
    red, black, diagonal = geometry(source.shape)
    scale = 4.0 ** level
    if level == LEVELS - 1:
        for sweep_index in range(COARSE_SWEEPS):
            field = half_sweep(field, source, red, diagonal, scale)
            field = half_sweep(field, source, black, diagonal, scale)
        return field
    field = half_sweep(field, source, red, diagonal, scale)
    field = half_sweep(field, source, black, diagonal, scale)
    coarse = restrict(residual_of(field, source, diagonal, 0.25 ** level))
    correction = cycle(jnp.zeros_like(coarse), coarse, level + 1)
    field = field + prolong(odd_pad(correction))
    field = half_sweep(field, source, red, diagonal, scale)
    return half_sweep(field, source, black, diagonal, scale)


def reference(right_side, guess):
    solution = cycle(guess, right_side, 0)
    red, black, diagonal = geometry(right_side.shape)
    return solution, residual_of(solution, right_side, diagonal, 1.0)
```

```python
import itertools

import jax
import jax.numpy as jnp
from jax import lax
from jax.experimental import pallas as pl
from jax.experimental.pallas import tpu as pltpu
from jax.sharding import PartitionSpec as P

COARSE_SWEEPS = 4
MESH = pl.DeviceIdType.MESH
SIDE = 8
F32 = jnp.float32


class Level:
    def __init__(self, n, total, po, oy, p0, np_, r0, nr, pairs, rows, whole_z):
        self.n, self.total, self.po, self.oy = n, total, po, oy
        self.p0, self.np, self.r0, self.nr = p0, np_, r0, nr
        self.pairs, self.rows, self.whole_z = pairs, rows, whole_z

    def shape(self):
        return (self.pairs, self.rows, 128)


LEV = [
    Level(64, 512, 3, 8, 1, 36, 4, 72, 38, 80, False),
    Level(32, 256, 5, 16, 1, 24, 8, 48, 26, 64, False),
    Level(16, 128, 5, 16, 1, 16, 8, 32, 18, 48, False),
    Level(8, 64, 5, 16, 1, 12, 8, 24, 14, 40, True),
    Level(32, 32, 4, 8, 4, 16, 8, 32, 24, 48, True),
    Level(16, 16, 1, 8, 1, 8, 8, 16, 10, 32, True),
    Level(8, 8, 1, 8, 1, 4, 8, 8, 6, 24, True),
]
GIVE = {0: (3, 20, 12, 40), 1: (2, 14, 12, 24), 2: (2, 10, 12, 16), 3: (0, 8, 0, 12), 4: (0, 10, 8, 16), 5: (0, 6, 8, 8)}
WIDTH = {1: 6, 2: 7}


def iota(shape, axis):
    return lax.broadcasted_iota(jnp.int32, shape, axis)


def odd(rows):
    return ((iota((rows, 128), 0) + iota((rows, 128), 1)) & 1) == 1


def lanes(rows):
    return iota((rows, 128), 1)


def sweep_loop(start, count, step, body):
    step = max(k for k in range(1, step + 1) if count % k == 0)
    if count == step:
        for i in range(count):
            body(start + i)
        return

    def some(j, carry):
        for i in range(step):
            body(start + j * step + i)
        return carry

    lax.fori_loop(0, count // step, some, 0)


def around(src, p, r0, nr, up):
    here = src[p, pl.ds(r0, nr), :]
    side = jnp.where(up, src[p + 1, pl.ds(r0, nr), :], src[p - 1, pl.ds(r0, nr), :])
    rows = src[p, pl.ds(r0 - 1, nr), :] + src[p, pl.ds(r0 + 1, nr), :]
    return (here + side) + rows + (pltpu.roll(here, 1, axis=1) + pltpu.roll(here, 127, axis=1))


def kernel(*refs):
    it = iter(refs)
    f_hbm, u_hbm, out_u, out_r = (next(it) for _ in range(4))
    f_in, u_in = next(it), next(it)
    R = [next(it) for _ in range(7)]
    B = [next(it) for _ in range(7)]
    FR = [next(it) for _ in range(7)]
    FB = [next(it) for _ in range(7)]
    C = [next(it) for _ in range(7)]
    D = [next(it) for _ in range(7)]
    A = [next(it) for _ in range(6)]
    Q = [next(it) for _ in range(6)]
    EX = [next(it) for _ in range(6)]
    EZ = [next(it) for _ in range(6)]
    T, H = next(it), next(it)
    G = {1: next(it), 2: next(it)}
    N = {5: next(it), 6: next(it)}
    zs = {k: (next(it), next(it)) for k in ("f", "v", 1, 2)}
    zr = {k: (next(it), next(it)) for k in ("f", "v", 1, 2)}
    pack3, Z3, pack4, G4, A4 = (next(it) for _ in range(5))
    sems = {k: (next(it), next(it)) for k in ("f", "v", 1, 2, "3", "4")}
    in_sem, out_sem = next(it), next(it)

    gx, gy, gz = lax.axis_index("gx"), lax.axis_index("gy"), lax.axis_index("gz")
    me = (gx, gy, gz)

    copies_in = []
    for i, (src, dst) in enumerate(((u_hbm, u_in), (f_hbm, f_in))):
        copy = pltpu.make_async_copy(src, dst, in_sem.at[i])
        copy.start()
        copies_in.append(copy)

    barrier = pltpu.get_barrier_semaphore()
    count = jnp.int32(0)
    for dx, dy in itertools.product((-1, 0, 1), repeat=2):
        there = inside((dx, dy, 0), me)

        def column(k, carry, dx=dx, dy=dy):
            @pl.when(k != gz)
            def _():
                pl.semaphore_signal(barrier, inc=1, device_id=(gx + dx, gy + dy, k), device_id_type=MESH)

            return carry

        @pl.when(there)
        def _():
            lax.fori_loop(0, SIDE, column, 0)

        count = count + jnp.where(there, SIDE - 1, 0)

    def plane(k, carry):
        x, y = k // SIDE, k % SIDE

        @pl.when((x != gx) | (y != gy))
        def _():
            pl.semaphore_signal(barrier, inc=1, device_id=(x, y, gz), device_id_type=MESH)

        return carry

    lax.fori_loop(0, SIDE * SIDE, plane, 0)
    pl.semaphore_wait(barrier, count + SIDE * SIDE - 1)

    lv = LEV[0]
    m64 = ((iota((64, 64), 0) + iota((64, 64), 1)) & 1) == 1
    for copy in copies_in:
        copy.wait()

    def apart(p):
        a, b = u_in[2 * (p - lv.po)], u_in[2 * (p - lv.po) + 1]
        B[0][p, 8:72, 0:64] = jnp.where(m64, a, b)
        a, b = f_in[2 * (p - lv.po)], f_in[2 * (p - lv.po) + 1]
        FR[0][p, 8:72, 0:64] = jnp.where(m64, b, a)
        FB[0][p, 8:72, 0:64] = jnp.where(m64, a, b)

    sweep_loop(3, 32, 8, apart)

    lane64 = lanes(64)

    def pack_first(get, keys, slots, low, high, width):
        for g in range(slots // 16):
            lo = hi = None
            for j in range(16):
                t = get(16 * g + j)
                t = pltpu.roll(t, 8 * j, axis=1) if j else t
                rows = t.shape[0]
                lane = lanes(rows)
                if lo is None:
                    lo, hi = t, t
                else:
                    lo = jnp.where(((lane - 8 * j) & 127) < width, t, lo)
                    hi = jnp.where(((lane - high - 8 * j) & 127) < width, t, hi)
            keys[0][g] = lo
            keys[1][g] = hi

    def face_first(i):
        b = B[0][3 + i, 8:72, :]
        r = pltpu.roll(FR[0][3 + i, 8:72, :], 3, axis=1)
        k = pltpu.roll(FB[0][3 + i, 8:72, :], 5, axis=1)
        t = jnp.where((lane64 == 5) | (lane64 == 68), k, b)
        return jnp.where((lane64 == 3) | (lane64 == 4) | (lane64 == 65) | (lane64 == 66), r, t)

    pack_first(face_first, zs["f"], 32, 0, 61, 8)

    def exchange(key, arrays, po, own, oy, n, hz):
        send, recv = sems[key]
        groups = zs[key][0].shape[0]
        waits = []
        at = 0
        for d in sorted(itertools.product((-1, 0, 1), repeat=3), key=lambda d: -sum(map(abs, d))):
            if d == (0, 0, 0):
                continue
            dx, dy, dz = d
            device = (gx + dx, gy + dy, gz + dz)
            pieces = []
            if dz == 0:
                for src_ref, dst_ref, hp, hr in arrays:
                    ps, pd, pw = {-1: (po, po + own, hp), 0: (po, po, own), 1: (po + own - hp, po - hp, hp)}[dx]
                    rs, rd, rw = {-1: (oy, oy + n, hr), 0: (oy, oy, n), 1: (oy + n - hr, oy - hr, hr)}[dy]
                    pieces.append((src_ref.at[pl.ds(ps, pw), pl.ds(rs, rw), :], dst_ref.at[pl.ds(pd, pw), pl.ds(rd, rw), :]))
            else:
                hr = hz
                qs, qd, qw = {-1: (0, groups + 1, 1), 0: (0, 1, groups), 1: (groups - 1, 0, 1)}[dx]
                rs, rd, rw = {-1: (0, oy + n, hr), 0: (0, oy, n), 1: (n - hr, oy - hr, hr)}[dy]
                src_ref, dst_ref = (zs[key][0], zr[key][1]) if dz < 0 else (zs[key][1], zr[key][0])
                pieces.append((src_ref.at[pl.ds(qs, qw), pl.ds(rs, rw), :], dst_ref.at[pl.ds(qd, qw), pl.ds(rd, rw), :]))
            copies = []
            for src, dst in pieces:
                copies.append(pltpu.make_async_remote_copy(src, dst, send.at[at], recv.at[at], device_id=device, device_id_type=MESH))
                at += 1
            to, source = inside(d, me), inside((-dx, -dy, -dz), me)

            @pl.when(to)
            def _(copies=copies):
                for copy in copies:
                    copy.start()

            waits.append((to, source, copies))
        return waits

    def wait_recv(waits):
        for _, source, copies in waits:

            @pl.when(source)
            def _(copies=copies):
                for copy in copies:
                    copy.wait_recv()

    def wait_send(waits):
        for to, _, copies in waits:

            @pl.when(to)
            def _(copies=copies):
                for copy in copies:
                    copy.wait_send()

    first = exchange("f", ((B[0], B[0], 2, 3), (FR[0], FR[0], 1, 2), (FB[0], FB[0], 1, 1)), 3, 32, 8, 64, 3)

    def outside(ref, po, own, hp, oy, n, hr):
        planes, rows = ref.shape[0], ref.shape[1]
        for cond, cut in (
            (gx == 0, (slice(po - hp, po), slice(0, rows))),
            (gx == SIDE - 1, (slice(po + own, po + own + hp), slice(0, rows))),
            (gy == 0, (slice(0, planes), slice(oy - hr, oy))),
            (gy == SIDE - 1, (slice(0, planes), slice(oy + n, oy + n + hr))),
        ):

            @pl.when(cond)
            def _(cut=cut):
                shape = (cut[1].stop - cut[1].start, 128)
                for p in range(cut[0].start, cut[0].stop):
                    ref[p, cut[1], :] = jnp.zeros(shape, F32)

    def outside_z(key):
        for side, cond in ((0, gz == 0), (1, gz == SIDE - 1)):

            @pl.when(cond)
            def _(side=side):
                ref = zr[key][side]
                ref[...] = jnp.zeros(ref.shape, F32)

    def edges_z(key, po, n, hz, oy, groups):
        for side in (0, 1):
            ref = zr[key][side]
            rows = ref.shape[1]
            for cond, cut in (
                (gx == 0, (0, 1, 0, rows)),
                (gx == SIDE - 1, (groups + 1, 1, 0, rows)),
                (gy == 0, (0, groups + 2, oy - hz, hz)),
                (gy == SIDE - 1, (0, groups + 2, oy + n, hz)),
            ):

                @pl.when(cond)
                def _(cut=cut, ref=ref):
                    ref[pl.ds(cut[0], cut[1]), pl.ds(cut[2], cut[3]), :] = jnp.zeros((cut[1], cut[3], 128), F32)

    for ref, hp, hr in ((B[0], 2, 3), (FR[0], 1, 2), (FB[0], 1, 1), (H, 2, 3)):
        outside(ref, 3, 32, hp, 8, 64, hr)
    for key, n, oy, groups, hz in (("f", 64, 8, 2, 3), ("v", 64, 8, 2, 3), (1, 32, 16, 2, 6), (2, 16, 16, 1, 7)):
        outside_z(key)
        edges_z(key, 3, n, hz, oy, groups)
    outside(G[1], 8, 32, 8, 16, 32, 8)
    outside(G[2], 8, 16, 8, 16, 16, 8)
    for dx, dy in itertools.product((-1, 0, 1), repeat=2):
        if (dx, dy) != (0, 0):

            @pl.when(jnp.logical_not(inside((dx, dy, 0), me)))
            def _(dx=dx, dy=dy):
                Z3[dx + 1, dy + 1] = jnp.zeros((SIDE, 8, 128), F32)

    for l in (4, 5, 6):
        R[l][...] = jnp.zeros(LEV[l].shape(), F32)
        B[l][...] = jnp.zeros(LEV[l].shape(), F32)
    for l in (4, 5):
        EX[l][...] = jnp.zeros(EX[l].shape, F32)

    def tables(l):
        lv = LEV[l]
        shape = (lv.nr, 128)
        row, lane = iota(shape, 0) + lv.r0, iota(shape, 1)
        y = row - lv.oy
        z = jnp.where(lane < 100, lane, lane - 128)
        if l < 4:
            y = y + gy * lv.n
        if l < 3:
            z = z + gz * lv.n
        last = lv.total - 1
        within = (y >= 0) & (y <= last) & (z >= 0) & (z <= last)
        one = lambda c: jnp.where(c, 1, 0)
        w = one(y == 0) + one(y == last) + one(z == 0) + one(z == last)
        high = one(odd(lv.nr))
        for kind, colour in itertools.product(range(3), range(2)):
            a = high if colour == 0 else 1 - high
            d = w if kind == 0 else (w + 1 - a if kind == 1 else w + a)
            inv = jnp.where(d == 0, 1 / 6, jnp.where(d == 1, 1 / 7, jnp.where(d == 2, 1 / 8, 1 / 9)))
            C[l][kind, colour] = jnp.where(within, inv, 0.0)
            D[l][kind, colour] = 6.0 + d.astype(F32)
            if colour == 1 and l < 6:
                q = jnp.where(within, 0.25, 0.0)
                Q[l][kind] = q
                A[l][kind] = (1.0 - d.astype(F32)) * q
        for colour in range(2):
            C[l][3, colour] = jnp.zeros(shape, F32)
            D[l][3, colour] = jnp.full(shape, 6.0, F32)
        if l < 6:
            Q[l][3] = jnp.zeros(shape, F32)
            A[l][3] = jnp.zeros(shape, F32)

    for l in range(7):
        tables(l)

    def kind(l, p):
        lv = LEV[l]
        x = 2 * (p - lv.po) + (gx * lv.n if l < 4 else 0)
        if l >= 4:
            return jnp.where(x == 0, 1, jnp.where(x == lv.total - 2, 2, 0))
        return jnp.where(x == 0, 1, jnp.where(x == lv.total - 2, 2, jnp.where((x < 0) | (x >= lv.total), 3, 0)))

    wait_recv(first)
    wait_send(first)
    lane72 = lanes(72)

    def slot_of(i, n):
        groups = n // 16
        if i < 0:
            return 0, 16 + i
        if i >= n:
            return groups + 1, i - n
        return 1 + i // 16, i % 16

    def unpack_first(i, first_half):
        g, j = slot_of(i, 32)
        p = 3 + i
        low, high = zr["f"][0][g, 4:76, :], zr["f"][1][g, 4:76, :]
        for ref, at, width, shift in ((B[0], 0, 3, 64), (FR[0], 3, 2, 61), (FB[0], 5, 1, 59)):
            w = jnp.where(((lane72 - 8 * j - at) & 127) < width, high, low)
            w = pltpu.roll(w, (shift - 8 * j) % 128, axis=1)
            ref[p, 4:76, :] = jnp.where(lane72 < 64, ref[p, 4:76, :], w)

    for i in range(-2, 34):
        unpack_first(i, None)

    def red_sweep(l):
        lv = LEV[l]
        m = odd(lv.nr)

        def body(p):
            s = around(B[l], p, lv.r0, lv.nr, m)
            R[l][p, pl.ds(lv.r0, lv.nr), :] = (FR[l][p, pl.ds(lv.r0, lv.nr), :] + s) * C[l][kind(l, p), 0]

        sweep_loop(lv.p0, lv.np, 12, body)

    def black_sweep(l, keep):
        lv = LEV[l]
        m = jnp.logical_not(odd(lv.nr))

        def body(p):
            t = kind(l, p)
            rows = pl.ds(lv.r0, lv.nr)
            fs = FB[l][p, rows, :] + around(R[l], p, lv.r0, lv.nr, m)
            b = fs * C[l][t, 1]
            B[l][p, rows, :] = b
            if keep:
                T[p, rows, :] = fs - D[l][t, 1] * b

        sweep_loop(lv.p0, lv.np, 12, body)

    def red_residual(l, p):
        lv = LEV[l]
        s = around(B[l], p, lv.oy, lv.n, odd(lv.n))
        at = lv.oy - lv.r0
        return FR[l][p, pl.ds(lv.oy, lv.n), :] + s - D[l][kind(l, p), 0, pl.ds(at, lv.n), :] * R[l][p, pl.ds(lv.oy, lv.n), :]

    def coarse_side(l, p):
        lv = LEV[l]
        T[p, pl.ds(lv.oy, lv.n), :] = T[p, pl.ds(lv.oy, lv.n), :] + red_residual(l, p)
        half = lv.n // 2
        u = T[p, pl.ds(lv.oy, half, stride=2), :] + T[p, pl.ds(lv.oy + 1, half, stride=2), :]
        u = u + pltpu.roll(u, 127, axis=1)
        return 0.5 * jnp.take_along_axis(u, (2 * lanes(half)) & 127, axis=1, mode="promise_in_bounds")

    red_sweep(0)
    black_sweep(0, True)

    def keep_black(p):
        H[p, 8:72, :] = B[0][p, 8:72, :]

    sweep_loop(3, 32, 8, keep_black)

    def restrict_to(l, dst, first_plane, first_row):
        lv = LEV[l]

        def body(p):
            dst[p - lv.po + first_plane, pl.ds(first_row, lv.n // 2), :] = coarse_side(l, p)

        sweep_loop(lv.po, lv.n // 2, 8, body)

    restrict_to(0, G[1], 8, 16)

    def send_right_side(l):
        n, w = LEV[l].n, WIDTH[l]
        pack_first(lambda i: G[l][8 + i, pl.ds(16, n), :], zs[l], n, 0, n - 8, 8)
        return exchange(l, ((G[l], G[l], w, w),), 8, n, 16, n, w)

    def split_right_side(l):
        lv = LEV[l]
        n = lv.n
        lane, m = lanes(lv.nr), odd(lv.nr)

        def natural(i):
            g, j = slot_of(i, n)
            rows = pl.ds(lv.r0, lv.nr)
            low = pltpu.roll(zr[l][0][g, rows, :], (128 - n - 8 * j) % 128, axis=1)
            high = pltpu.roll(zr[l][1][g, rows, :], (n - 8 * j) % 128, axis=1)
            return jnp.where(lane < n, G[l][8 + i, rows, :], jnp.where(lane < 100, high, low))

        for p in range(lv.p0, lv.p0 + lv.np):
            a, b = natural(2 * (p - lv.po)), natural(2 * (p - lv.po) + 1)
            store_colours(l, p, a, b, m)

    def store_colours(l, p, a, b, m):
        lv = LEV[l]
        rows = pl.ds(lv.r0, lv.nr)
        red = jnp.where(m, b, a)
        FR[l][p, rows, :] = red
        FB[l][p, rows, :] = jnp.where(m, a, b)
        R[l][p, rows, :] = red * C[l][kind(l, p), 0]

    second = send_right_side(1)
    pack_first(lambda i: B[0][3 + i, 8:72, :], zs["v"], 32, 0, 61, 3)
    kept = exchange("v", ((B[0], H, 2, 3),), 3, 32, 8, 64, 3)
    wait_recv(second)
    split_right_side(1)
    black_sweep(1, True)
    restrict_to(1, G[2], 8, 16)
    third = send_right_side(2)
    wait_recv(third)
    split_right_side(2)
    black_sweep(2, True)

    lane8 = lanes(8)
    own3 = None
    for i in range(8):
        g = coarse_side(2, LEV[2].po + i)
        slot = lax.rem(gz + i, 16)
        g = pltpu.roll(jnp.where(lane8 < 8, g, 0.0), 8 * slot, axis=1)
        own3 = g if own3 is None else own3 + g
    pack3[...] = own3
    Z3[1, 1, gz] = own3

    def to_columns(act):
        for dx, dy in itertools.product((-1, 0, 1), repeat=2):

            def column(k, carry, dx=dx, dy=dy):
                @pl.when(k != gz)
                def _():
                    act(dx, dy, k)

                if (dx, dy) != (0, 0):

                    @pl.when(k == gz)
                    def _():
                        act(dx, dy, k)

                return carry

            yield dx, dy, column

    def start3(dx, dy, k):
        copy3(dx, dy, k).start()

    def copy3(dx, dy, k):
        at = (dx + 1) * 24 + (dy + 1) * 8
        return pltpu.make_async_remote_copy(
            pack3, Z3.at[1 - dx, 1 - dy, gz], sems["3"][0].at[at + k], sems["3"][1].at[at + gz], device_id=(gx + dx, gy + dy, k), device_id_type=MESH
        )

    def arrive3(dx, dy, k):
        at = (dx + 1) * 24 + (dy + 1) * 8
        pltpu.make_async_remote_copy(
            pack3, Z3.at[1 - dx, 1 - dy, k], sems["3"][0].at[at + k], sems["3"][1].at[at + k], device_id=(gx - dx, gy - dy, k), device_id_type=MESH
        ).wait_recv()

    def left3(dx, dy, k):
        copy3(dx, dy, k).wait_send()

    def over_columns(act, sign):
        for dx, dy, column in to_columns(act):

            @pl.when(inside((sign * dx, sign * dy, 0), me))
            def _(column=column):
                lax.fori_loop(0, SIDE, column, 0)

    over_columns(start3, 1)
    over_columns(arrive3, -1)

    m3 = odd(24)
    for p in range(1, 13):
        ab = []
        for i in (2 * (p - 1), 2 * (p - 1) + 1):
            x = i % 8
            tiles = []
            for cy in range(3):
                t = jnp.zeros((8, 128), F32)
                for k in range(SIDE):
                    s = 8 * ((x + k) % 16)
                    t = jnp.where((lane8 >= s) & (lane8 < s + 8), Z3[i // 8, cy, k], t)
                tiles.append(pltpu.roll(t, (128 - 8 * x) % 128, axis=1) if x else t)
            ab.append(jnp.concatenate(tiles, axis=0))
        store_colours(3, p, ab[0], ab[1], m3)
    black_sweep(3, True)

    lane4 = lanes(4)
    own4 = None
    for i in range(4):
        g = jnp.where(lane4 < 32, coarse_side(3, LEV[3].po + i), 0.0)
        g = pltpu.roll(g, 32 * i, axis=1) if i else g
        own4 = g if own4 is None else own4 + g
    pack4[0:4, :] = own4
    pack4[4:8, :] = own4
    G4[gx, gy, 0:4, :] = own4

    def copy4(k):
        return pltpu.make_async_remote_copy(
            pack4, G4.at[gx, gy], sems["4"][0].at[k], sems["4"][1].at[gx * SIDE + gy], device_id=(k // SIDE, k % SIDE, gz), device_id_type=MESH
        )

    def over_plane(act):
        def body(k, carry):
            @pl.when(k != gx * SIDE + gy)
            def _():
                act(k)

            return carry

        lax.fori_loop(0, SIDE * SIDE, body, 0)

    over_plane(lambda k: copy4(k).start())
    over_plane(
        lambda k: pltpu.make_async_remote_copy(
            pack4, G4.at[k // SIDE, k % SIDE], sems["4"][0].at[k], sems["4"][1].at[k], device_id=(k // SIDE, k % SIDE, gz), device_id_type=MESH
        ).wait_recv()
    )
    for x, y in itertools.product(range(SIDE), repeat=2):
        A4[x, pl.ds(4 * y, 4), :] = G4[x, y, 0:4, :]
    m4 = odd(32)
    for x in range(SIDE):
        a = A4[x]
        parts = [a] + [pltpu.roll(a, 128 - 32 * i, axis=1) for i in (1, 2, 3)]
        store_colours(4, 4 + 2 * x, parts[0], parts[1], m4)
        store_colours(4, 5 + 2 * x, parts[2], parts[3], m4)
    for l in (4, 5):
        black_sweep(l, True)
        restrict_to(l, N[l + 1], 0, 0)
        lv = LEV[l + 1]
        m = odd(lv.nr)
        for p in range(lv.p0, lv.p0 + lv.np):
            store_colours(l + 1, p, N[l + 1][2 * (p - 1)], N[l + 1][2 * (p - 1) + 1], m)
    black_sweep(6, False)
    for _ in range(COARSE_SWEEPS - 1):
        red_sweep(6)
        black_sweep(6, False)

    def expand(l):
        lf, lc = LEV[l], LEV[l + 1]
        c0, cn, r0, rn = GIVE[l]
        fine0 = lf.oy + 2 * (r0 - lc.oy)
        if l == 3:
            c0, r0 = 2 * gx + 1, 4 * gy + 4
            fine0 = 8
        m = odd(rn)
        lane = lanes(rn)
        z = (jnp.where(lane < 100, lane, lane - 128) >> 1) + (8 * gz if l == 2 else 0)
        at, beside = z & 127, (z + 2 * (lane & 1) - 1) & 127

        def body(i):
            rows = pl.ds(r0, rn)
            r, b = R[l + 1][c0 + i, rows, :], B[l + 1][c0 + i, rows, :]
            for a, e in ((0, jnp.where(m, b, r)), (1, jnp.where(m, r, b))):
                here = jnp.take_along_axis(e, at, axis=1, mode="promise_in_bounds")
                there = jnp.take_along_axis(e, beside, axis=1, mode="promise_in_bounds")
                for k in (0, 1):
                    EX[l][2 * i + a, pl.ds(fine0 + k, rn, stride=2), :] = here
                    EZ[l][2 * i + a, pl.ds(fine0 + k, rn, stride=2), :] = there

        sweep_loop(0, cn, 4 if l == 0 else 16, body)

    def correct(l):
        lv = LEV[l]
        m = odd(lv.nr)
        second_row = (iota((lv.nr, 128), 0) & 1) == 1
        rows = pl.ds(lv.r0, lv.nr)

        def body(p):
            e = p - EDGE[l]
            t = kind(l, p)
            sides = jnp.where(m, EX[l][e - 1, rows, :], EX[l][e + 1, rows, :])
            sides = sides + jnp.where(second_row, EX[l][e, pl.ds(lv.r0 + 1, lv.nr), :], EX[l][e, pl.ds(lv.r0 - 1, lv.nr), :])
            add = EX[l][e, rows, :] * A[l][t] + (EZ[l][e, rows, :] + sides) * Q[l][t]
            return add, B[l]

        if l > 0:

            def plain(p):
                add, ref = body(p)
                ref[p, rows, :] = ref[p, rows, :] + add

            sweep_loop(lv.p0, lv.np, 12, plain)
        else:
            for i in range(-2, 34):
                g, j = slot_of(i, 32)
                p = 3 + i
                low, high = zr["v"][0][g, 4:76, :], zr["v"][1][g, 4:76, :]
                w = jnp.where(((lane72 - 8 * j) & 127) < 3, high, low)
                w = pltpu.roll(w, (64 - 8 * j) % 128, axis=1)
                add, ref = body(p)
                ref[p, rows, :] = jnp.where(lane72 < 64, H[p, rows, :], w) + add

    for l in (5, 4, 3, 2, 1, 0):
        expand(l)
        if l == 0:
            wait_recv(kept)
            wait_send(kept)
        correct(l)
        red_sweep(l)
        black_sweep(l, l == 0)

    lv = LEV[0]
    m = ((iota((64, 64), 0) + iota((64, 64), 1)) & 1) == 1

    def results(p):
        r, b = R[0][p, 8:72, 0:64], B[0][p, 8:72, 0:64]
        x = 2 * (p - lv.po)
        u_in[x] = jnp.where(m, b, r)
        u_in[x + 1] = jnp.where(m, r, b)
        r, b = red_residual(0, p)[:, 0:64], T[p, 8:72, 0:64]
        f_in[x] = jnp.where(m, b, r)
        f_in[x + 1] = jnp.where(m, r, b)

    copies_out = []
    for part in range(2):
        sweep_loop(3 + 16 * part, 16, 8, results)
        for i, (src, dst) in enumerate(((u_in, out_u), (f_in, out_r))):
            cut = pl.ds(32 * part, 32)
            copy = pltpu.make_async_copy(src.at[cut], dst.at[cut], out_sem.at[2 * part + i])
            copy.start()
            copies_out.append(copy)
    wait_send(second)
    wait_send(third)
    over_columns(left3, 1)
    over_plane(lambda k: copy4(k).wait_send())
    for copy in copies_out:
        copy.wait()


EDGE = {0: -1, 1: -1, 2: -1, 3: -1, 4: 2, 5: -1}


def inside(d, me):
    ok = None
    for step, at in zip(d, me):
        if step:
            here = (at > 0) if step < 0 else (at < SIDE - 1)
            ok = here if ok is None else ok & here
    return True if ok is None else ok


def vmem(*shape):
    return pltpu.VMEM(shape, F32)


def per_device(right_side, guess):
    whole = vmem(64, 64, 64)
    scratch = [whole, whole]
    for _ in range(4):
        scratch += [vmem(*lv.shape()) for lv in LEV]
    for _ in range(2):
        scratch += [vmem(4, 2, lv.nr, 128) for lv in LEV]
    for _ in range(2):
        scratch += [vmem(4, lv.nr, 128) for lv in LEV[:6]]
    for _ in range(2):
        scratch += [vmem(2 * GIVE[l][1], LEV[l].rows, 128) for l in range(6)]
    scratch += [vmem(*LEV[0].shape())] * 2
    scratch += [vmem(48, 64, 128), vmem(32, 48, 128)]
    scratch += [vmem(16, 16, 128), vmem(8, 8, 128)]
    packed = ((2, 64, 80), (2, 64, 80), (2, 32, 64), (1, 16, 48))
    for groups, n, _ in packed:
        scratch += [vmem(groups, n, 128)] * 2
    for groups, _, rows in packed:
        scratch += [vmem(groups + 2, rows, 128)] * 2
    scratch += [vmem(8, 128), vmem(3, 3, 8, 8, 128), vmem(8, 128), vmem(8, 8, 8, 128), vmem(8, 32, 128)]
    for copies in (42, 26, 26, 26, 72, 64):
        scratch += [pltpu.SemaphoreType.DMA((copies,))] * 2
    scratch += [pltpu.SemaphoreType.DMA((2,)), pltpu.SemaphoreType.DMA((4,))]
    block = jax.ShapeDtypeStruct(right_side.shape, F32)
    return pl.pallas_call(
        kernel,
        out_shape=(block, block),
        in_specs=[pl.BlockSpec(memory_space=pl.ANY)] * 2,
        out_specs=(pl.BlockSpec(memory_space=pl.ANY),) * 2,
        scratch_shapes=scratch,
        compiler_params=pltpu.CompilerParams(collective_id=0, has_side_effects=True, vmem_limit_bytes=60 * 2**20),
    )(right_side, guess)


def solution(mesh):
    spec = P("gx", "gy", "gz")
    return jax.shard_map(per_device, mesh=mesh, in_specs=(spec, spec), out_specs=(spec, spec), check_vma=False)
```

```python
import itertools

import jax
import jax.numpy as jnp
from jax import lax
from jax.experimental import pallas as pl
from jax.experimental.pallas import tpu as pltpu
from jax.sharding import PartitionSpec as P

COARSE_SWEEPS = 4
MESH = pl.DeviceIdType.MESH
SIDE = 8
F32 = jnp.float32


class Level:
    def __init__(self, n, total, po, oy, p0, np_, r0, nr, pairs, rows, whole_z):
        self.n, self.total, self.po, self.oy = n, total, po, oy
        self.p0, self.np, self.r0, self.nr = p0, np_, r0, nr
        self.pairs, self.rows, self.whole_z = pairs, rows, whole_z

    def shape(self):
        return (self.pairs, self.rows, 128)


LEV = [
    Level(64, 512, 3, 8, 1, 36, 4, 72, 38, 80, False),
    Level(32, 256, 5, 16, 1, 24, 8, 48, 26, 64, False),
    Level(16, 128, 5, 16, 1, 16, 8, 32, 18, 48, False),
    Level(8, 64, 5, 16, 1, 12, 8, 24, 14, 40, True),
    Level(32, 32, 4, 8, 4, 16, 8, 32, 24, 48, True),
    Level(16, 16, 1, 8, 1, 8, 8, 16, 10, 32, True),
    Level(8, 8, 1, 8, 1, 4, 8, 8, 6, 24, True),
]
GIVE = {0: (3, 20, 12, 40), 1: (2, 14, 12, 24), 2: (2, 10, 12, 16), 3: (0, 8, 0, 12), 4: (0, 10, 8, 16), 5: (0, 6, 8, 8)}
PHASES = ("f", "v", 1, 2, "3", "4")
WIDTH = {1: 6, 2: 7}


def iota(shape, axis):
    return lax.broadcasted_iota(jnp.int32, shape, axis)


def odd():
    return ((iota((8, 128), 0) + iota((8, 128), 1)) & 1) == 1


def lanes():
    return iota((8, 128), 1)


def pick(mask, a, b):
    shape = a.shape
    if shape[0] <= 8:
        return jnp.where(mask[: shape[0]], a, b)
    tiles = (shape[0] // 8, 8, 128)
    return jnp.where(mask[None], a.reshape(tiles), b.reshape(tiles)).reshape(shape)


def within(start, width):
    return ((lanes() - start) & 127) < width


def turn(a, shift):
    return pltpu.roll(a, shift % 128, axis=1) if shift % 128 else a


def take(a, index):
    return jnp.take_along_axis(a, index, axis=1, mode="promise_in_bounds")


def lane_index(rows):
    return iota((rows, 128), 1)


def sweep_loop(start, count, step, body):
    step = max(k for k in range(1, step + 1) if count % k == 0)
    if count == step:
        for i in range(count):
            body(start + i)
        return

    def some(j, carry):
        for i in range(step):
            body(start + j * step + i)
        return carry

    lax.fori_loop(0, count // step, some, 0)


def around(src, p, r0, nr, up):
    here = src[p, pl.ds(r0, nr), :]
    side = pick(up, src[p + 1, pl.ds(r0, nr), :], src[p - 1, pl.ds(r0, nr), :])
    rows = src[p, pl.ds(r0 - 1, nr), :] + src[p, pl.ds(r0 + 1, nr), :]
    return (here + side) + rows + (pltpu.roll(here, 1, axis=1) + pltpu.roll(here, 127, axis=1))


def kernel(*refs):
    it = iter(refs)
    f_hbm, u_hbm, u_out, r_out = (next(it) for _ in range(4))
    f_in, u_in = next(it), next(it)
    R = [next(it) for _ in range(7)]
    B = [next(it) for _ in range(7)]
    FR = [next(it) for _ in range(7)]
    FB = [next(it) for _ in range(7)]
    C = [next(it) for _ in range(7)]
    D = [next(it) for _ in range(7)]
    A = [next(it) for _ in range(6)]
    Q = [next(it) for _ in range(6)]
    EX = [next(it) for _ in range(6)]
    EZ = [next(it) for _ in range(6)]
    T, H = next(it), next(it)
    G = {1: next(it), 2: next(it)}
    PS = {1: next(it), 2: next(it)}
    PR = {1: next(it), 2: next(it)}
    N = {5: next(it), 6: next(it)}
    zs = {k: (next(it), next(it)) for k in ("f", "v", 1, 2)}
    zr = {k: (next(it), next(it)) for k in ("f", "v", 1, 2)}
    pack3, Z3, pack4, G4, tally = (next(it) for _ in range(5))
    send_sem, recv_sem, in_sem, token = (next(it) for _ in range(4))

    gx, gy, gz = lax.axis_index("gx"), lax.axis_index("gy"), lax.axis_index("gz")
    me = (gx, gy, gz)

    copies_in = []
    for i, (src, dst) in enumerate(((u_hbm, u_in), (f_hbm, f_in))):
        copy = pltpu.make_async_copy(src, dst, in_sem.at[i])
        copy.start()
        copies_in.append(copy)

    barrier = pltpu.get_barrier_semaphore()
    rooms = [jnp.where((at > 0) & (at < SIDE - 1), 3, 2) for at in me]
    for d in itertools.product((-1, 0, 1), repeat=3):
        if d != (0, 0, 0):

            @pl.when(inside(d, me))
            def _(d=d):
                pl.semaphore_signal(barrier, inc=1, device_id=tuple(at + step for at, step in zip(me, d)), device_id_type=MESH)

    pl.semaphore_wait(barrier, rooms[0] * rooms[1] * rooms[2] - 1)

    def tokens(k, far, act):
        count = jnp.int32(0)
        for d in itertools.product((-1, 0, 1), repeat=3):
            if d == (0, 0, 0) or (d[2] and (d[0] or d[1])):
                continue
            there = inside(d, me, far)
            count = count + jnp.where(there, 1, 0)
            if act:

                @pl.when(there)
                def _(d=d):
                    device = tuple(at + far * step for at, step in zip(me, d))
                    pl.semaphore_signal(token.at[k], inc=1, device_id=device, device_id_type=MESH)

        if not act:
            pl.semaphore_wait(token.at[k], count)

    lv = LEV[0]
    m64 = ((iota((64, 64), 0) + iota((64, 64), 1)) & 1) == 1
    for copy in copies_in:
        copy.wait()

    def apart(p):
        a, b = u_in[2 * (p - lv.po)], u_in[2 * (p - lv.po) + 1]
        B[0][p, 8:72, 0:64] = jnp.where(m64, a, b)
        a, b = f_in[2 * (p - lv.po)], f_in[2 * (p - lv.po) + 1]
        FR[0][p, 8:72, 0:64] = jnp.where(m64, b, a)
        FB[0][p, 8:72, 0:64] = jnp.where(m64, a, b)

    sweep_loop(3, 32, 8, apart)

    def pack_faces(get, out, count, low, high, width, apart):
        for g in range(count // 16):
            lo = hi = None
            for j in range(16):
                t = get(16 * g + j)
                a = turn(t, 8 * j)
                b = turn(t, 8 * j + apart) if apart else a
                if lo is None:
                    lo, hi = a, b
                else:
                    lo = pick(within(low + 8 * j, width), a, lo)
                    hi = pick(within(high + apart + 8 * j, width), b, hi)
            out[0][g] = lo
            out[1][g] = hi

    at_fb = within(5, 1) | within(68, 1)
    at_fr = within(3, 2) | within(65, 2)

    def face_first(i):
        t = pick(at_fb, turn(FB[0][3 + i, 8:72, :], 5), B[0][3 + i, 8:72, :])
        return pick(at_fr, turn(FR[0][3 + i, 8:72, :], 3), t)

    pack_faces(face_first, zs["f"], 32, 0, 61, 8, 0)

    at_edge = [(at == 0) | (at == SIDE - 1) for at in me]

    def exchange(key, arrays, oy, n, hz):
        k = PHASES.index(key)
        groups = zs[key][0].shape[0]
        total = dict.fromkeys(itertools.product((False, True), repeat=3), 0)
        for d in sorted(itertools.product((-1, 0, 1), repeat=3), key=lambda d: -sum(map(abs, d))):
            if d == (0, 0, 0):
                continue
            dx, dy, dz = d
            pieces = []
            if dz == 0:
                for src, ps, dst, pd, own, hp, hr in arrays:
                    s0, d0, w = {-1: (ps, pd + own, hp), 0: (ps, pd, own), 1: (ps + own - hp, pd - hp, hp)}[dx]
                    rs, rd, rw = {-1: (0, oy + n, hr), 0: (0, oy, n), 1: (n - hr, oy - hr, hr)}[dy]
                    rs = rs + (oy if src.shape[1] > n else 0)
                    pieces.append((src.at[pl.ds(s0, w), pl.ds(rs, rw), :], dst.at[pl.ds(d0, w), pl.ds(rd, rw), :], w * rw))
            else:
                s0, d0, w = {-1: (0, groups + 1, 1), 0: (0, 1, groups), 1: (groups - 1, 0, 1)}[dx]
                rs, rd, rw = {-1: (0, oy + n, hz), 0: (0, oy, n), 1: (n - hz, oy - hz, hz)}[dy]
                src, dst = (zs[key][0], zr[key][1]) if dz < 0 else (zs[key][1], zr[key][0])
                pieces.append((src.at[pl.ds(s0, w), pl.ds(rs, rw), :], dst.at[pl.ds(d0, w), pl.ds(rd, rw), :], w * rw))

            @pl.when(inside(d, me))
            def _(d=d, pieces=pieces):
                device = tuple(at + step for at, step in zip(me, d))
                for src, dst, _ in pieces:
                    pltpu.make_async_remote_copy(
                        src, dst, send_sem.at[k], recv_sem.at[k], device_id=device, device_id_type=MESH
                    ).start()

            for edge in total:
                if not any(e and step > 0 for e, step in zip(edge, d)):
                    total[edge] += sum(rows for _, _, rows in pieces)
        return k, total

    def settle(what, arrived, left):
        k, total = what
        other = tuple(jnp.where(at == 0, at + 1, at - 1) for at in me)
        for edge, rows in total.items():
            same = None
            for e, here in zip(edge, at_edge):
                t = here if e else jnp.logical_not(here)
                same = t if same is None else same & t

            @pl.when(same)
            def _(rows=rows):
                cut = tally.at[pl.ds(0, rows), :]
                copy = pltpu.make_async_remote_copy(cut, cut, send_sem.at[k], recv_sem.at[k], device_id=other, device_id_type=MESH)
                if arrived:
                    copy.wait_recv()
                if left:
                    copy.wait_send()

    first = exchange("f", [(ref, 3, ref, 3, 32, hp, hr) for ref, hp, hr in ((B[0], 2, 3), (FR[0], 1, 2), (FB[0], 1, 1))], 8, 64, 3)

    def outside(ref, po, own, hp, oy, n, hr):
        planes, rows = ref.shape[0], ref.shape[1]
        for cond, cut in (
            (gx == 0, (slice(po - hp, po), slice(0, rows))),
            (gx == SIDE - 1, (slice(po + own, po + own + hp), slice(0, rows))),
            (gy == 0, (slice(0, planes), slice(oy - hr, oy))),
            (gy == SIDE - 1, (slice(0, planes), slice(oy + n, oy + n + hr))),
        ):

            @pl.when(cond)
            def _(cut=cut):
                shape = (cut[1].stop - cut[1].start, 128)
                for p in range(cut[0].start, cut[0].stop):
                    ref[p, cut[1], :] = jnp.zeros(shape, F32)

    def outside_z(key):
        for side, cond in ((0, gz == 0), (1, gz == SIDE - 1)):

            @pl.when(cond)
            def _(side=side):
                ref = zr[key][side]
                ref[...] = jnp.zeros(ref.shape, F32)

    def edges_z(key, po, n, hz, oy, groups):
        for side in (0, 1):
            ref = zr[key][side]
            rows = ref.shape[1]
            for cond, cut in (
                (gx == 0, (0, 1, 0, rows)),
                (gx == SIDE - 1, (groups + 1, 1, 0, rows)),
                (gy == 0, (0, groups + 2, oy - hz, hz)),
                (gy == SIDE - 1, (0, groups + 2, oy + n, hz)),
            ):

                @pl.when(cond)
                def _(cut=cut, ref=ref):
                    ref[pl.ds(cut[0], cut[1]), pl.ds(cut[2], cut[3]), :] = jnp.zeros((cut[1], cut[3], 128), F32)

    for ref, hp, hr in ((B[0], 2, 3), (FR[0], 1, 2), (FB[0], 1, 1), (H, 2, 3)):
        outside(ref, 3, 32, hp, 8, 64, hr)
    for key, n, oy, groups, hz in (("f", 64, 8, 2, 3), ("v", 64, 8, 2, 3), (1, 32, 16, 2, 6), (2, 16, 16, 1, 7)):
        outside_z(key)
        edges_z(key, 3, n, hz, oy, groups)
    outside(PR[1], 2, 8, 2, 16, 32, 8)
    outside(PR[2], 1, 2, 1, 16, 16, 8)
    for dx, dy in itertools.product((-1, 0, 1), repeat=2):
        if (dx, dy) != (0, 0):

            @pl.when(jnp.logical_not(inside((dx, dy, 0), me)))
            def _(dx=dx, dy=dy):
                Z3[dx + 1, dy + 1] = jnp.zeros((SIDE, 8, 128), F32)

    for l in (4, 5, 6):
        R[l][...] = jnp.zeros(LEV[l].shape(), F32)
        B[l][...] = jnp.zeros(LEV[l].shape(), F32)
    for l in (4, 5):
        EX[l][...] = jnp.zeros(EX[l].shape, F32)

    def tables(l):
        lv = LEV[l]
        shape = (lv.nr, 128)
        row, lane = iota(shape, 0) + lv.r0, iota(shape, 1)
        y = row - lv.oy
        z = jnp.where(lane < 100, lane, lane - 128)
        if l < 4:
            y = y + gy * lv.n
        if l < 3:
            z = z + gz * lv.n
        last = lv.total - 1
        within = (y >= 0) & (y <= last) & (z >= 0) & (z <= last)
        one = lambda c: jnp.where(c, 1, 0)
        w = one(y == 0) + one(y == last) + one(z == 0) + one(z == last)
        high = one(((row + lane) & 1) == 1)
        for kind, colour in itertools.product(range(3), range(2)):
            a = high if colour == 0 else 1 - high
            d = w if kind == 0 else (w + 1 - a if kind == 1 else w + a)
            inv = jnp.where(d == 0, 1 / 6, jnp.where(d == 1, 1 / 7, jnp.where(d == 2, 1 / 8, 1 / 9)))
            C[l][kind, colour] = jnp.where(within, inv, 0.0)
            D[l][kind, colour] = 6.0 + d.astype(F32)
            if colour == 1 and l < 6:
                q = jnp.where(within, 0.25, 0.0)
                Q[l][kind] = q
                A[l][kind] = (1.0 - d.astype(F32)) * q
        for colour in range(2):
            C[l][3, colour] = jnp.zeros(shape, F32)
            D[l][3, colour] = jnp.full(shape, 6.0, F32)
        if l < 6:
            Q[l][3] = jnp.zeros(shape, F32)
            A[l][3] = jnp.zeros(shape, F32)

    for l in range(7):
        tables(l)

    def kind(l, p):
        lv = LEV[l]
        x = 2 * (p - lv.po) + (gx * lv.n if l < 4 else 0)
        if l >= 4:
            return jnp.where(x == 0, 1, jnp.where(x == lv.total - 2, 2, 0))
        return jnp.where(x == 0, 1, jnp.where(x == lv.total - 2, 2, jnp.where((x < 0) | (x >= lv.total), 3, 0)))

    settle(first, True, True)
    tokens(0, 2, True)
    lane, m = lanes(), odd()
    not_m = jnp.logical_not(m)

    def slot_of(i, n):
        groups = n // 16
        if i < 0:
            return 0, 16 + i
        if i >= n:
            return groups + 1, i - n
        return 1 + i // 16, i % 16

    def unpack_first(i):
        g, j = slot_of(i, 32)
        low, high = zr["f"][0][g, 4:76, :], zr["f"][1][g, 4:76, :]
        for ref, at, width, shift in ((B[0], 0, 3, 64), (FR[0], 3, 2, 61), (FB[0], 5, 1, 59)):
            w = turn(pick(within(8 * j + at, width), high, low), shift - 8 * j)
            ref[3 + i, 4:76, :] = pick(lane < 64, ref[3 + i, 4:76, :], w)

    for i in range(-2, 34):
        unpack_first(i)

    def red_sweep(l):
        lv = LEV[l]

        def body(p):
            s = around(B[l], p, lv.r0, lv.nr, m)
            R[l][p, pl.ds(lv.r0, lv.nr), :] = (FR[l][p, pl.ds(lv.r0, lv.nr), :] + s) * C[l][kind(l, p), 0]

        sweep_loop(lv.p0, lv.np, 36, body)

    def black_sweep(l, keep):
        lv = LEV[l]

        def body(p):
            t = kind(l, p)
            rows = pl.ds(lv.r0, lv.nr)
            fs = FB[l][p, rows, :] + around(R[l], p, lv.r0, lv.nr, not_m)
            b = fs * C[l][t, 1]
            B[l][p, rows, :] = b
            if keep:
                T[p, rows, :] = fs - D[l][t, 1] * b

        sweep_loop(lv.p0, lv.np, 36, body)

    def red_residual(l, p):
        lv = LEV[l]
        s = around(B[l], p, lv.oy, lv.n, m)
        at = lv.oy - lv.r0
        return FR[l][p, pl.ds(lv.oy, lv.n), :] + s - D[l][kind(l, p), 0, pl.ds(at, lv.n), :] * R[l][p, pl.ds(lv.oy, lv.n), :]

    def residual(l):
        lv = LEV[l]

        def body(p):
            T[p, pl.ds(lv.oy, lv.n), :] = T[p, pl.ds(lv.oy, lv.n), :] + red_residual(l, p)

        sweep_loop(lv.po, lv.n // 2, 16, body)

    def coarse_side(l, p):
        lv = LEV[l]
        half = lv.n // 2
        u = T[p, pl.ds(lv.oy, half, stride=2), :] + T[p, pl.ds(lv.oy + 1, half, stride=2), :]
        z = 2 * lane_index(half)
        return 0.5 * (take(u, z & 127) + take(u, (z + 1) & 127))

    red_sweep(0)
    black_sweep(0, True)

    def keep_black(p):
        H[p, 8:72, :] = B[0][p, 8:72, :]

    sweep_loop(3, 32, 8, keep_black)

    def restrict_to(l, dst, first_plane, first_row):
        lv = LEV[l]

        def body(p):
            dst[p - lv.po + first_plane, pl.ds(first_row, lv.n // 2), :] = coarse_side(l, p)

        sweep_loop(lv.po, lv.n // 2, 16, body)

    residual(0)
    restrict_to(0, G[1], 0, 0)

    def send_right_side(l):
        n, w = LEV[l].n, WIDTH[l]
        per = 128 // n
        for q in range(n // per):
            t = G[l][per * q]
            for j in range(1, per):
                t = pick(within(n * j, n), turn(G[l][per * q + j], n * j), t)
            PS[l][q] = t
        pack_faces(lambda i: G[l][i], zs[l], n, 0, n - 8, 8, 128 - 2 * n)
        wide = 8 // per
        return exchange(l, [(PS[l], 0, PR[l], wide, n // per, wide, w)], 16, n, w)

    def split_right_side(l):
        lv = LEV[l]
        n = lv.n
        per = 128 // n

        def natural(i):
            g, j = slot_of(i, n)
            rows = pl.ds(lv.r0, lv.nr)
            side = pick(within(8 * j, 8), zr[l][1][g, rows, :], zr[l][0][g, rows, :])
            q, k = (i + 8) // per, (i + 8) % per
            if 0 <= i < n:
                below, above = (turn(PR[l][q, pl.ds(r, 8), :], -n * k) for r in (8, 16 + n))
                here = jnp.concatenate([below, G[l][i], above], axis=0)
            else:
                here = turn(PR[l][q, rows, :], -n * k)
            return pick(lane < n, here, turn(side, n - 8 * j))

        for p in range(lv.p0, lv.p0 + lv.np):
            a, b = natural(2 * (p - lv.po)), natural(2 * (p - lv.po) + 1)
            store_colours(l, p, a, b)

    def store_colours(l, p, a, b):
        lv = LEV[l]
        rows = pl.ds(lv.r0, lv.nr)
        red = pick(m, b, a)
        FR[l][p, rows, :] = red
        FB[l][p, rows, :] = pick(m, a, b)
        R[l][p, rows, :] = red * C[l][kind(l, p), 0]

    second = send_right_side(1)
    tokens(0, 2, False)
    tokens(1, 4, True)
    pack_faces(lambda i: B[0][3 + i, 8:72, :], zs["v"], 32, 0, 61, 3, 0)
    kept = exchange("v", [(B[0], 3, H, 3, 32, 2, 3)], 8, 64, 3)
    settle(second, True, False)
    split_right_side(1)
    black_sweep(1, True)
    residual(1)
    restrict_to(1, G[2], 0, 0)
    third = send_right_side(2)
    settle(third, True, False)
    split_right_side(2)
    black_sweep(2, True)
    residual(2)

    own3 = None
    for i in range(8):
        g = pick(lane < 8, coarse_side(2, LEV[2].po + i), jnp.zeros((8, 128), F32))
        g = pltpu.roll(g, 8 * lax.rem(gz + i, 16), axis=1)
        own3 = g if own3 is None else own3 + g
    pack3[...] = own3
    Z3[1, 1, gz] = own3
    tokens(1, 4, False)

    k3 = PHASES.index("3")
    for dx, dy in itertools.product((-1, 0, 1), repeat=2):

        def column(k, carry, dx=dx, dy=dy):
            @pl.when((k != gz) | ((dx, dy) != (0, 0)))
            def _():
                pltpu.make_async_remote_copy(
                    pack3, Z3.at[1 - dx, 1 - dy, gz], send_sem.at[k3], recv_sem.at[k3], device_id=(gx + dx, gy + dy, k), device_id_type=MESH
                ).start()

            return carry

        @pl.when(inside((dx, dy, 0), me))
        def _(column=column):
            lax.fori_loop(0, SIDE, column, 0)

    blocks = {edge: 8 * ((2 if edge[0] else 3) * (2 if edge[1] else 3) * SIDE - 1) for edge in itertools.product((False, True), repeat=3)}
    settle((k3, blocks), True, False)

    for p in range(1, 13):
        ab = []
        for i in (2 * (p - 1), 2 * (p - 1) + 1):
            x = i % 8
            tiles = []
            for cy in range(3):
                t = jnp.zeros((8, 128), F32)
                for k in range(SIDE):
                    t = jnp.where(within(8 * (x + k), 8), Z3[i // 8, cy, k], t)
                tiles.append(turn(t, -8 * x))
            ab.append(jnp.concatenate(tiles, axis=0))
        store_colours(3, p, ab[0], ab[1])
    black_sweep(3, True)

    residual(3)
    own4 = None
    for i in range(4):
        g = turn(pick(lane < 32, coarse_side(3, LEV[3].po + i), jnp.zeros((4, 128), F32)), 32 * i)
        own4 = g if own4 is None else own4 + g
    pack4[0:4, :] = own4
    G4[gx, pl.ds(4 * gy, 4), :] = own4

    k4 = PHASES.index("4")

    def column4(k, carry):
        x, y = k // SIDE, k % SIDE

        @pl.when((x != gx) | (y != gy))
        def _():
            pltpu.make_async_remote_copy(
                pack4.at[pl.ds(0, 4), :],
                G4.at[gx, pl.ds(4 * gy, 4), :],
                send_sem.at[k4],
                recv_sem.at[k4],
                device_id=(x, y, gz),
                device_id_type=MESH,
            ).start()

        return carry

    lax.fori_loop(0, SIDE * SIDE, column4, 0)
    plane = (k4, dict.fromkeys(itertools.product((False, True), repeat=3), 4 * (SIDE * SIDE - 1)))
    settle(plane, True, False)
    for x in range(SIDE):
        parts = [turn(G4[x], -32 * i) for i in range(4)]
        store_colours(4, 4 + 2 * x, parts[0], parts[1])
        store_colours(4, 5 + 2 * x, parts[2], parts[3])
    for l in (4, 5):
        black_sweep(l, True)
        residual(l)
        restrict_to(l, N[l + 1], 0, 0)
        lv = LEV[l + 1]
        for p in range(lv.p0, lv.p0 + lv.np):
            store_colours(l + 1, p, N[l + 1][2 * (p - 1)], N[l + 1][2 * (p - 1) + 1])
    black_sweep(6, False)
    for _ in range(COARSE_SWEEPS - 1):
        red_sweep(6)
        black_sweep(6, False)

    def expand(l):
        lf, lc = LEV[l], LEV[l + 1]
        c0, cn, r0, rn = GIVE[l]
        fine0 = lf.oy + 2 * (r0 - lc.oy)
        if l == 3:
            c0, r0 = 2 * gx + 1, 4 * gy + 4
            fine0 = 8
        zf = lane_index(rn)
        z = (jnp.where(zf < 100, zf, zf - 128) >> 1) + (8 * gz if l == 2 else 0)
        at, beside = z & 127, (z + 2 * (zf & 1) - 1) & 127

        def body(i):
            rows = pl.ds(r0, rn)
            r, b = R[l + 1][c0 + i, rows, :], B[l + 1][c0 + i, rows, :]
            if rn % 8:
                mm = ((iota((rn, 128), 0) + iota((rn, 128), 1)) & 1) == 1
                both = jnp.where(mm, b, r), jnp.where(mm, r, b)
            else:
                both = pick(m, b, r), pick(m, r, b)
            for a, e in enumerate(both):
                here, there = take(e, at), take(e, beside)
                for k in (0, 1):
                    EX[l][2 * i + a, pl.ds(fine0 + k, rn, stride=2), :] = here
                    EZ[l][2 * i + a, pl.ds(fine0 + k, rn, stride=2), :] = there

        sweep_loop(0, cn, 20, body)

    def correct(l):
        lv = LEV[l]
        second_row = (iota((8, 128), 0) & 1) == 1
        rows = pl.ds(lv.r0, lv.nr)

        def body(p):
            e = p - EDGE[l]
            t = kind(l, p)
            sides = pick(m, EX[l][e - 1, rows, :], EX[l][e + 1, rows, :])
            sides = sides + pick(second_row, EX[l][e, pl.ds(lv.r0 + 1, lv.nr), :], EX[l][e, pl.ds(lv.r0 - 1, lv.nr), :])
            add = EX[l][e, rows, :] * A[l][t] + (EZ[l][e, rows, :] + sides) * Q[l][t]
            return add, B[l]

        if l > 0:

            def plain(p):
                add, ref = body(p)
                ref[p, rows, :] = ref[p, rows, :] + add

            sweep_loop(lv.p0, lv.np, 12, plain)
        else:
            for i in range(-2, 34):
                g, j = slot_of(i, 32)
                p = 3 + i
                low, high = zr["v"][0][g, 4:76, :], zr["v"][1][g, 4:76, :]
                w = turn(pick(within(8 * j, 3), high, low), 64 - 8 * j)
                add, ref = body(p)
                ref[p, rows, :] = pick(lane < 64, H[p, rows, :], w) + add

    for l in (5, 4):
        expand(l)
        correct(l)
        red_sweep(l)
        black_sweep(l, False)
    expand(3)
    correct(3)
    red_sweep(3)
    black_sweep(3, False)
    expand(2)
    correct(2)
    red_sweep(2)
    black_sweep(2, False)
    expand(1)
    correct(1)
    red_sweep(1)
    black_sweep(1, False)
    expand(0)
    settle(kept, True, True)
    correct(0)
    red_sweep(0)
    black_sweep(0, True)

    lv = LEV[0]

    def results(p):
        r, b = R[0][p, 8:72, :], B[0][p, 8:72, :]
        x = 2 * (p - lv.po)
        u_out[x] = pick(m, b, r)[:, 0:64]
        u_out[x + 1] = pick(m, r, b)[:, 0:64]
        r, b = red_residual(0, p), T[p, 8:72, :]
        r_out[x] = pick(m, b, r)[:, 0:64]
        r_out[x + 1] = pick(m, r, b)[:, 0:64]

    sweep_loop(3, 32, 32, results)
    for what in (second, third, (k3, blocks), plane):
        settle(what, False, True)


EDGE = {0: -1, 1: -1, 2: -1, 3: -1, 4: 2, 5: -1}


def inside(d, me, far=1):
    ok = None
    for step, at in zip(d, me):
        if step:
            here = (at >= far) if step < 0 else (at < SIDE - far)
            ok = here if ok is None else ok & here
    return True if ok is None else ok


def vmem(*shape):
    return pltpu.VMEM(shape, F32)


def per_device(right_side, guess):
    whole = vmem(64, 64, 64)
    scratch = [whole, whole]
    for _ in range(4):
        scratch += [vmem(*lv.shape()) for lv in LEV]
    for _ in range(2):
        scratch += [vmem(4, 2, lv.nr, 128) for lv in LEV]
    for _ in range(2):
        scratch += [vmem(4, lv.nr, 128) for lv in LEV[:6]]
    for _ in range(2):
        scratch += [vmem(2 * GIVE[l][1], LEV[l].rows, 128) for l in range(6)]
    scratch += [vmem(*LEV[0].shape())] * 2
    scratch += [vmem(32, 32, 128), vmem(16, 16, 128)]
    scratch += [vmem(8, 32, 128), vmem(2, 16, 128), vmem(12, 64, 128), vmem(4, 48, 128)]
    scratch += [vmem(16, 16, 128), vmem(8, 8, 128)]
    packed = ((2, 64, 80), (2, 64, 80), (2, 32, 64), (1, 16, 48))
    for groups, n, _ in packed:
        scratch += [vmem(groups, n, 128)] * 2
    for groups, _, rows in packed:
        scratch += [vmem(groups + 2, rows, 128)] * 2
    scratch += [vmem(8, 128), vmem(3, 3, 8, 8, 128), vmem(8, 128), vmem(8, 32, 128), vmem(2048, 128)]
    dma = pltpu.SemaphoreType.DMA((len(PHASES),))
    scratch += [dma, dma, pltpu.SemaphoreType.DMA((2,)), pltpu.SemaphoreType.REGULAR((2,))]
    block = pltpu.VMEM(right_side.shape, F32)
    return pl.pallas_call(
        kernel,
        out_shape=(block, block),
        in_specs=[pl.BlockSpec(memory_space=pl.ANY)] * 2,
        out_specs=(pl.BlockSpec(memory_space=pltpu.VMEM),) * 2,
        scratch_shapes=scratch,
        compiler_params=pltpu.CompilerParams(collective_id=0, has_side_effects=True, vmem_limit_bytes=50 * 2**20),
    )(right_side, guess)


def solution(mesh):
    spec = P("gx", "gy", "gz")
    return jax.shard_map(per_device, mesh=mesh, in_specs=(spec, spec), out_specs=(spec, spec), check_vma=False)
```

```python
import itertools

import jax
import jax.numpy as jnp
from jax import lax
from jax.experimental import pallas as pl
from jax.experimental.pallas import tpu as pltpu
from jax.sharding import PartitionSpec as P

COARSE_SWEEPS = 4
MESH = pl.DeviceIdType.MESH
SIDE = 8
F32 = jnp.float32


class Level:
    def __init__(self, n, total, po, oy, p0, np_, r0, nr, pairs, rows, whole_z):
        self.n, self.total, self.po, self.oy = n, total, po, oy
        self.p0, self.np, self.r0, self.nr = p0, np_, r0, nr
        self.pairs, self.rows, self.whole_z = pairs, rows, whole_z

    def shape(self):
        return (self.pairs, self.rows, 128)


LEV = [
    Level(64, 512, 3, 8, 1, 36, 4, 72, 38, 80, False),
    Level(32, 256, 5, 16, 1, 24, 8, 48, 26, 64, False),
    Level(16, 128, 5, 16, 1, 16, 8, 32, 18, 48, False),
    Level(8, 64, 5, 16, 1, 12, 8, 24, 14, 40, True),
    Level(32, 32, 4, 8, 4, 16, 8, 32, 24, 48, True),
    Level(16, 16, 1, 8, 1, 8, 8, 16, 10, 32, True),
    Level(8, 8, 1, 8, 1, 4, 8, 8, 6, 24, True),
]
GIVE = {0: (3, 20, 12, 40), 1: (2, 14, 12, 24), 2: (2, 10, 12, 16), 3: (0, 8, 0, 12), 4: (0, 10, 8, 16), 5: (0, 6, 8, 8)}
PHASES = ("f", "v", 1, 2, "3", "4")
WIDTH = {1: 6, 2: 7}


def iota(shape, axis):
    return lax.broadcasted_iota(jnp.int32, shape, axis)


def odd():
    return ((iota((8, 128), 0) + iota((8, 128), 1)) & 1) == 1


def lanes():
    return iota((8, 128), 1)


def pick(mask, a, b):
    shape = a.shape
    if shape[0] <= 8:
        return jnp.where(mask[: shape[0]], a, b)
    tiles = (shape[0] // 8, 8, 128)
    return jnp.where(mask[None], a.reshape(tiles), b.reshape(tiles)).reshape(shape)


def within(start, width):
    return ((lanes() - start) & 127) < width


def turn(a, shift):
    return pltpu.roll(a, shift % 128, axis=1) if shift % 128 else a


def take(a, index):
    return jnp.take_along_axis(a, index, axis=1, mode="promise_in_bounds")


def lane_index(rows):
    return iota((rows, 128), 1)


def sweep_loop(start, count, step, body):
    step = max(k for k in range(1, step + 1) if count % k == 0)
    if count == step:
        for i in range(count):
            body(start + i)
        return

    def some(j, carry):
        for i in range(step):
            body(start + j * step + i)
        return carry

    lax.fori_loop(0, count // step, some, 0)


def around(src, p, r0, nr, up):
    here = src[p, pl.ds(r0, nr), :]
    side = pick(up, src[p + 1, pl.ds(r0, nr), :], src[p - 1, pl.ds(r0, nr), :])
    rows = src[p, pl.ds(r0 - 1, nr), :] + src[p, pl.ds(r0 + 1, nr), :]
    return (here + side) + rows + (pltpu.roll(here, 1, axis=1) + pltpu.roll(here, 127, axis=1))


def kernel(*refs):
    it = iter(refs)
    f_hbm, u_hbm, R0, B0, FR0, T, D0 = (next(it) for _ in range(7))
    f_in, u_in = next(it), next(it)
    R = [R0] + [next(it) for _ in range(6)]
    B = [B0] + [next(it) for _ in range(6)]
    FR = [FR0] + [next(it) for _ in range(6)]
    FB = [next(it) for _ in range(7)]
    C = [next(it) for _ in range(7)]
    D = [D0] + [next(it) for _ in range(6)]
    A = [next(it) for _ in range(6)]
    Q = [next(it) for _ in range(6)]
    EX = [next(it) for _ in range(6)]
    EZ = [next(it) for _ in range(6)]
    H = next(it)
    xs, xr = (next(it), next(it)), (next(it), next(it))
    ys, yr = (next(it), next(it)), (next(it), next(it))
    G = {1: next(it), 2: next(it)}
    PS = {1: next(it), 2: next(it)}
    PR = {1: next(it), 2: next(it)}
    N = {5: next(it), 6: next(it)}
    zs = {k: (next(it), next(it)) for k in ("f", "v", 1, 2)}
    zr = {k: (next(it), next(it)) for k in ("f", "v", 1, 2)}
    pack3, Z3, pack4, G4, tally = (next(it) for _ in range(5))
    send_sem, recv_sem, in_sem, token = (next(it) for _ in range(4))

    gx, gy, gz = lax.axis_index("gx"), lax.axis_index("gy"), lax.axis_index("gz")
    me = (gx, gy, gz)

    copies_in = []
    for i, (src, dst) in enumerate(((u_hbm, u_in), (f_hbm, f_in))):
        copy = pltpu.make_async_copy(src, dst, in_sem.at[i])
        copy.start()
        copies_in.append(copy)

    barrier = pltpu.get_barrier_semaphore()
    rooms = [jnp.where((at > 0) & (at < SIDE - 1), 3, 2) for at in me]
    for d in itertools.product((-1, 0, 1), repeat=3):
        if d != (0, 0, 0):

            @pl.when(inside(d, me))
            def _(d=d):
                pl.semaphore_signal(barrier, inc=1, device_id=tuple(at + step for at, step in zip(me, d)), device_id_type=MESH)

    pl.semaphore_wait(barrier, rooms[0] * rooms[1] * rooms[2] - 1)

    def tokens(k, far, act):
        count = jnp.int32(0)
        for d in itertools.product((-1, 0, 1), repeat=3):
            if d == (0, 0, 0) or (d[2] and (d[0] or d[1])):
                continue
            there = inside(d, me, far)
            count = count + jnp.where(there, 1, 0)
            if act:

                @pl.when(there)
                def _(d=d):
                    device = tuple(at + far * step for at, step in zip(me, d))
                    pl.semaphore_signal(token.at[k], inc=1, device_id=device, device_id_type=MESH)

        if not act:
            pl.semaphore_wait(token.at[k], count)

    lv = LEV[0]
    m64 = ((iota((64, 64), 0) + iota((64, 64), 1)) & 1) == 1
    for copy in copies_in:
        copy.wait()

    def apart(p):
        a, b = u_in[2 * (p - lv.po)], u_in[2 * (p - lv.po) + 1]
        B[0][p, 8:72, 0:64] = jnp.where(m64, a, b)
        a, b = f_in[2 * (p - lv.po)], f_in[2 * (p - lv.po) + 1]
        FR[0][p, 8:72, 0:64] = jnp.where(m64, b, a)
        FB[0][p, 8:72, 0:64] = jnp.where(m64, a, b)

    sweep_loop(3, 32, 8, apart)

    def pack_faces(get, out, count, low, high, width, apart):
        for g in range(count // 16):
            lo = hi = None
            for j in range(16):
                t = get(16 * g + j)
                a = turn(t, 8 * j)
                b = turn(t, 8 * j + apart) if apart else a
                if lo is None:
                    lo, hi = a, b
                else:
                    lo = pick(within(low + 8 * j, width), a, lo)
                    hi = pick(within(high + apart + 8 * j, width), b, hi)
            out[0][g] = lo
            out[1][g] = hi

    at_edge = [(at == 0) | (at == SIDE - 1) for at in me]

    def halo(key, directions, pieces):
        k = PHASES.index(key)
        total = dict.fromkeys(EDGES, 0)
        for d in directions:
            copies = pieces(d)

            @pl.when(inside(d, me))
            def _(d=d, copies=copies):
                device = tuple(at + step for at, step in zip(me, d))
                for src, dst, _ in copies:
                    pltpu.make_async_remote_copy(
                        src, dst, send_sem.at[k], recv_sem.at[k], device_id=device, device_id_type=MESH
                    ).start()

            for edge in total:
                if not any(e and step > 0 for e, step in zip(edge, d)):
                    total[edge] += sum(rows for _, _, rows in copies)
        return k, total

    def both(a, b):
        return a[0], {edge: a[1][edge] + b[1][edge] for edge in EDGES}

    def sides(arrays, oy, n):
        def pieces(d):
            out = []
            for src, ps, dst, pd, own, hp, hr in arrays:
                s0, d0, w = {-1: (ps, pd + own, hp), 0: (ps, pd, own), 1: (ps + own - hp, pd - hp, hp)}[d[0]]
                rs, rd, rw = {-1: (0, oy + n, hr), 0: (0, oy, n), 1: (n - hr, oy - hr, hr)}[d[1]]
                rs = rs + (oy if src.shape[1] > n else 0)
                out.append((src.at[pl.ds(s0, w), pl.ds(rs, rw), :], dst.at[pl.ds(d0, w), pl.ds(rd, rw), :], w * rw))
            return out

        return pieces

    def faces(key, oy, n, hz):
        groups = zs[key][0].shape[0]

        def pieces(d):
            s0, d0, w = {-1: (0, groups + 1, 1), 0: (0, 1, groups), 1: (groups - 1, 0, 1)}[d[0]]
            rs, rd, rw = {-1: (0, oy + n, hz), 0: (0, oy, n), 1: (n - hz, oy - hz, hz)}[d[1]]
            src, dst = (zs[key][0], zr[key][1]) if d[2] < 0 else (zs[key][1], zr[key][0])
            return [(src.at[pl.ds(s0, w), pl.ds(rs, rw), :], dst.at[pl.ds(d0, w), pl.ds(rd, rw), :], w * rw)]

        return pieces

    def exchange(key, arrays, oy, n, hz):
        packed = halo(key, ACROSS, faces(key, oy, n, hz))
        return both(packed, halo(key, FLAT, sides(arrays, oy, n)))

    def settle(what, arrived, left):
        k, total = what
        other = tuple(jnp.where(at == 0, at + 1, at - 1) for at in me)
        for edge, rows in total.items():
            same = None
            for e, here in zip(edge, at_edge):
                t = here if e else jnp.logical_not(here)
                same = t if same is None else same & t

            @pl.when(same)
            def _(rows=rows):
                cut = tally.at[pl.ds(0, rows), :]
                copy = pltpu.make_async_remote_copy(cut, cut, send_sem.at[k], recv_sem.at[k], device_id=other, device_id_type=MESH)
                if arrived:
                    copy.wait_recv()
                if left:
                    copy.wait_send()

    lane, m = lanes(), odd()
    not_m = jnp.logical_not(m)
    for side, (near, next_) in enumerate(((3, 4), (34, 33))):
        for k, (a, other) in enumerate(((near, FR[0]), (next_, FB[0]))):
            xs[side][k] = pick(lane < 64, B[0][a, 8:72, :], turn(other[near, 8:72, :], 64))

    def first_sides(d):
        side = 0 if d[0] < 0 else 1
        rs, rd, rw = {-1: (0, 72, 3), 0: (0, 8, 64), 1: (61, 5, 3)}[d[1]]
        return [(xs[side].at[:, pl.ds(rs, rw), :], xr[1 - side].at[:, pl.ds(rd, rw), :], 2 * rw)]

    first = halo("f", [d for d in FLAT if d[0]], first_sides)
    third_row = iota((8, 128), 0) == 2
    for i in range(32):
        p = 3 + i
        for side, (rb, rr, rk) in enumerate(((8, 8, 6), (69, 70, 69))):
            t = turn(jnp.where(third_row, FB[0][p, rk : rk + 8, :], FR[0][p, rr : rr + 8, :]), 64)
            ys[side][i] = jnp.where(lane < 64, B[0][p, rb : rb + 8, :], t)

    def first_rows(d):
        side = 0 if d[1] < 0 else 1
        return [(ys[side].at[:, pl.ds(0, 3), :], yr[1 - side].at[:, pl.ds(0, 3), :], 96)]

    first = both(first, halo("f", [d for d in FLAT if not d[0]], first_rows))
    at_fb = within(5, 1) | within(68, 1)
    at_fr = within(3, 2) | within(65, 2)

    for p in range(3, 35):
        t = pick(at_fb, turn(FB[0][p, 8:72, :], 5), B[0][p, 8:72, :])
        T[p, 8:72, :] = pick(at_fr, turn(FR[0][p, 8:72, :], 3), t)
    pack_faces(lambda i: T[3 + i, 8:72, :], zs["f"], 32, 0, 61, 8, 0)
    first = both(first, halo("f", ACROSS, faces("f", 8, 64, 3)))

    def outside(ref, po, own, hp, oy, n, hr):
        planes, rows = ref.shape[0], ref.shape[1]
        for cond, cut in (
            (gx == 0, (slice(po - hp, po), slice(0, rows))),
            (gx == SIDE - 1, (slice(po + own, po + own + hp), slice(0, rows))),
            (gy == 0, (slice(0, planes), slice(oy - hr, oy))),
            (gy == SIDE - 1, (slice(0, planes), slice(oy + n, oy + n + hr))),
        ):

            @pl.when(cond)
            def _(cut=cut):
                shape = (cut[1].stop - cut[1].start, 128)
                for p in range(cut[0].start, cut[0].stop):
                    ref[p, cut[1], :] = jnp.zeros(shape, F32)

    def outside_z(key):
        for side, cond in ((0, gz == 0), (1, gz == SIDE - 1)):

            @pl.when(cond)
            def _(side=side):
                ref = zr[key][side]
                ref[...] = jnp.zeros(ref.shape, F32)

    def edges_z(key, po, n, hz, oy, groups):
        for side in (0, 1):
            ref = zr[key][side]
            rows = ref.shape[1]
            for cond, cut in (
                (gx == 0, (0, 1, 0, rows)),
                (gx == SIDE - 1, (groups + 1, 1, 0, rows)),
                (gy == 0, (0, groups + 2, oy - hz, hz)),
                (gy == SIDE - 1, (0, groups + 2, oy + n, hz)),
            ):

                @pl.when(cond)
                def _(cut=cut, ref=ref):
                    ref[pl.ds(cut[0], cut[1]), pl.ds(cut[2], cut[3]), :] = jnp.zeros((cut[1], cut[3], 128), F32)

    outside(H, 3, 32, 2, 8, 64, 3)
    for i in range(2):
        for cond, refs0 in ((gx == (0, SIDE - 1)[i], (xr[i],)), (gy == (0, SIDE - 1)[i], (yr[i],))):

            @pl.when(cond)
            def _(refs0=refs0):
                for ref in refs0:
                    ref[...] = jnp.zeros(ref.shape, F32)

        @pl.when(gy == (0, SIDE - 1)[i])
        def _(i=i):
            for ref in xr:
                for k in range(2):
                    ref[k, pl.ds((5, 72)[i], 3), :] = jnp.zeros((3, 128), F32)

    for key, n, oy, groups, hz in (("f", 64, 8, 2, 3), ("v", 64, 8, 2, 3), (1, 32, 16, 2, 6), (2, 16, 16, 1, 7)):
        outside_z(key)
        edges_z(key, 3, n, hz, oy, groups)
    outside(PR[1], 2, 8, 2, 16, 32, 8)
    outside(PR[2], 1, 2, 1, 16, 16, 8)
    for dx, dy in itertools.product((-1, 0, 1), repeat=2):
        if (dx, dy) != (0, 0):

            @pl.when(jnp.logical_not(inside((dx, dy, 0), me)))
            def _(dx=dx, dy=dy):
                Z3[dx + 1, dy + 1] = jnp.zeros((4 * SIDE, 128), F32)

    for l in (4, 5, 6):
        R[l][...] = jnp.zeros(LEV[l].shape(), F32)
        B[l][...] = jnp.zeros(LEV[l].shape(), F32)
    for l in (4, 5):
        EX[l][...] = jnp.zeros(EX[l].shape, F32)

    def tables(l):
        lv = LEV[l]
        shape = (lv.nr, 128)
        row, lane = iota(shape, 0) + lv.r0, iota(shape, 1)
        y = row - lv.oy
        z = jnp.where(lane < 100, lane, lane - 128)
        if l < 4:
            y = y + gy * lv.n
        if l < 3:
            z = z + gz * lv.n
        last = lv.total - 1
        within = (y >= 0) & (y <= last) & (z >= 0) & (z <= last)
        one = lambda c: jnp.where(c, 1, 0)
        w = one(y == 0) + one(y == last) + one(z == 0) + one(z == last)
        high = one(((row + lane) & 1) == 1)
        for kind, colour in itertools.product(range(3), range(2)):
            a = high if colour == 0 else 1 - high
            d = w if kind == 0 else (w + 1 - a if kind == 1 else w + a)
            inv = jnp.where(d == 0, 1 / 6, jnp.where(d == 1, 1 / 7, jnp.where(d == 2, 1 / 8, 1 / 9)))
            C[l][kind, colour] = jnp.where(within, inv, 0.0)
            D[l][kind, colour] = 6.0 + d.astype(F32)
            if colour == 1 and l < 6:
                q = jnp.where(within, 0.25, 0.0)
                Q[l][kind] = q
                A[l][kind] = (1.0 - d.astype(F32)) * q
        for colour in range(2):
            C[l][3, colour] = jnp.zeros(shape, F32)
            D[l][3, colour] = jnp.full(shape, 6.0, F32)
        if l < 6:
            Q[l][3] = jnp.zeros(shape, F32)
            A[l][3] = jnp.zeros(shape, F32)

    for l in range(7):
        tables(l)

    def kind(l, p):
        lv = LEV[l]
        x = 2 * (p - lv.po) + (gx * lv.n if l < 4 else 0)
        if l >= 4:
            return jnp.where(x == 0, 1, jnp.where(x == lv.total - 2, 2, 0))
        return jnp.where(x == 0, 1, jnp.where(x == lv.total - 2, 2, jnp.where((x < 0) | (x >= lv.total), 3, 0)))

    settle(first, True, True)
    tokens(0, 2, True)

    def slot_of(i, n):
        groups = n // 16
        if i < 0:
            return 0, 16 + i
        if i >= n:
            return groups + 1, i - n
        return 1 + i // 16, i % 16

    def unpack_first(i):
        g, j = slot_of(i, 32)
        low, high = zr["f"][0][g, 4:76, :], zr["f"][1][g, 4:76, :]
        for ref, at, width, shift in ((B[0], 0, 3, 64), (FR[0], 3, 2, 61), (FB[0], 5, 1, 59)):
            w = turn(pick(within(8 * j + at, width), high, low), shift - 8 * j)
            ref[3 + i, 4:76, :] = pick(lane < 64, ref[3 + i, 4:76, :], w)

    for side, (near, next_) in enumerate(((2, 1), (35, 36))):
        rows = pl.ds(4, 72)
        a, b = xr[side][0, rows, :], xr[side][1, rows, :]
        B[0][near, rows, :] = a
        B[0][next_, rows, :] = b
        FR[0][near, rows, :] = turn(a, 64)
        FB[0][near, rows, :] = turn(b, 64)
    for i in range(32):
        for side, (rb, rr, rk) in enumerate(((5, 6, 7), (72, 72, 72))):
            t = yr[side][i]
            f = turn(t, 64)
            B[0][3 + i, rb : rb + 3, :] = t[0:3]
            FR[0][3 + i, rr : rr + 2, :] = f[0:2]
            FB[0][3 + i, rk : rk + 1, :] = f[2:3]
    for i in range(-2, 34):
        unpack_first(i)

    def red_sweep(l):
        lv = LEV[l]

        def body(p):
            s = around(B[l], p, lv.r0, lv.nr, m)
            R[l][p, pl.ds(lv.r0, lv.nr), :] = (FR[l][p, pl.ds(lv.r0, lv.nr), :] + s) * C[l][kind(l, p), 0]

        sweep_loop(lv.p0, lv.np, 36, body)

    def black_sweep(l, keep):
        lv = LEV[l]

        def body(p):
            t = kind(l, p)
            rows = pl.ds(lv.r0, lv.nr)
            fs = FB[l][p, rows, :] + around(R[l], p, lv.r0, lv.nr, not_m)
            b = fs * C[l][t, 1]
            B[l][p, rows, :] = b
            if keep:
                T[p, rows, :] = fs - D[l][t, 1] * b

        sweep_loop(lv.p0, lv.np, 36, body)

    def red_residual(l, p):
        lv = LEV[l]
        s = around(B[l], p, lv.oy, lv.n, m)
        at = lv.oy - lv.r0
        return FR[l][p, pl.ds(lv.oy, lv.n), :] + s - D[l][kind(l, p), 0, pl.ds(at, lv.n), :] * R[l][p, pl.ds(lv.oy, lv.n), :]

    def residual(l):
        lv = LEV[l]

        def body(p):
            T[p, pl.ds(lv.oy, lv.n), :] = T[p, pl.ds(lv.oy, lv.n), :] + red_residual(l, p)

        sweep_loop(lv.po, lv.n // 2, 16, body)

    def coarse_side(l, p):
        lv = LEV[l]
        half = lv.n // 2
        u = T[p, pl.ds(lv.oy, half, stride=2), :] + T[p, pl.ds(lv.oy + 1, half, stride=2), :]
        z = 2 * lane_index(half)
        return 0.5 * (take(u, z & 127) + take(u, (z + 1) & 127))

    red_sweep(0)
    black_sweep(0, True)

    def keep_black(p):
        H[p, 8:72, :] = B[0][p, 8:72, :]

    sweep_loop(3, 32, 8, keep_black)

    def restrict_to(l, dst, first_plane, first_row):
        lv = LEV[l]

        def body(p):
            dst[p - lv.po + first_plane, pl.ds(first_row, lv.n // 2), :] = coarse_side(l, p)

        sweep_loop(lv.po, lv.n // 2, 16, body)

    residual(0)
    restrict_to(0, G[1], 0, 0)

    def send_right_side(l):
        n, w = LEV[l].n, WIDTH[l]
        per = 128 // n
        for q in range(n // per):
            t = G[l][per * q]
            for j in range(1, per):
                t = pick(within(n * j, n), turn(G[l][per * q + j], n * j), t)
            PS[l][q] = t
        pack_faces(lambda i: G[l][i], zs[l], n, 0, n - 8, 8, 128 - 2 * n)
        wide = 8 // per
        return exchange(l, [(PS[l], 0, PR[l], wide, n // per, wide, w)], 16, n, w)

    def split_right_side(l):
        lv = LEV[l]
        n = lv.n
        per = 128 // n

        def natural(i):
            g, j = slot_of(i, n)
            rows = pl.ds(lv.r0, lv.nr)
            side = pick(within(8 * j, 8), zr[l][1][g, rows, :], zr[l][0][g, rows, :])
            q, k = (i + 8) // per, (i + 8) % per
            if 0 <= i < n:
                below, above = (turn(PR[l][q, pl.ds(r, 8), :], -n * k) for r in (8, 16 + n))
                here = jnp.concatenate([below, G[l][i], above], axis=0)
            else:
                here = turn(PR[l][q, rows, :], -n * k)
            return pick(lane < n, here, turn(side, n - 8 * j))

        for p in range(lv.p0, lv.p0 + lv.np):
            a, b = natural(2 * (p - lv.po)), natural(2 * (p - lv.po) + 1)
            store_colours(l, p, a, b)

    def store_colours(l, p, a, b):
        lv = LEV[l]
        rows = pl.ds(lv.r0, lv.nr)
        red = pick(m, b, a)
        FR[l][p, rows, :] = red
        FB[l][p, rows, :] = pick(m, a, b)
        R[l][p, rows, :] = red * C[l][kind(l, p), 0]

    second = send_right_side(1)
    tokens(0, 2, False)
    tokens(1, 4, True)
    pack_faces(lambda i: B[0][3 + i, 8:72, :], zs["v"], 32, 0, 61, 3, 0)
    kept = exchange("v", [(B[0], 3, H, 3, 32, 2, 3)], 8, 64, 3)
    settle(second, True, False)
    split_right_side(1)
    black_sweep(1, True)
    residual(1)
    restrict_to(1, G[2], 0, 0)
    third = send_right_side(2)
    settle(kept, True, True)
    for i in range(-2, 34):
        g, j = slot_of(i, 32)
        w = turn(pick(within(8 * j, 3), zr["v"][1][g, 4:76, :], zr["v"][0][g, 4:76, :]), 64 - 8 * j)
        H[3 + i, 4:76, :] = pick(lane < 64, H[3 + i, 4:76, :], w)
    settle(third, True, False)
    split_right_side(2)
    black_sweep(2, True)
    residual(2)

    own3 = None
    for i in range(8):
        g = jnp.where(lane < 8, coarse_side(2, LEV[2].po + i), 0.0)
        g = pltpu.roll(g, 8 * lax.rem(gz + i, 8), axis=1)
        own3 = g if own3 is None else own3 + g
    pack3[0:8, :] = own3
    own3 = jnp.where(lane[0:4] < 64, pack3[0:4, :], turn(pack3[4:8, :], 64))
    pack3[8:12, :] = own3
    Z3[1, 1, pl.ds(4 * gz, 4), :] = own3
    tokens(1, 4, False)

    k3 = PHASES.index("3")
    for dx, dy in sorted(itertools.product((-1, 0, 1), repeat=2), key=lambda d: -abs(d[0]) - abs(d[1])):

        @pl.when(inside((dx, dy, 0), me))
        def _(dx=dx, dy=dy):
            for far in (4, 3, 5, 2, 6, 1, 7, 0):
                if (dx, dy, far) != (0, 0, 0):
                    pltpu.make_async_remote_copy(
                        pack3.at[pl.ds(8, 4), :],
                        Z3.at[1 - dx, 1 - dy, pl.ds(4 * gz, 4), :],
                        send_sem.at[k3],
                        recv_sem.at[k3],
                        device_id=(gx + dx, gy + dy, (gz + far) & (SIDE - 1)),
                        device_id_type=MESH,
                    ).start()

    blocks = {edge: 4 * ((2 if edge[0] else 3) * (2 if edge[1] else 3) * SIDE - 1) for edge in EDGES}
    settle((k3, blocks), True, False)

    for p in range(1, 13):
        ab = []
        for i in (2 * (p - 1), 2 * (p - 1) + 1):
            x = i % 8
            tiles = []
            for cy in range(3):
                t = None
                for k in range(SIDE):
                    block = Z3[i // 8, cy, 4 * k : 4 * k + 4, :]
                    s = 8 * ((x + k) % 8)
                    t = block if t is None else jnp.where((within(s, 8) | within(s + 64, 8))[0:4], block, t)
                other = turn(t, 64)
                low = lane[0:4] < 64
                t = jnp.concatenate([jnp.where(low, t, other), jnp.where(low, other, t)], axis=0)
                tiles.append(turn(t, -8 * x))
            ab.append(jnp.concatenate(tiles, axis=0))
        store_colours(3, p, ab[0], ab[1])
    black_sweep(3, True)

    residual(3)
    own4 = None
    for i in range(4):
        g = turn(pick(lane < 32, coarse_side(3, LEV[3].po + i), jnp.zeros((4, 128), F32)), 32 * i)
        own4 = g if own4 is None else own4 + g
    pack4[0:4, :] = own4
    G4[gx, pl.ds(4 * gy, 4), :] = own4

    k4 = PHASES.index("4")

    ring = lambda k: min(k, SIDE - k)
    for dx, dy in sorted(itertools.product(range(SIDE), repeat=2), key=lambda d: -ring(d[0]) - ring(d[1])):
        if (dx, dy) != (0, 0):
            pltpu.make_async_remote_copy(
                pack4.at[pl.ds(0, 4), :],
                G4.at[gx, pl.ds(4 * gy, 4), :],
                send_sem.at[k4],
                recv_sem.at[k4],
                device_id=((gx + dx) & (SIDE - 1), (gy + dy) & (SIDE - 1), gz),
                device_id_type=MESH,
            ).start()
    plane = (k4, dict.fromkeys(EDGES, 4 * (SIDE * SIDE - 1)))
    settle(plane, True, False)
    for x in range(SIDE):
        parts = [turn(G4[x], -32 * i) for i in range(4)]
        store_colours(4, 4 + 2 * x, parts[0], parts[1])
        store_colours(4, 5 + 2 * x, parts[2], parts[3])
    for l in (4, 5):
        black_sweep(l, True)
        residual(l)
        restrict_to(l, N[l + 1], 0, 0)
        lv = LEV[l + 1]
        for p in range(lv.p0, lv.p0 + lv.np):
            store_colours(l + 1, p, N[l + 1][2 * (p - 1)], N[l + 1][2 * (p - 1) + 1])
    black_sweep(6, False)
    for _ in range(COARSE_SWEEPS - 1):
        red_sweep(6)
        black_sweep(6, False)

    def expand(l):
        lf, lc = LEV[l], LEV[l + 1]
        c0, cn, r0, rn = GIVE[l]
        fine0 = lf.oy + 2 * (r0 - lc.oy)
        if l == 3:
            c0, r0 = 2 * gx + 1, 4 * gy + 4
            fine0 = 8
        zf = lane_index(rn)
        z = (jnp.where(zf < 100, zf, zf - 128) >> 1) + (8 * gz if l == 2 else 0)
        at, beside = z & 127, (z + 2 * (zf & 1) - 1) & 127

        def body(i):
            rows = pl.ds(r0, rn)
            r, b = R[l + 1][c0 + i, rows, :], B[l + 1][c0 + i, rows, :]
            if rn % 8:
                mm = ((iota((rn, 128), 0) + iota((rn, 128), 1)) & 1) == 1
                both = jnp.where(mm, b, r), jnp.where(mm, r, b)
            else:
                both = pick(m, b, r), pick(m, r, b)
            for a, e in enumerate(both):
                here, there = take(e, at), take(e, beside)
                for k in (0, 1):
                    EX[l][2 * i + a, pl.ds(fine0 + k, rn, stride=2), :] = here
                    EZ[l][2 * i + a, pl.ds(fine0 + k, rn, stride=2), :] = there

        sweep_loop(0, cn, 20, body)

    def correct(l):
        lv = LEV[l]
        second_row = (iota((8, 128), 0) & 1) == 1
        rows = pl.ds(lv.r0, lv.nr)

        def body(p):
            e = p - EDGE[l]
            t = kind(l, p)
            sides = pick(m, EX[l][e - 1, rows, :], EX[l][e + 1, rows, :])
            sides = sides + pick(second_row, EX[l][e, pl.ds(lv.r0 + 1, lv.nr), :], EX[l][e, pl.ds(lv.r0 - 1, lv.nr), :])
            add = EX[l][e, rows, :] * A[l][t] + (EZ[l][e, rows, :] + sides) * Q[l][t]
            return add

        start = B[l] if l else H

        def plain(p):
            B[l][p, rows, :] = start[p, rows, :] + body(p)

        sweep_loop(lv.p0, lv.np, 36, plain)

    for l in (5, 4):
        expand(l)
        correct(l)
        red_sweep(l)
        black_sweep(l, False)
    expand(3)
    correct(3)
    red_sweep(3)
    black_sweep(3, False)
    expand(2)
    correct(2)
    red_sweep(2)
    black_sweep(2, False)
    expand(1)
    correct(1)
    red_sweep(1)
    black_sweep(1, False)
    expand(0)
    correct(0)
    red_sweep(0)
    black_sweep(0, True)

    for what in (second, third, (k3, blocks), plane):
        settle(what, False, True)


def results(R, B, FR, T, D, u_out, r_out):
    lv = LEV[0]
    m = odd()
    first = lv.po + 8 * pl.program_id(0)
    for k in range(8):
        p = first + k
        x = lax.axis_index("gx") * lv.n + 2 * (p - lv.po)
        kind = jnp.where(x == 0, 1, jnp.where(x == lv.total - 2, 2, 0))
        r, b = R[p, 8:72, :], B[p, 8:72, :]
        u_out[2 * k] = pick(m, b, r)[:, 0:64]
        u_out[2 * k + 1] = pick(m, r, b)[:, 0:64]
        left = FR[p, 8:72, :] + around(B, p, lv.oy, lv.n, m) - D[kind, 0, 4:68, :] * r
        b = T[p, 8:72, :]
        r_out[2 * k] = pick(m, b, left)[:, 0:64]
        r_out[2 * k + 1] = pick(m, left, b)[:, 0:64]


EDGES = tuple(itertools.product((False, True), repeat=3))
AROUND = sorted((d for d in itertools.product((-1, 0, 1), repeat=3) if any(d)), key=lambda d: -sum(map(abs, d)))
FLAT = [d for d in AROUND if d[2] == 0]
ACROSS = [d for d in AROUND if d[2]]
EDGE = {0: -1, 1: -1, 2: -1, 3: -1, 4: 2, 5: -1}


def inside(d, me, far=1):
    ok = None
    for step, at in zip(d, me):
        if step:
            here = (at >= far) if step < 0 else (at < SIDE - far)
            ok = here if ok is None else ok & here
    return True if ok is None else ok


def vmem(*shape):
    return pltpu.VMEM(shape, F32)


def per_device(right_side, guess):
    whole = vmem(64, 64, 64)
    scratch = [whole, whole]
    for _ in range(3):
        scratch += [vmem(*lv.shape()) for lv in LEV[1:]]
    scratch += [vmem(*lv.shape()) for lv in LEV]
    scratch += [vmem(4, 2, lv.nr, 128) for lv in LEV]
    scratch += [vmem(4, 2, lv.nr, 128) for lv in LEV[1:]]
    for _ in range(2):
        scratch += [vmem(4, lv.nr, 128) for lv in LEV[:6]]
    for _ in range(2):
        scratch += [vmem(2 * GIVE[l][1], LEV[l].rows, 128) for l in range(6)]
    scratch += [vmem(*LEV[0].shape())]
    scratch += [vmem(2, 64, 128)] * 2 + [vmem(2, 80, 128)] * 2 + [vmem(32, 8, 128)] * 4
    scratch += [vmem(32, 32, 128), vmem(16, 16, 128)]
    scratch += [vmem(8, 32, 128), vmem(2, 16, 128), vmem(12, 64, 128), vmem(4, 48, 128)]
    scratch += [vmem(16, 16, 128), vmem(8, 8, 128)]
    packed = ((2, 64, 80), (2, 64, 80), (2, 32, 64), (1, 16, 48))
    for groups, n, _ in packed:
        scratch += [vmem(groups, n, 128)] * 2
    for groups, _, rows in packed:
        scratch += [vmem(groups + 2, rows, 128)] * 2
    scratch += [vmem(16, 128), vmem(3, 3, 32, 128), vmem(8, 128), vmem(8, 32, 128), vmem(2048, 128)]
    dma = pltpu.SemaphoreType.DMA((len(PHASES),))
    scratch += [dma, dma, pltpu.SemaphoreType.DMA((2,)), pltpu.SemaphoreType.REGULAR((2,))]
    level0 = pltpu.VMEM(LEV[0].shape(), F32)
    parts = pl.pallas_call(
        kernel,
        out_shape=(level0,) * 4 + (pltpu.VMEM((4, 2, LEV[0].nr, 128), F32),),
        in_specs=[pl.BlockSpec(memory_space=pl.ANY)] * 2,
        out_specs=(pl.BlockSpec(memory_space=pltpu.VMEM),) * 5,
        scratch_shapes=scratch,
        compiler_params=pltpu.CompilerParams(collective_id=0, has_side_effects=True, vmem_limit_bytes=48 * 2**20),
    )(right_side, guess)
    block = jax.ShapeDtypeStruct(right_side.shape, F32)
    return pl.pallas_call(
        results,
        grid=(4,),
        out_shape=(block, block),
        in_specs=[pl.BlockSpec(memory_space=pltpu.VMEM)] * 5,
        out_specs=(pl.BlockSpec((16, 64, 64), lambda i: (i, 0, 0)),) * 2,
        compiler_params=pltpu.CompilerParams(vmem_limit_bytes=12 * 2**20),
    )(*parts)


def solution(mesh):
    spec = P("gx", "gy", "gz")
    return jax.shard_map(per_device, mesh=mesh, in_specs=(spec, spec), out_specs=(spec, spec), check_vma=False)
```

```python
import itertools

import jax
import jax.numpy as jnp
from jax import lax
from jax.experimental import pallas as pl
from jax.experimental.pallas import tpu as pltpu
from jax.sharding import PartitionSpec as P

COARSE_SWEEPS = 4
MESH = pl.DeviceIdType.MESH
SIDE = 8
F32 = jnp.float32


class Level:
    def __init__(self, n, total, po, oy, p0, np_, r0, nr, pairs, rows, whole_z):
        self.n, self.total, self.po, self.oy = n, total, po, oy
        self.p0, self.np, self.r0, self.nr = p0, np_, r0, nr
        self.pairs, self.rows, self.whole_z = pairs, rows, whole_z

    def shape(self):
        return (self.pairs, self.rows, 128)


LEV = [
    Level(64, 512, 3, 8, 1, 36, 4, 72, 38, 80, False),
    Level(32, 256, 5, 16, 1, 24, 8, 48, 26, 64, False),
    Level(16, 128, 5, 16, 1, 16, 8, 32, 18, 48, False),
    Level(8, 64, 5, 16, 1, 12, 8, 24, 14, 40, True),
    Level(32, 32, 4, 8, 4, 16, 8, 32, 24, 48, True),
    Level(16, 16, 1, 8, 1, 8, 8, 16, 10, 32, True),
    Level(8, 8, 1, 8, 1, 4, 8, 8, 6, 24, True),
]
GIVE = {0: (3, 20, 12, 40), 1: (2, 14, 12, 24), 2: (2, 10, 12, 16), 3: (0, 8, 0, 12), 4: (0, 10, 8, 16), 5: (0, 6, 8, 8)}
ALL = {4: (4, 16, 8, 32), 5: (1, 8, 8, 16), 6: (1, 4, 8, 8)}
RED = {0: (2, 34, 4, 72), 1: (3, 20, 12, 40), 2: (2, 14, 8, 32), 3: (2, 10, 8, 24), **ALL}
BLACK_DOWN = {0: (2, 34, 4, 72), 1: (2, 22, 8, 48), 2: (2, 14, 8, 32), 3: (2, 10, 8, 24), **ALL}
BLACK_UP = {1: (3, 20, 12, 40), 2: (3, 12, 12, 24), 3: (3, 8, 12, 16), **ALL}
CORRECTED = {0: (1, 36, 4, 72), 1: (2, 22, 8, 48), 2: (2, 14, 8, 32), 3: (2, 10, 8, 24), **ALL}
PHASES = ("f", "v", 1, 2, "3", "4")
WIDTH = {1: 6, 2: 7}


def iota(shape, axis):
    return lax.broadcasted_iota(jnp.int32, shape, axis)


def odd():
    return ((iota((8, 128), 0) + iota((8, 128), 1)) & 1) == 1


def lanes():
    return iota((8, 128), 1)


def pick(mask, a, b):
    shape = a.shape
    if shape[0] <= 8:
        return jnp.where(mask[: shape[0]], a, b)
    tiles = (shape[0] // 8, 8, 128)
    return jnp.where(mask[None], a.reshape(tiles), b.reshape(tiles)).reshape(shape)


def within(start, width):
    return ((lanes() - start) & 127) < width


def turn(a, shift):
    return pltpu.roll(a, shift % 128, axis=1) if shift % 128 else a


def take(a, index):
    return jnp.take_along_axis(a, index, axis=1, mode="promise_in_bounds")


def lane_index(rows):
    return iota((rows, 128), 1)


def sweep_loop(start, count, step, body):
    step = max(k for k in range(1, step + 1) if count % k == 0)
    if count == step:
        for i in range(count):
            body(start + i)
        return

    def some(j, carry):
        for i in range(step):
            body(start + j * step + i)
        return carry

    lax.fori_loop(0, count // step, some, 0)


def around(src, p, r0, nr, up):
    here = src[p, pl.ds(r0, nr), :]
    side = pick(up, src[p + 1, pl.ds(r0, nr), :], src[p - 1, pl.ds(r0, nr), :])
    rows = src[p, pl.ds(r0 - 1, nr), :] + src[p, pl.ds(r0 + 1, nr), :]
    return (here + side) + rows + (pltpu.roll(here, 1, axis=1) + pltpu.roll(here, 127, axis=1))


def kernel(*refs):
    it = iter(refs)
    f_hbm, u_hbm, R0, FR0, FB0, C0, D0 = (next(it) for _ in range(7))
    f_in, u_in = next(it), next(it)
    R = [R0] + [next(it) for _ in range(6)]
    B = [next(it) for _ in range(7)]
    FR = [FR0] + [next(it) for _ in range(6)]
    FB = [FB0] + [next(it) for _ in range(6)]
    C = [C0] + [next(it) for _ in range(6)]
    D = [D0] + [next(it) for _ in range(6)]
    A = [next(it) for _ in range(6)]
    Q = [next(it) for _ in range(6)]
    EX = [next(it) for _ in range(6)]
    EZ = [next(it) for _ in range(6)]
    T, H = next(it), next(it)
    xs, xr = (next(it), next(it)), (next(it), next(it))
    ys, yr = (next(it), next(it)), (next(it), next(it))
    G = {1: next(it), 2: next(it)}
    PS = {1: next(it), 2: next(it)}
    PR = {1: next(it), 2: next(it)}
    N = {5: next(it), 6: next(it)}
    zs = {k: (next(it), next(it)) for k in ("f", "v", 1, 2)}
    zr = {k: (next(it), next(it)) for k in ("f", "v", 1, 2)}
    pack3, Z3, pack4, G4, tally = (next(it) for _ in range(5))
    send_sem, recv_sem, in_sem, token = (next(it) for _ in range(4))

    gx, gy, gz = lax.axis_index("gx"), lax.axis_index("gy"), lax.axis_index("gz")
    me = (gx, gy, gz)

    def fetch(c):
        cut = pl.ds(32 * c, 32)
        return [
            pltpu.make_async_copy(src.at[cut], dst.at[cut], in_sem.at[2 * c + i])
            for i, (src, dst) in enumerate(((u_hbm, u_in), (f_hbm, f_in)))
        ]

    for c in range(2):
        for copy in fetch(c):
            copy.start()

    barrier = pltpu.get_barrier_semaphore()
    rooms = [jnp.where((at > 0) & (at < SIDE - 1), 3, 2) for at in me]
    for d in itertools.product((-1, 0, 1), repeat=3):
        if d != (0, 0, 0):

            @pl.when(inside(d, me))
            def _(d=d):
                pl.semaphore_signal(barrier, inc=1, device_id=tuple(at + step for at, step in zip(me, d)), device_id_type=MESH)

    def tokens(k, far, act):
        count = jnp.int32(0)
        for d in itertools.product((-1, 0, 1), repeat=3):
            if d == (0, 0, 0) or (d[2] and (d[0] or d[1])):
                continue
            there = inside(d, me, far)
            count = count + jnp.where(there, 1, 0)
            if act:

                @pl.when(there)
                def _(d=d):
                    device = tuple(at + far * step for at, step in zip(me, d))
                    pl.semaphore_signal(token.at[k], inc=1, device_id=device, device_id_type=MESH)

        if not act:
            pl.semaphore_wait(token.at[k], count)

    lv = LEV[0]
    m64 = ((iota((64, 64), 0) + iota((64, 64), 1)) & 1) == 1
    lane, m = lanes(), odd()
    not_m = jnp.logical_not(m)
    at_fb = within(5, 1) | within(68, 1)
    at_fr = within(3, 2) | within(65, 2)
    third_row = iota((8, 128), 0) == 2

    def apart(p):
        a, b = u_in[2 * (p - lv.po)], u_in[2 * (p - lv.po) + 1]
        B[0][p, 8:72, 0:64] = jnp.where(m64, a, b)
        a, b = f_in[2 * (p - lv.po)], f_in[2 * (p - lv.po) + 1]
        FR[0][p, 8:72, 0:64] = jnp.where(m64, b, a)
        FB[0][p, 8:72, 0:64] = jnp.where(m64, a, b)

    def faces_of(p):
        for side, (rb, rr, rk) in enumerate(((8, 8, 6), (69, 70, 69))):
            t = turn(jnp.where(third_row, FB[0][p, rk : rk + 8, :], FR[0][p, rr : rr + 8, :]), 64)
            ys[side][p - 3] = jnp.where(lane < 64, B[0][p, rb : rb + 8, :], t)
        t = pick(at_fb, turn(FB[0][p, 8:72, :], 5), B[0][p, 8:72, :])
        T[p, 8:72, :] = pick(at_fr, turn(FR[0][p, 8:72, :], 3), t)

    def pack_faces(get, out, count, low, high, width, apart, start=0):
        for i0 in range(start, start + count, 16):
            half = i0 % 16
            lo = hi = None
            for i in range(i0, min(i0 + 16 - half, start + count)):
                j = i % 16
                t = get(i)
                a = turn(t, 8 * j)
                b = turn(t, 8 * j + apart) if apart else a
                if lo is None:
                    lo, hi = a, b
                else:
                    lo = pick(within(low + 8 * j, width), a, lo)
                    hi = pick(within(high + apart + 8 * j, width), b, hi)
            if half:
                lo = pick(within(low + 64, 64), lo, out[0][i0 // 16])
                hi = pick(within(high + apart + 64, 64), hi, out[1][i0 // 16])
            out[0][i0 // 16] = lo
            out[1][i0 // 16] = hi

    for c in range(2):
        for copy in fetch(c):
            copy.wait()
        for p in range(3 + 16 * c, 19 + 16 * c):
            apart(p)
        for p in range(3 + 16 * c, 19 + 16 * c):
            faces_of(p)
        pack_faces(lambda i: T[3 + i, 8:72, :], zs["f"], 16, 0, 61, 8, 0, 16 * c)
    for side, (near, next_) in enumerate(((3, 4), (34, 33))):
        for k, (a, other) in enumerate(((near, FR[0]), (next_, FB[0]))):
            xs[side][k] = pick(lane < 64, B[0][a, 8:72, :], turn(other[near, 8:72, :], 64))
    pl.semaphore_wait(barrier, rooms[0] * rooms[1] * rooms[2] - 1)

    at_edge = [(at == 0) | (at == SIDE - 1) for at in me]

    def halo(key, directions, pieces):
        k = PHASES.index(key)
        total = dict.fromkeys(EDGES, 0)
        for d in directions:
            copies = pieces(d)

            @pl.when(inside(d, me))
            def _(d=d, copies=copies):
                device = tuple(at + step for at, step in zip(me, d))
                for src, dst, _ in copies:
                    pltpu.make_async_remote_copy(
                        src, dst, send_sem.at[k], recv_sem.at[k], device_id=device, device_id_type=MESH
                    ).start()

            for edge in total:
                if not any(e and step > 0 for e, step in zip(edge, d)):
                    total[edge] += sum(rows for _, _, rows in copies)
        return k, total

    def both(a, b):
        return a[0], {edge: a[1][edge] + b[1][edge] for edge in EDGES}

    def sides(arrays, oy, n):
        def pieces(d):
            out = []
            for src, ps, dst, pd, own, hp, hr in arrays:
                s0, d0, w = {-1: (ps, pd + own, hp), 0: (ps, pd, own), 1: (ps + own - hp, pd - hp, hp)}[d[0]]
                rs, rd, rw = {-1: (0, oy + n, hr), 0: (0, oy, n), 1: (n - hr, oy - hr, hr)}[d[1]]
                rs = rs + (oy if src.shape[1] > n else 0)
                out.append((src.at[pl.ds(s0, w), pl.ds(rs, rw), :], dst.at[pl.ds(d0, w), pl.ds(rd, rw), :], w * rw))
            return out

        return pieces

    def faces(key, oy, n, hz):
        groups = zs[key][0].shape[0]

        def pieces(d):
            s0, d0, w = {-1: (0, groups + 1, 1), 0: (0, 1, groups), 1: (groups - 1, 0, 1)}[d[0]]
            rs, rd, rw = {-1: (0, oy + n, hz), 0: (0, oy, n), 1: (n - hz, oy - hz, hz)}[d[1]]
            src, dst = (zs[key][0], zr[key][1]) if d[2] < 0 else (zs[key][1], zr[key][0])
            return [(src.at[pl.ds(s0, w), pl.ds(rs, rw), :], dst.at[pl.ds(d0, w), pl.ds(rd, rw), :], w * rw)]

        return pieces

    def exchange(key, arrays, oy, n, hz):
        packed = halo(key, ACROSS, faces(key, oy, n, hz))
        return both(packed, halo(key, FLAT, sides(arrays, oy, n)))

    def settle(what, arrived, left):
        k, total = what
        other = tuple(jnp.where(at == 0, at + 1, at - 1) for at in me)
        for edge, rows in total.items():
            same = None
            for e, here in zip(edge, at_edge):
                t = here if e else jnp.logical_not(here)
                same = t if same is None else same & t

            @pl.when(same)
            def _(rows=rows):
                cut = tally.at[pl.ds(0, rows), :]
                copy = pltpu.make_async_remote_copy(cut, cut, send_sem.at[k], recv_sem.at[k], device_id=other, device_id_type=MESH)
                if arrived:
                    copy.wait_recv()
                if left:
                    copy.wait_send()

    def first_sides(d):
        side = 0 if d[0] < 0 else 1
        rs, rd, rw = {-1: (0, 72, 3), 0: (0, 8, 64), 1: (61, 5, 3)}[d[1]]
        return [(xs[side].at[:, pl.ds(rs, rw), :], xr[1 - side].at[:, pl.ds(rd, rw), :], 2 * rw)]

    def first_rows(d):
        side = 0 if d[1] < 0 else 1
        return [(ys[side].at[:, pl.ds(0, 3), :], yr[1 - side].at[:, pl.ds(0, 3), :], 96)]

    first = halo("f", ACROSS, faces("f", 8, 64, 3))
    first = both(first, halo("f", FLAT, lambda d: first_sides(d) if d[0] else first_rows(d)))
    def outside(ref, po, own, hp, oy, n, hr):
        planes, rows = ref.shape[0], ref.shape[1]
        for cond, cut in (
            (gx == 0, (slice(po - hp, po), slice(0, rows))),
            (gx == SIDE - 1, (slice(po + own, po + own + hp), slice(0, rows))),
            (gy == 0, (slice(0, planes), slice(oy - hr, oy))),
            (gy == SIDE - 1, (slice(0, planes), slice(oy + n, oy + n + hr))),
        ):

            @pl.when(cond)
            def _(cut=cut):
                shape = (cut[1].stop - cut[1].start, 128)
                for p in range(cut[0].start, cut[0].stop):
                    ref[p, cut[1], :] = jnp.zeros(shape, F32)

    def outside_z(key):
        for side, cond in ((0, gz == 0), (1, gz == SIDE - 1)):

            @pl.when(cond)
            def _(side=side):
                ref = zr[key][side]
                ref[...] = jnp.zeros(ref.shape, F32)

    def edges_z(key, po, n, hz, oy, groups):
        for side in (0, 1):
            ref = zr[key][side]
            rows = ref.shape[1]
            for cond, cut in (
                (gx == 0, (0, 1, 0, rows)),
                (gx == SIDE - 1, (groups + 1, 1, 0, rows)),
                (gy == 0, (0, groups + 2, oy - hz, hz)),
                (gy == SIDE - 1, (0, groups + 2, oy + n, hz)),
            ):

                @pl.when(cond)
                def _(cut=cut, ref=ref):
                    ref[pl.ds(cut[0], cut[1]), pl.ds(cut[2], cut[3]), :] = jnp.zeros((cut[1], cut[3], 128), F32)

    outside(H, 3, 32, 2, 8, 64, 3)
    for i in range(2):
        for cond, refs0 in ((gx == (0, SIDE - 1)[i], (xr[i],)), (gy == (0, SIDE - 1)[i], (yr[i],))):

            @pl.when(cond)
            def _(refs0=refs0):
                for ref in refs0:
                    ref[...] = jnp.zeros(ref.shape, F32)

        @pl.when(gy == (0, SIDE - 1)[i])
        def _(i=i):
            for ref in xr:
                for k in range(2):
                    ref[k, pl.ds((5, 72)[i], 3), :] = jnp.zeros((3, 128), F32)

    for key, n, oy, groups, hz in (("f", 64, 8, 2, 3), ("v", 64, 8, 2, 3), (1, 32, 16, 2, 6), (2, 16, 16, 1, 7)):
        outside_z(key)
        edges_z(key, 3, n, hz, oy, groups)
    outside(PR[1], 2, 8, 2, 16, 32, 8)
    outside(PR[2], 1, 2, 1, 16, 16, 8)
    for dx, dy in itertools.product((-1, 0, 1), repeat=2):
        if (dx, dy) != (0, 0):

            @pl.when(jnp.logical_not(inside((dx, dy, 0), me)))
            def _(dx=dx, dy=dy):
                Z3[dx + 1, dy + 1] = jnp.zeros((4 * SIDE, 128), F32)

    for l in (4, 5, 6):
        R[l][...] = jnp.zeros(LEV[l].shape(), F32)
        B[l][...] = jnp.zeros(LEV[l].shape(), F32)
    for l in (4, 5):
        EX[l][...] = jnp.zeros(EX[l].shape, F32)

    def tables(l):
        lv = LEV[l]
        shape = (lv.nr, 128)
        row, lane = iota(shape, 0) + lv.r0, iota(shape, 1)
        y = row - lv.oy
        z = jnp.where(lane < 100, lane, lane - 128)
        if l < 4:
            y = y + gy * lv.n
        if l < 3:
            z = z + gz * lv.n
        last = lv.total - 1
        within = (y >= 0) & (y <= last) & (z >= 0) & (z <= last)
        one = lambda c: jnp.where(c, 1, 0)
        w = one(y == 0) + one(y == last) + one(z == 0) + one(z == last)
        high = one(((row + lane) & 1) == 1)
        for kind, colour in itertools.product(range(3), range(2)):
            a = high if colour == 0 else 1 - high
            d = w if kind == 0 else (w + 1 - a if kind == 1 else w + a)
            inv = jnp.where(d == 0, 1 / 6, jnp.where(d == 1, 1 / 7, jnp.where(d == 2, 1 / 8, 1 / 9)))
            C[l][kind, colour] = jnp.where(within, inv, 0.0)
            D[l][kind, colour] = 6.0 + d.astype(F32)
            if colour == 1 and l < 6:
                q = jnp.where(within, 0.25, 0.0)
                Q[l][kind] = q
                A[l][kind] = (1.0 - d.astype(F32)) * q
        for colour in range(2):
            C[l][3, colour] = jnp.zeros(shape, F32)
            D[l][3, colour] = jnp.full(shape, 6.0, F32)
        if l < 6:
            Q[l][3] = jnp.zeros(shape, F32)
            A[l][3] = jnp.zeros(shape, F32)

    for l in range(7):
        tables(l)

    def kind(l, p):
        lv = LEV[l]
        x = 2 * (p - lv.po) + (gx * lv.n if l < 4 else 0)
        if l >= 4:
            return jnp.where(x == 0, 1, jnp.where(x == lv.total - 2, 2, 0))
        return jnp.where(x == 0, 1, jnp.where(x == lv.total - 2, 2, jnp.where((x < 0) | (x >= lv.total), 3, 0)))

    settle(first, True, True)
    tokens(0, 2, True)

    def slot_of(i, n):
        groups = n // 16
        if i < 0:
            return 0, 16 + i
        if i >= n:
            return groups + 1, i - n
        return 1 + i // 16, i % 16

    def unpack_first(i):
        g, j = slot_of(i, 32)
        low, high = zr["f"][0][g, 4:76, :], zr["f"][1][g, 4:76, :]
        for ref, at, width, shift in ((B[0], 0, 3, 64), (FR[0], 3, 2, 61), (FB[0], 5, 1, 59)):
            w = turn(pick(within(8 * j + at, width), high, low), shift - 8 * j)
            ref[3 + i, 4:76, :] = pick(lane < 64, ref[3 + i, 4:76, :], w)

    for side, (near, next_) in enumerate(((2, 1), (35, 36))):
        rows = pl.ds(4, 72)
        a, b = xr[side][0, rows, :], xr[side][1, rows, :]
        B[0][near, rows, :] = a
        B[0][next_, rows, :] = b
        FR[0][near, rows, :] = turn(a, 64)
        FB[0][near, rows, :] = turn(b, 64)
    for i in range(32):
        for side, (rb, rr, rk) in enumerate(((5, 6, 7), (72, 72, 72))):
            t = yr[side][i]
            f = turn(t, 64)
            B[0][3 + i, rb : rb + 3, :] = t[0:3]
            FR[0][3 + i, rr : rr + 2, :] = f[0:2]
            FB[0][3 + i, rk : rk + 1, :] = f[2:3]
    for i in range(-2, 34):
        unpack_first(i)

    def red_sweep(l):
        lv = LEV[l]
        p0, count, r0, nr = RED[l]
        rows, table = pl.ds(r0, nr), pl.ds(r0 - lv.r0, nr)

        def body(p):
            R[l][p, rows, :] = (FR[l][p, rows, :] + around(B[l], p, r0, nr, m)) * C[l][kind(l, p), 0, table, :]

        sweep_loop(p0, count, 36, body)

    def black_sweep(l, region, keep):
        lv = LEV[l]
        p0, count, r0, nr = region[l]
        rows, table = pl.ds(r0, nr), pl.ds(r0 - lv.r0, nr)

        def body(p):
            t = kind(l, p)
            fs = FB[l][p, rows, :] + around(R[l], p, r0, nr, not_m)
            b = fs * C[l][t, 1, table, :]
            B[l][p, rows, :] = b
            if keep:
                T[p, rows, :] = fs - D[l][t, 1, table, :] * b

        sweep_loop(p0, count, 36, body)

    def red_residual(l, p):
        lv = LEV[l]
        s = around(B[l], p, lv.oy, lv.n, m)
        at = lv.oy - lv.r0
        return FR[l][p, pl.ds(lv.oy, lv.n), :] + s - D[l][kind(l, p), 0, pl.ds(at, lv.n), :] * R[l][p, pl.ds(lv.oy, lv.n), :]

    def residual(l):
        lv = LEV[l]

        def body(p):
            T[p, pl.ds(lv.oy, lv.n), :] = T[p, pl.ds(lv.oy, lv.n), :] + red_residual(l, p)

        sweep_loop(lv.po, lv.n // 2, 32, body)

    def coarse_side(l, p):
        lv = LEV[l]
        half = lv.n // 2
        u = T[p, pl.ds(lv.oy, half, stride=2), :] + T[p, pl.ds(lv.oy + 1, half, stride=2), :]
        z = 2 * lane_index(half)
        return 0.5 * (take(u, z & 127) + take(u, (z + 1) & 127))

    red_sweep(0)
    black_sweep(0, BLACK_DOWN, True)

    def restrict_to(l, dst, first_plane, first_row):
        lv = LEV[l]

        def body(p):
            dst[p - lv.po + first_plane, pl.ds(first_row, lv.n // 2), :] = coarse_side(l, p)

        sweep_loop(lv.po, lv.n // 2, 32, body)

    residual(0)
    restrict_to(0, G[1], 0, 0)

    def send_right_side(l):
        n, w = LEV[l].n, WIDTH[l]
        per = 128 // n
        for q in range(n // per):
            t = G[l][per * q]
            for j in range(1, per):
                t = pick(within(n * j, n), turn(G[l][per * q + j], n * j), t)
            PS[l][q] = t
        pack_faces(lambda i: G[l][i], zs[l], n, 0, n - 8, 8, 128 - 2 * n)
        wide = 8 // per
        return exchange(l, [(PS[l], 0, PR[l], wide, n // per, wide, w)], 16, n, w)

    def split_right_side(l):
        lv = LEV[l]
        n = lv.n
        per = 128 // n

        def natural(i):
            g, j = slot_of(i, n)
            rows = pl.ds(lv.r0, lv.nr)
            side = pick(within(8 * j, 8), zr[l][1][g, rows, :], zr[l][0][g, rows, :])
            q, k = (i + 8) // per, (i + 8) % per
            if 0 <= i < n:
                below, above = (turn(PR[l][q, pl.ds(r, 8), :], -n * k) for r in (8, 16 + n))
                here = jnp.concatenate([below, G[l][i], above], axis=0)
            else:
                here = turn(PR[l][q, rows, :], -n * k)
            return pick(lane < n, here, turn(side, n - 8 * j))

        for p in range(lv.p0, lv.p0 + lv.np):
            a, b = natural(2 * (p - lv.po)), natural(2 * (p - lv.po) + 1)
            store_colours(l, p, a, b)

    def store_colours(l, p, a, b):
        lv = LEV[l]
        rows = pl.ds(lv.r0, lv.nr)
        red = pick(m, b, a)
        FR[l][p, rows, :] = red
        FB[l][p, rows, :] = pick(m, a, b)
        R[l][p, rows, :] = red * C[l][kind(l, p), 0]

    second = send_right_side(1)
    def keep_black(p):
        H[p, 8:72, :] = B[0][p, 8:72, :]

    sweep_loop(3, 32, 8, keep_black)

    tokens(0, 2, False)
    tokens(1, 4, True)
    settle(second, True, False)
    split_right_side(1)
    black_sweep(1, BLACK_DOWN, True)
    residual(1)
    restrict_to(1, G[2], 0, 0)
    third = send_right_side(2)
    pack_faces(lambda i: B[0][3 + i, 8:72, :], zs["v"], 32, 0, 61, 3, 0)
    kept = exchange("v", [(B[0], 3, H, 3, 32, 2, 3)], 8, 64, 3)
    settle(third, True, False)
    split_right_side(2)
    black_sweep(2, BLACK_DOWN, True)
    residual(2)

    own3 = None
    for i in range(8):
        g = jnp.where(lane < 8, coarse_side(2, LEV[2].po + i), 0.0)
        g = pltpu.roll(g, 8 * lax.rem(gz + i, 8), axis=1)
        own3 = g if own3 is None else own3 + g
    pack3[0:8, :] = own3
    own3 = jnp.where(lane[0:4] < 64, pack3[0:4, :], turn(pack3[4:8, :], 64))
    pack3[8:12, :] = own3
    Z3[1, 1, pl.ds(4 * gz, 4), :] = own3
    tokens(1, 4, False)

    k3 = PHASES.index("3")
    for dx, dy in sorted(itertools.product((-1, 0, 1), repeat=2), key=lambda d: -abs(d[0]) - abs(d[1])):

        @pl.when(inside((dx, dy, 0), me))
        def _(dx=dx, dy=dy):
            for far in (4, 3, 5, 2, 6, 1, 7, 0):
                if (dx, dy, far) != (0, 0, 0):
                    pltpu.make_async_remote_copy(
                        pack3.at[pl.ds(8, 4), :],
                        Z3.at[1 - dx, 1 - dy, pl.ds(4 * gz, 4), :],
                        send_sem.at[k3],
                        recv_sem.at[k3],
                        device_id=(gx + dx, gy + dy, (gz + far) & (SIDE - 1)),
                        device_id_type=MESH,
                    ).start()

    blocks = {edge: 4 * ((2 if edge[0] else 3) * (2 if edge[1] else 3) * SIDE - 1) for edge in EDGES}
    settle((k3, blocks), True, False)

    for p in range(1, 13):
        ab = []
        for i in (2 * (p - 1), 2 * (p - 1) + 1):
            x = i % 8
            tiles = []
            for cy in range(3):
                t = None
                for k in range(SIDE):
                    block = Z3[i // 8, cy, 4 * k : 4 * k + 4, :]
                    s = 8 * ((x + k) % 8)
                    t = block if t is None else jnp.where((within(s, 8) | within(s + 64, 8))[0:4], block, t)
                other = turn(t, 64)
                low = lane[0:4] < 64
                t = jnp.concatenate([jnp.where(low, t, other), jnp.where(low, other, t)], axis=0)
                tiles.append(turn(t, -8 * x))
            ab.append(jnp.concatenate(tiles, axis=0))
        store_colours(3, p, ab[0], ab[1])
    black_sweep(3, BLACK_DOWN, True)

    residual(3)
    own4 = None
    for i in range(4):
        g = turn(pick(lane < 32, coarse_side(3, LEV[3].po + i), jnp.zeros((4, 128), F32)), 32 * i)
        own4 = g if own4 is None else own4 + g
    pack4[0:4, :] = own4
    G4[gx, pl.ds(4 * gy, 4), :] = own4

    k4 = PHASES.index("4")

    ring = lambda k: min(k, SIDE - k)
    for dx, dy in sorted(itertools.product(range(SIDE), repeat=2), key=lambda d: -ring(d[0]) - ring(d[1])):
        if (dx, dy) != (0, 0):
            pltpu.make_async_remote_copy(
                pack4.at[pl.ds(0, 4), :],
                G4.at[gx, pl.ds(4 * gy, 4), :],
                send_sem.at[k4],
                recv_sem.at[k4],
                device_id=((gx + dx) & (SIDE - 1), (gy + dy) & (SIDE - 1), gz),
                device_id_type=MESH,
            ).start()
    plane = (k4, dict.fromkeys(EDGES, 4 * (SIDE * SIDE - 1)))
    settle(kept, True, True)
    for i in range(-2, 34):
        g, j = slot_of(i, 32)
        w = turn(pick(within(8 * j, 3), zr["v"][1][g, 4:76, :], zr["v"][0][g, 4:76, :]), 64 - 8 * j)
        H[3 + i, 4:76, :] = pick(lane < 64, H[3 + i, 4:76, :], w)
    settle(plane, True, False)
    for x in range(SIDE):
        parts = [turn(G4[x], -32 * i) for i in range(4)]
        store_colours(4, 4 + 2 * x, parts[0], parts[1])
        store_colours(4, 5 + 2 * x, parts[2], parts[3])
    for l in (4, 5):
        black_sweep(l, BLACK_DOWN, True)
        residual(l)
        restrict_to(l, N[l + 1], 0, 0)
        lv = LEV[l + 1]
        for p in range(lv.p0, lv.p0 + lv.np):
            store_colours(l + 1, p, N[l + 1][2 * (p - 1)], N[l + 1][2 * (p - 1) + 1])
    black_sweep(6, BLACK_UP, False)
    for _ in range(COARSE_SWEEPS - 1):
        red_sweep(6)
        black_sweep(6, BLACK_UP, False)

    def expand(l):
        lf, lc = LEV[l], LEV[l + 1]
        c0, cn, r0, rn = GIVE[l]
        fine0 = lf.oy + 2 * (r0 - lc.oy)
        if l == 3:
            c0, r0 = 2 * gx + 1, 4 * gy + 4
            fine0 = 8
        zf = lane_index(rn)
        z = (jnp.where(zf < 100, zf, zf - 128) >> 1) + (8 * gz if l == 2 else 0)
        at, beside = z & 127, (z + 2 * (zf & 1) - 1) & 127

        def body(i):
            rows = pl.ds(r0, rn)
            r, b = R[l + 1][c0 + i, rows, :], B[l + 1][c0 + i, rows, :]
            if rn % 8:
                mm = ((iota((rn, 128), 0) + iota((rn, 128), 1)) & 1) == 1
                both = jnp.where(mm, b, r), jnp.where(mm, r, b)
            else:
                both = pick(m, b, r), pick(m, r, b)
            for a, e in enumerate(both):
                here, there = take(e, at), take(e, beside)
                for k in (0, 1):
                    EX[l][2 * i + a, pl.ds(fine0 + k, rn, stride=2), :] = here
                    EZ[l][2 * i + a, pl.ds(fine0 + k, rn, stride=2), :] = there

        sweep_loop(0, cn, 20, body)

    def correct(l):
        lv = LEV[l]
        second_row = (iota((8, 128), 0) & 1) == 1
        p0, count, r0, nr = CORRECTED[l]
        rows, table = pl.ds(r0, nr), pl.ds(r0 - lv.r0, nr)

        def body(p):
            e = p - EDGE[l]
            t = kind(l, p)
            sides = pick(m, EX[l][e - 1, rows, :], EX[l][e + 1, rows, :])
            sides = sides + pick(second_row, EX[l][e, pl.ds(r0 + 1, nr), :], EX[l][e, pl.ds(r0 - 1, nr), :])
            add = EX[l][e, rows, :] * A[l][t, table, :] + (EZ[l][e, rows, :] + sides) * Q[l][t, table, :]
            return add

        start = B[l] if l else H

        def plain(p):
            B[l][p, rows, :] = start[p, rows, :] + body(p)

        sweep_loop(p0, count, 36, plain)

    for l in (5, 4):
        expand(l)
        correct(l)
        red_sweep(l)
        black_sweep(l, BLACK_UP, False)
    expand(3)
    correct(3)
    red_sweep(3)
    black_sweep(3, BLACK_UP, False)
    expand(2)
    correct(2)
    red_sweep(2)
    black_sweep(2, BLACK_UP, False)
    expand(1)
    correct(1)
    red_sweep(1)
    black_sweep(1, BLACK_UP, False)
    expand(0)
    correct(0)
    red_sweep(0)
    for what in (second, third, (k3, blocks), plane):
        settle(what, False, True)


def results(R, FR, FB, C, D, u_hbm, r_hbm, B, T, u_out, r_out, sem):
    lv = LEV[0]
    m = odd()
    not_m = jnp.logical_not(m)

    def kind(p):
        x = lax.axis_index("gx") * lv.n + 2 * (p - lv.po)
        return jnp.where(x == 0, 1, jnp.where(x == lv.total - 2, 2, jnp.where((x < 0) | (x >= lv.total), 3, 0)))

    def black(p):
        t = kind(p)
        fs = FB[p, 4:76, :] + around(R, p, 4, 72, not_m)
        b = fs * C[t, 1]
        B[p, 4:76, :] = b
        T[p, 4:76, :] = fs - D[t, 1] * b

    def finish(p):
        x = 2 * (p - lv.po)
        r, b = R[p, 8:72, :], B[p, 8:72, :]
        u_out[x] = pick(m, b, r)[:, 0:64]
        u_out[x + 1] = pick(m, r, b)[:, 0:64]
        left = FR[p, 8:72, :] + around(B, p, lv.oy, lv.n, m) - D[kind(p), 0, 4:68, :] * r
        b = T[p, 8:72, :]
        r_out[x] = pick(m, b, left)[:, 0:64]
        r_out[x + 1] = pick(m, left, b)[:, 0:64]

    done, first, copies = 2, 3, []
    for part in PARTS:
        ready = min(first + part + (PARTS[0] if first == 3 else part), 35)
        for p in range(done, ready + 1):
            black(p)
        done = ready + 1
        for p in range(first, first + part):
            finish(p)
        cut = pl.ds(2 * (first - 3), 2 * part)
        for src, dst in ((u_out, u_hbm), (r_out, r_hbm)):
            copy = pltpu.make_async_copy(src.at[cut], dst.at[cut], sem.at[len(copies)])
            copy.start()
            copies.append(copy)
        first += part
    for copy in copies:
        copy.wait()


PARTS = (4, 4, 4, 4, 4, 4, 4, 4)
EDGES = tuple(itertools.product((False, True), repeat=3))
AROUND = sorted((d for d in itertools.product((-1, 0, 1), repeat=3) if any(d)), key=lambda d: -sum(map(abs, d)))
FLAT = [d for d in AROUND if d[2] == 0]
ACROSS = [d for d in AROUND if d[2]]
EDGE = {0: -1, 1: -1, 2: -1, 3: -1, 4: 2, 5: -1}


def inside(d, me, far=1):
    ok = None
    for step, at in zip(d, me):
        if step:
            here = (at >= far) if step < 0 else (at < SIDE - far)
            ok = here if ok is None else ok & here
    return True if ok is None else ok


def vmem(*shape):
    return pltpu.VMEM(shape, F32)


def per_device(right_side, guess):
    whole = vmem(64, 64, 64)
    scratch = [whole, whole]
    scratch += [vmem(*lv.shape()) for lv in LEV[1:]]
    scratch += [vmem(*lv.shape()) for lv in LEV]
    for _ in range(2):
        scratch += [vmem(*lv.shape()) for lv in LEV[1:]]
    for _ in range(2):
        scratch += [vmem(4, 2, lv.nr, 128) for lv in LEV[1:]]
    for _ in range(2):
        scratch += [vmem(4, lv.nr, 128) for lv in LEV[:6]]
    for _ in range(2):
        scratch += [vmem(2 * GIVE[l][1], LEV[l].rows, 128) for l in range(6)]
    scratch += [vmem(*LEV[0].shape())] * 2
    scratch += [vmem(2, 64, 128)] * 2 + [vmem(2, 80, 128)] * 2 + [vmem(32, 8, 128)] * 4
    scratch += [vmem(32, 32, 128), vmem(16, 16, 128)]
    scratch += [vmem(8, 32, 128), vmem(2, 16, 128), vmem(12, 64, 128), vmem(4, 48, 128)]
    scratch += [vmem(16, 16, 128), vmem(8, 8, 128)]
    packed = ((2, 64, 80), (2, 64, 80), (2, 32, 64), (1, 16, 48))
    for groups, n, _ in packed:
        scratch += [vmem(groups, n, 128)] * 2
    for groups, _, rows in packed:
        scratch += [vmem(groups + 2, rows, 128)] * 2
    scratch += [vmem(16, 128), vmem(3, 3, 32, 128), vmem(8, 128), vmem(8, 32, 128), vmem(2048, 128)]
    dma = pltpu.SemaphoreType.DMA((len(PHASES),))
    scratch += [dma, dma, pltpu.SemaphoreType.DMA((8,)), pltpu.SemaphoreType.REGULAR((2,))]
    level0, table = pltpu.VMEM(LEV[0].shape(), F32), pltpu.VMEM((4, 2, LEV[0].nr, 128), F32)
    parts = pl.pallas_call(
        kernel,
        out_shape=(level0,) * 3 + (table, table),
        in_specs=[pl.BlockSpec(memory_space=pl.ANY)] * 2,
        out_specs=(pl.BlockSpec(memory_space=pltpu.VMEM),) * 5,
        scratch_shapes=scratch,
        compiler_params=pltpu.CompilerParams(collective_id=0, has_side_effects=True, vmem_limit_bytes=48 * 2**20),
    )(right_side, guess)
    block = jax.ShapeDtypeStruct(right_side.shape, F32)
    return pl.pallas_call(
        results,
        out_shape=(block, block),
        in_specs=[pl.BlockSpec(memory_space=pltpu.VMEM)] * 5,
        out_specs=(pl.BlockSpec(memory_space=pl.ANY),) * 2,
        scratch_shapes=[vmem(*LEV[0].shape())] * 2 + [vmem(64, 64, 64)] * 2 + [pltpu.SemaphoreType.DMA((2 * len(PARTS),))],
        compiler_params=pltpu.CompilerParams(vmem_limit_bytes=12 * 2**20),
    )(*parts)


def solution(mesh):
    spec = P("gx", "gy", "gz")
    return jax.shard_map(per_device, mesh=mesh, in_specs=(spec, spec), out_specs=(spec, spec), check_vma=False)
```

```python
import itertools

import jax
import jax.numpy as jnp
from jax import lax
from jax.experimental import pallas as pl
from jax.experimental.pallas import tpu as pltpu
from jax.sharding import PartitionSpec as P

COARSE_SWEEPS = 4
MESH = pl.DeviceIdType.MESH
SIDE = 8
F32 = jnp.float32


class Level:
    def __init__(self, n, total, po, oy, p0, np_, r0, nr, pairs, rows, whole_z):
        self.n, self.total, self.po, self.oy = n, total, po, oy
        self.p0, self.np, self.r0, self.nr = p0, np_, r0, nr
        self.pairs, self.rows, self.whole_z = pairs, rows, whole_z

    def shape(self):
        return (self.pairs, self.rows, 128)


LEV = [
    Level(64, 512, 3, 8, 1, 36, 4, 72, 38, 80, False),
    Level(32, 256, 5, 16, 1, 24, 8, 48, 26, 64, False),
    Level(16, 128, 5, 16, 1, 16, 8, 32, 18, 48, False),
    Level(8, 64, 5, 16, 1, 12, 8, 24, 14, 40, True),
    Level(32, 32, 4, 8, 4, 16, 8, 32, 24, 48, True),
    Level(16, 16, 1, 8, 1, 8, 8, 16, 10, 32, True),
    Level(8, 8, 1, 8, 1, 4, 8, 8, 6, 24, True),
]
GIVE = {0: (3, 20, 12, 40), 1: (2, 14, 12, 24), 2: (2, 10, 12, 16), 3: (0, 8, 0, 12), 4: (0, 10, 8, 16), 5: (0, 6, 8, 8)}
ALL = {4: (4, 16, 8, 32), 5: (1, 8, 8, 16), 6: (1, 4, 8, 8)}
RED = {0: (2, 34, 4, 72), 1: (3, 20, 12, 40), 2: (2, 14, 8, 32), 3: (2, 10, 8, 24), **ALL}
BLACK_DOWN = {0: (2, 34, 4, 72), 1: (2, 22, 8, 48), 2: (2, 14, 8, 32), 3: (2, 10, 8, 24), **ALL}
BLACK_UP = {1: (3, 20, 12, 40), 2: (3, 12, 12, 24), 3: (3, 8, 12, 16), **ALL}
CORRECTED = {0: (1, 36, 4, 72), 1: (2, 22, 8, 48), 2: (2, 14, 8, 32), 3: (2, 10, 8, 24), **ALL}
PHASES = ("f", "v", 1, 2, "3", "4", "fz", "1z", "2z")
BESIDE = [(0, 0, -1), (0, 0, 1)]
WIDTH = {1: 6, 2: 7}


def iota(shape, axis):
    return lax.broadcasted_iota(jnp.int32, shape, axis)


def odd():
    return ((iota((8, 128), 0) + iota((8, 128), 1)) & 1) == 1


def lanes():
    return iota((8, 128), 1)


def pick(mask, a, b):
    shape = a.shape
    if shape[0] <= 8:
        return jnp.where(mask[: shape[0]], a, b)
    tiles = (shape[0] // 8, 8, 128)
    return jnp.where(mask[None], a.reshape(tiles), b.reshape(tiles)).reshape(shape)


def within(start, width):
    return ((lanes() - start) & 127) < width


def turn(a, shift):
    return pltpu.roll(a, shift % 128, axis=1) if shift % 128 else a


def take(a, index):
    return jnp.take_along_axis(a, index, axis=1, mode="promise_in_bounds")


def lane_index(rows):
    return iota((rows, 128), 1)


def sweep_loop(start, count, step, body):
    step = max(k for k in range(1, step + 1) if count % k == 0)
    if count == step:
        for i in range(count):
            body(start + i)
        return

    def some(j, carry):
        for i in range(step):
            body(start + j * step + i)
        return carry

    lax.fori_loop(0, count // step, some, 0)


def around(src, p, r0, nr, up):
    here = src[p, pl.ds(r0, nr), :]
    side = pick(up, src[p + 1, pl.ds(r0, nr), :], src[p - 1, pl.ds(r0, nr), :])
    rows = src[p, pl.ds(r0 - 1, nr), :] + src[p, pl.ds(r0 + 1, nr), :]
    return (here + side) + rows + (pltpu.roll(here, 1, axis=1) + pltpu.roll(here, 127, axis=1))


def kernel(*refs):
    it = iter(refs)
    f_hbm, u_hbm, R0, FR0, FB0, C0, D0 = (next(it) for _ in range(7))
    f_in, u_in = next(it), next(it)
    R = [R0] + [next(it) for _ in range(6)]
    B = [next(it) for _ in range(7)]
    FR = [FR0] + [next(it) for _ in range(6)]
    FB = [FB0] + [next(it) for _ in range(6)]
    C = [C0] + [next(it) for _ in range(6)]
    D = [D0] + [next(it) for _ in range(6)]
    A = [next(it) for _ in range(6)]
    Q = [next(it) for _ in range(6)]
    EX = [next(it) for _ in range(6)]
    EZ = [next(it) for _ in range(6)]
    T, H = next(it), next(it)
    xs, xr = (next(it), next(it)), (next(it), next(it))
    ys, yr = (next(it), next(it)), (next(it), next(it))
    G = {1: next(it), 2: next(it)}
    PS = {1: next(it), 2: next(it)}
    PR = {1: next(it), 2: next(it)}
    N = {5: next(it), 6: next(it)}
    zs = {k: (next(it), next(it)) for k in ("f", "v", 1, 2)}
    zr = {k: (next(it), next(it)) for k in ("f", "v", 1, 2)}
    pack3, Z3, pack4, G4, tally = (next(it) for _ in range(5))
    send_sem, recv_sem, in_sem, token = (next(it) for _ in range(4))

    gx, gy, gz = lax.axis_index("gx"), lax.axis_index("gy"), lax.axis_index("gz")
    me = (gx, gy, gz)

    def fetch(c):
        cut = pl.ds(2 * FETCHED[c], 2 * (FETCHED[c + 1] - FETCHED[c]))
        return [
            pltpu.make_async_copy(src.at[cut], dst.at[cut], in_sem.at[2 * c + i])
            for i, (src, dst) in enumerate(((u_hbm, u_in), (f_hbm, f_in)))
        ]

    for c in range(len(FETCHED) - 1):
        for copy in fetch(c):
            copy.start()

    barrier = pltpu.get_barrier_semaphore()
    rooms = [jnp.where((at > 0) & (at < SIDE - 1), 3, 2) for at in me]
    for d in itertools.product((-1, 0, 1), repeat=3):
        if d != (0, 0, 0):

            @pl.when(inside(d, me))
            def _(d=d):
                pl.semaphore_signal(barrier, inc=1, device_id=tuple(at + step for at, step in zip(me, d)), device_id_type=MESH)

    def tokens(k, far, act):
        count = jnp.int32(0)
        for d in itertools.product((-1, 0, 1), repeat=3):
            if d == (0, 0, 0) or (d[2] and (d[0] or d[1])):
                continue
            there = inside(d, me, far)
            count = count + jnp.where(there, 1, 0)
            if act:

                @pl.when(there)
                def _(d=d):
                    device = tuple(at + far * step for at, step in zip(me, d))
                    pl.semaphore_signal(token.at[k], inc=1, device_id=device, device_id_type=MESH)

        if not act:
            pl.semaphore_wait(token.at[k], count)

    lv = LEV[0]
    m64 = ((iota((64, 64), 0) + iota((64, 64), 1)) & 1) == 1
    lane, m = lanes(), odd()
    not_m = jnp.logical_not(m)
    at_fb = within(5, 1) | within(68, 1)
    at_fr = within(3, 2) | within(65, 2)
    third_row = iota((8, 128), 0) == 2

    def apart(p):
        a, b = u_in[2 * (p - lv.po)], u_in[2 * (p - lv.po) + 1]
        B[0][p, 8:72, 0:64] = jnp.where(m64, a, b)
        a, b = f_in[2 * (p - lv.po)], f_in[2 * (p - lv.po) + 1]
        FR[0][p, 8:72, 0:64] = jnp.where(m64, b, a)
        FB[0][p, 8:72, 0:64] = jnp.where(m64, a, b)

    def faces_of(p):
        for side, (rb, rr, rk) in enumerate(((8, 8, 6), (69, 70, 69))):
            t = turn(jnp.where(third_row, FB[0][p, rk : rk + 8, :], FR[0][p, rr : rr + 8, :]), 64)
            ys[side][p - 3] = jnp.where(lane < 64, B[0][p, rb : rb + 8, :], t)
        t = pick(at_fb, turn(FB[0][p, 8:72, :], 5), B[0][p, 8:72, :])
        T[p, 8:72, :] = pick(at_fr, turn(FR[0][p, 8:72, :], 3), t)

    def pack_faces(get, out, count, low, high, width, apart, start=0):
        for i0 in range(start, start + count, 16):
            half = i0 % 16
            lo = hi = None
            for i in range(i0, min(i0 + 16 - half, start + count)):
                j = i % 16
                t = get(i)
                a = turn(t, 8 * j)
                b = turn(t, 8 * j + apart) if apart else a
                if lo is None:
                    lo, hi = a, b
                else:
                    lo = pick(within(low + 8 * j, width), a, lo)
                    hi = pick(within(high + apart + 8 * j, width), b, hi)
            if half:
                lo = pick(within(low + 64, 64), lo, out[0][i0 // 16])
                hi = pick(within(high + apart + 64, 64), hi, out[1][i0 // 16])
            out[0][i0 // 16] = lo
            out[1][i0 // 16] = hi

    for c, (start, end) in enumerate(zip(FETCHED, FETCHED[1:])):
        for copy in fetch(c):
            copy.wait()
        for p in range(3 + start, 3 + end):
            apart(p)
        for p in range(3 + start, 3 + end):
            faces_of(p)
        pack_faces(lambda i: T[3 + i, 8:72, :], zs["f"], end - start, 0, 61, 8, 0, start)
    for side, (near, next_) in enumerate(((3, 4), (34, 33))):
        for k, (a, other) in enumerate(((near, FR[0]), (next_, FB[0]))):
            xs[side][k] = pick(lane < 64, B[0][a, 8:72, :], turn(other[near, 8:72, :], 64))
    pl.semaphore_wait(barrier, rooms[0] * rooms[1] * rooms[2] - 1)

    at_edge = [(at == 0) | (at == SIDE - 1) for at in me]

    def halo(key, directions, pieces):
        k = PHASES.index(key)
        total = dict.fromkeys(EDGES, 0)
        for d in directions:
            copies = pieces(d)

            @pl.when(inside(d, me))
            def _(d=d, copies=copies):
                device = tuple(at + step for at, step in zip(me, d))
                for src, dst, _ in copies:
                    pltpu.make_async_remote_copy(
                        src, dst, send_sem.at[k], recv_sem.at[k], device_id=device, device_id_type=MESH
                    ).start()

            for edge in total:
                if not any(e and step > 0 for e, step in zip(edge, d)):
                    total[edge] += sum(rows for _, _, rows in copies)
        return k, total

    def both(a, b):
        return a[0], {edge: a[1][edge] + b[1][edge] for edge in EDGES}

    def sides(arrays, oy, n):
        def pieces(d):
            out = []
            for src, ps, dst, pd, own, hp, hr in arrays:
                s0, d0, w = {-1: (ps, pd + own, hp), 0: (ps, pd, own), 1: (ps + own - hp, pd - hp, hp)}[d[0]]
                rs, rd, rw = {-1: (0, oy + n, hr), 0: (0, oy, n), 1: (n - hr, oy - hr, hr)}[d[1]]
                rs = rs + (oy if src.shape[1] > n else 0)
                out.append((src.at[pl.ds(s0, w), pl.ds(rs, rw), :], dst.at[pl.ds(d0, w), pl.ds(rd, rw), :], w * rw))
            return out

        return pieces

    def faces(key, oy, n, hz):
        groups = zs[key][0].shape[0]

        def pieces(d):
            s0, d0, w = {-1: (0, groups + 1, 1), 0: (0, 1, groups), 1: (groups - 1, 0, 1)}[d[0]]
            rs, rd, rw = {-1: (0, oy + n, hz), 0: (0, oy, n), 1: (n - hz, oy - hz, hz)}[d[1]]
            src, dst = (zs[key][0], zr[key][1]) if d[2] < 0 else (zs[key][1], zr[key][0])
            return [(src.at[pl.ds(s0, w), pl.ds(rs, rw), :], dst.at[pl.ds(d0, w), pl.ds(rd, rw), :], w * rw)]

        return pieces

    def exchange(key, arrays, oy, n, hz, directions):
        packed = halo(key, directions, faces(key, oy, n, hz))
        return both(packed, halo(key, FLAT, sides(arrays, oy, n)))

    def settle(what, arrived, left):
        k, total = what
        other = tuple(jnp.where(at == 0, at + 1, at - 1) for at in me)
        for edge, rows in total.items():
            same = None
            for e, here in zip(edge, at_edge):
                t = here if e else jnp.logical_not(here)
                same = t if same is None else same & t

            @pl.when(same)
            def _(rows=rows):
                cut = tally.at[pl.ds(0, rows), :]
                copy = pltpu.make_async_remote_copy(cut, cut, send_sem.at[k], recv_sem.at[k], device_id=other, device_id_type=MESH)
                if arrived:
                    copy.wait_recv()
                if left:
                    copy.wait_send()

    def first_sides(d):
        side = 0 if d[0] < 0 else 1
        rs, rd, rw = {-1: (0, 72, 3), 0: (0, 8, 64), 1: (61, 5, 3)}[d[1]]
        return [(xs[side].at[:, pl.ds(rs, rw), :], xr[1 - side].at[:, pl.ds(rd, rw), :], 2 * rw)]

    def first_rows(d):
        side = 0 if d[1] < 0 else 1
        return [(ys[side].at[:, pl.ds(0, 3), :], yr[1 - side].at[:, pl.ds(0, 3), :], 96)]

    beside0 = halo("fz", BESIDE, faces("f", 8, 64, 3))
    first = halo("f", FAR, faces("f", 8, 64, 3))
    first = both(first, halo("f", FLAT, lambda d: first_sides(d) if d[0] else first_rows(d)))
    def outside(ref, po, own, hp, oy, n, hr):
        planes, rows = ref.shape[0], ref.shape[1]
        for cond, cut in (
            (gx == 0, (slice(po - hp, po), slice(0, rows))),
            (gx == SIDE - 1, (slice(po + own, po + own + hp), slice(0, rows))),
            (gy == 0, (slice(0, planes), slice(oy - hr, oy))),
            (gy == SIDE - 1, (slice(0, planes), slice(oy + n, oy + n + hr))),
        ):

            @pl.when(cond)
            def _(cut=cut):
                shape = (cut[1].stop - cut[1].start, 128)
                for p in range(cut[0].start, cut[0].stop):
                    ref[p, cut[1], :] = jnp.zeros(shape, F32)

    def outside_z(key):
        for side, cond in ((0, gz == 0), (1, gz == SIDE - 1)):

            @pl.when(cond)
            def _(side=side):
                ref = zr[key][side]
                ref[...] = jnp.zeros(ref.shape, F32)

    def edges_z(key, po, n, hz, oy, groups):
        for side in (0, 1):
            ref = zr[key][side]
            rows = ref.shape[1]
            for cond, cut in (
                (gx == 0, (0, 1, 0, rows)),
                (gx == SIDE - 1, (groups + 1, 1, 0, rows)),
                (gy == 0, (0, groups + 2, oy - hz, hz)),
                (gy == SIDE - 1, (0, groups + 2, oy + n, hz)),
            ):

                @pl.when(cond)
                def _(cut=cut, ref=ref):
                    ref[pl.ds(cut[0], cut[1]), pl.ds(cut[2], cut[3]), :] = jnp.zeros((cut[1], cut[3], 128), F32)

    outside(H, 3, 32, 2, 8, 64, 3)
    for i in range(2):
        for cond, refs0 in ((gx == (0, SIDE - 1)[i], (xr[i],)), (gy == (0, SIDE - 1)[i], (yr[i],))):

            @pl.when(cond)
            def _(refs0=refs0):
                for ref in refs0:
                    ref[...] = jnp.zeros(ref.shape, F32)

        @pl.when(gy == (0, SIDE - 1)[i])
        def _(i=i):
            for ref in xr:
                for k in range(2):
                    ref[k, pl.ds((5, 72)[i], 3), :] = jnp.zeros((3, 128), F32)

    for key, n, oy, groups, hz in (("f", 64, 8, 2, 3), ("v", 64, 8, 2, 3), (1, 32, 16, 2, 6), (2, 16, 16, 1, 7)):
        outside_z(key)
        edges_z(key, 3, n, hz, oy, groups)
    outside(PR[1], 2, 8, 2, 16, 32, 8)
    outside(PR[2], 1, 2, 1, 16, 16, 8)
    for dx, dy in itertools.product((-1, 0, 1), repeat=2):
        if (dx, dy) != (0, 0):

            @pl.when(jnp.logical_not(inside((dx, dy, 0), me)))
            def _(dx=dx, dy=dy):
                Z3[dx + 1, dy + 1] = jnp.zeros((4 * SIDE, 128), F32)

    for l in (4, 5, 6):
        R[l][...] = jnp.zeros(LEV[l].shape(), F32)
        B[l][...] = jnp.zeros(LEV[l].shape(), F32)
    for l in (4, 5):
        EX[l][...] = jnp.zeros(EX[l].shape, F32)

    def tables(l):
        lv = LEV[l]
        shape = (lv.nr, 128)
        row, lane = iota(shape, 0) + lv.r0, iota(shape, 1)
        y = row - lv.oy
        z = jnp.where(lane < 100, lane, lane - 128)
        if l < 4:
            y = y + gy * lv.n
        if l < 3:
            z = z + gz * lv.n
        last = lv.total - 1
        within = (y >= 0) & (y <= last) & (z >= 0) & (z <= last)
        one = lambda c: jnp.where(c, 1, 0)
        w = one(y == 0) + one(y == last) + one(z == 0) + one(z == last)
        high = one(((row + lane) & 1) == 1)
        for kind, colour in itertools.product(range(3), range(2)):
            a = high if colour == 0 else 1 - high
            d = w if kind == 0 else (w + 1 - a if kind == 1 else w + a)
            inv = jnp.where(d == 0, 1 / 6, jnp.where(d == 1, 1 / 7, jnp.where(d == 2, 1 / 8, 1 / 9)))
            C[l][kind, colour] = jnp.where(within, inv, 0.0)
            D[l][kind, colour] = 6.0 + d.astype(F32)
            if colour == 1 and l < 6:
                q = jnp.where(within, 0.25, 0.0)
                Q[l][kind] = q
                A[l][kind] = (1.0 - d.astype(F32)) * q
        for colour in range(2):
            C[l][3, colour] = jnp.zeros(shape, F32)
            D[l][3, colour] = jnp.full(shape, 6.0, F32)
        if l < 6:
            Q[l][3] = jnp.zeros(shape, F32)
            A[l][3] = jnp.zeros(shape, F32)

    for l in range(7):
        tables(l)

    def kind(l, p):
        lv = LEV[l]
        x = 2 * (p - lv.po) + (gx * lv.n if l < 4 else 0)
        if l >= 4:
            return jnp.where(x == 0, 1, jnp.where(x == lv.total - 2, 2, 0))
        return jnp.where(x == 0, 1, jnp.where(x == lv.total - 2, 2, jnp.where((x < 0) | (x >= lv.total), 3, 0)))

    def slot_of(i, n):
        groups = n // 16
        if i < 0:
            return 0, 16 + i
        if i >= n:
            return groups + 1, i - n
        return 1 + i // 16, i % 16

    def unpack_first(i, r0, nr, which):
        g, j = slot_of(i, 32)
        rows = pl.ds(r0, nr)
        low, high = zr["f"][0][g, rows, :], zr["f"][1][g, rows, :]
        for k, at, width, shift in which:
            ref = (B, FR, FB)[k][0]
            w = turn(pick(within(8 * j + at, width), high, low), shift - 8 * j)
            ref[3 + i, rows, :] = pick(lane < 64, ref[3 + i, rows, :], w)

    settle(beside0, True, False)
    for i in range(32):
        unpack_first(i, 8, 64, LANE_FACES)

    settle(first, True, True)
    settle(beside0, False, True)
    tokens(0, 2, True)

    for side, (near, next_) in enumerate(((2, 1), (35, 36))):
        rows = pl.ds(4, 72)
        a, b = xr[side][0, rows, :], xr[side][1, rows, :]
        B[0][near, rows, :] = a
        B[0][next_, rows, :] = b
        FR[0][near, rows, :] = turn(a, 64)
        FB[0][near, rows, :] = turn(b, 64)
    for i in (-2, -1, 32, 33):
        unpack_first(i, 4, 72, LANE_FACES[: 3 if -1 <= i < 33 else 1])
    for i in range(32):
        for side, (rb, rr, rk) in enumerate(((5, 6, 7), (72, 72, 72))):
            t = yr[side][i]
            f = turn(t, 64)
            B[0][3 + i, rb : rb + 3, :] = t[0:3]
            FR[0][3 + i, rr : rr + 2, :] = f[0:2]
            FB[0][3 + i, rk : rk + 1, :] = f[2:3]
            unpack_first(i, (0, 72)[side], 8, LANE_FACES)

    def red_sweep(l):
        lv = LEV[l]
        p0, count, r0, nr = RED[l]
        rows, table = pl.ds(r0, nr), pl.ds(r0 - lv.r0, nr)

        def body(p):
            R[l][p, rows, :] = (FR[l][p, rows, :] + around(B[l], p, r0, nr, m)) * C[l][kind(l, p), 0, table, :]

        sweep_loop(p0, count, 36, body)

    def black_sweep(l, region, keep):
        lv = LEV[l]
        p0, count, r0, nr = region[l]
        rows, table = pl.ds(r0, nr), pl.ds(r0 - lv.r0, nr)

        def body(p):
            t = kind(l, p)
            fs = FB[l][p, rows, :] + around(R[l], p, r0, nr, not_m)
            b = fs * C[l][t, 1, table, :]
            B[l][p, rows, :] = b
            if keep:
                T[p, rows, :] = fs - D[l][t, 1, table, :] * b

        sweep_loop(p0, count, 36, body)

    def red_residual(l, p):
        lv = LEV[l]
        s = around(B[l], p, lv.oy, lv.n, m)
        at = lv.oy - lv.r0
        return FR[l][p, pl.ds(lv.oy, lv.n), :] + s - D[l][kind(l, p), 0, pl.ds(at, lv.n), :] * R[l][p, pl.ds(lv.oy, lv.n), :]

    def residual(l):
        lv = LEV[l]

        def body(p):
            T[p, pl.ds(lv.oy, lv.n), :] = T[p, pl.ds(lv.oy, lv.n), :] + red_residual(l, p)

        sweep_loop(lv.po, lv.n // 2, 32, body)

    def coarse_side(l, p):
        lv = LEV[l]
        half = lv.n // 2
        u = T[p, pl.ds(lv.oy, half, stride=2), :] + T[p, pl.ds(lv.oy + 1, half, stride=2), :]
        z = 2 * lane_index(half)
        return 0.5 * (take(u, z & 127) + take(u, (z + 1) & 127))

    red_sweep(0)
    black_sweep(0, BLACK_DOWN, True)

    def restrict_to(l, dst, first_plane, first_row):
        lv = LEV[l]

        def body(p):
            dst[p - lv.po + first_plane, pl.ds(first_row, lv.n // 2), :] = coarse_side(l, p)

        sweep_loop(lv.po, lv.n // 2, 32, body)

    residual(0)
    restrict_to(0, G[1], 0, 0)

    def send_right_side(l):
        n, w = LEV[l].n, WIDTH[l]
        per = 128 // n
        for q in range(n // per):
            t = G[l][per * q]
            for j in range(1, per):
                t = pick(within(n * j, n), turn(G[l][per * q + j], n * j), t)
            PS[l][q] = t
        pack_faces(lambda i: G[l][i], zs[l], n, 0, n - 8, 8, 128 - 2 * n)
        wide = 8 // per
        beside = halo(f"{l}z", BESIDE, faces(l, 16, n, w))
        return beside, exchange(l, [(PS[l], 0, PR[l], wide, n // per, wide, w)], 16, n, w, FAR)

    def side_lanes(l, i, rows):
        g, j = slot_of(i, LEV[l].n)
        return turn(pick(within(8 * j, 8), zr[l][1][g, rows, :], zr[l][0][g, rows, :]), LEV[l].n - 8 * j)

    def own_side_lanes(l):
        n = LEV[l].n
        for i in range(n):
            G[l][i] = pick(lane < n, G[l][i], side_lanes(l, i, pl.ds(16, n)))

    def split_right_side(l):
        lv = LEV[l]
        n = lv.n
        per = 128 // n

        def natural(i):
            q, k = (i + 8) // per, (i + 8) % per

            def tile(r, nr):
                rows = pl.ds(r, nr)
                return pick(lane < n, turn(PR[l][q, rows, :], -n * k), side_lanes(l, i, rows))

            if 0 <= i < n:
                return jnp.concatenate([tile(8, 8), G[l][i], tile(16 + n, 8)], axis=0)
            return tile(lv.r0, lv.nr)

        p0, count, _, _ = BLACK_DOWN[l] if l == 1 else (lv.p0, lv.np, 0, 0)
        for p in range(p0, p0 + count):
            a, b = natural(2 * (p - lv.po)), natural(2 * (p - lv.po) + 1)
            store_colours(l, p, a, b)

    def store_colours(l, p, a, b):
        lv = LEV[l]
        rows = pl.ds(lv.r0, lv.nr)
        red = pick(m, b, a)
        FR[l][p, rows, :] = red
        FB[l][p, rows, :] = pick(m, a, b)
        R[l][p, rows, :] = red * C[l][kind(l, p), 0]

    beside1, second = send_right_side(1)
    def keep_black(p):
        H[p, 8:72, :] = B[0][p, 8:72, :]

    sweep_loop(3, 32, 8, keep_black)

    tokens(0, 2, False)
    tokens(1, 4, True)
    settle(beside1, True, False)
    own_side_lanes(1)
    settle(second, True, False)
    split_right_side(1)
    black_sweep(1, BLACK_DOWN, True)
    residual(1)
    restrict_to(1, G[2], 0, 0)
    beside2, third = send_right_side(2)
    pack_faces(lambda i: B[0][3 + i, 8:72, :], zs["v"], 32, 0, 61, 3, 0)
    kept = exchange("v", [(B[0], 3, H, 3, 32, 2, 3)], 8, 64, 3, ACROSS)
    settle(beside2, True, False)
    own_side_lanes(2)
    settle(third, True, False)
    split_right_side(2)
    black_sweep(2, BLACK_DOWN, True)
    residual(2)

    own3 = None
    for i in range(8):
        g = jnp.where(lane < 8, coarse_side(2, LEV[2].po + i), 0.0)
        g = pltpu.roll(g, 8 * lax.rem(gz + i, 8), axis=1)
        own3 = g if own3 is None else own3 + g
    pack3[0:8, :] = own3
    own3 = jnp.where(lane[0:4] < 64, pack3[0:4, :], turn(pack3[4:8, :], 64))
    pack3[8:12, :] = own3
    Z3[1, 1, pl.ds(4 * gz, 4), :] = own3
    tokens(1, 4, False)

    k3 = PHASES.index("3")
    for dx, dy in sorted(itertools.product((-1, 0, 1), repeat=2), key=lambda d: -abs(d[0]) - abs(d[1])):

        @pl.when(inside((dx, dy, 0), me))
        def _(dx=dx, dy=dy):
            for far in (4, 3, 5, 2, 6, 1, 7, 0):
                if (dx, dy, far) != (0, 0, 0):
                    pltpu.make_async_remote_copy(
                        pack3.at[pl.ds(8, 4), :],
                        Z3.at[1 - dx, 1 - dy, pl.ds(4 * gz, 4), :],
                        send_sem.at[k3],
                        recv_sem.at[k3],
                        device_id=(gx + dx, gy + dy, (gz + far) & (SIDE - 1)),
                        device_id_type=MESH,
                    ).start()

    blocks = {edge: 4 * ((2 if edge[0] else 3) * (2 if edge[1] else 3) * SIDE - 1) for edge in EDGES}
    settle((k3, blocks), True, False)

    for p in range(1, 13):
        ab = []
        for i in (2 * (p - 1), 2 * (p - 1) + 1):
            x = i % 8
            tiles = []
            for cy in range(3):
                t = None
                for k in range(SIDE):
                    block = Z3[i // 8, cy, 4 * k : 4 * k + 4, :]
                    s = 8 * ((x + k) % 8)
                    t = block if t is None else jnp.where((within(s, 8) | within(s + 64, 8))[0:4], block, t)
                other = turn(t, 64)
                low = lane[0:4] < 64
                t = jnp.concatenate([jnp.where(low, t, other), jnp.where(low, other, t)], axis=0)
                tiles.append(turn(t, -8 * x))
            ab.append(jnp.concatenate(tiles, axis=0))
        store_colours(3, p, ab[0], ab[1])
    black_sweep(3, BLACK_DOWN, True)

    residual(3)
    own4 = None
    for i in range(4):
        g = turn(pick(lane < 32, coarse_side(3, LEV[3].po + i), jnp.zeros((4, 128), F32)), 32 * i)
        own4 = g if own4 is None else own4 + g
    pack4[0:4, :] = own4
    G4[gx, pl.ds(4 * gy, 4), :] = own4

    k4 = PHASES.index("4")

    ring = lambda k: min(k, SIDE - k)
    for dx, dy in sorted(itertools.product(range(SIDE), repeat=2), key=lambda d: -ring(d[0]) - ring(d[1])):
        if (dx, dy) != (0, 0):
            pltpu.make_async_remote_copy(
                pack4.at[pl.ds(0, 4), :],
                G4.at[gx, pl.ds(4 * gy, 4), :],
                send_sem.at[k4],
                recv_sem.at[k4],
                device_id=((gx + dx) & (SIDE - 1), (gy + dy) & (SIDE - 1), gz),
                device_id_type=MESH,
            ).start()
    plane = (k4, dict.fromkeys(EDGES, 4 * (SIDE * SIDE - 1)))
    settle(kept, True, True)
    for i in range(-2, 34):
        g, j = slot_of(i, 32)
        w = turn(pick(within(8 * j, 3), zr["v"][1][g, 4:76, :], zr["v"][0][g, 4:76, :]), 64 - 8 * j)
        H[3 + i, 4:76, :] = pick(lane < 64, H[3 + i, 4:76, :], w)
    settle(plane, True, False)
    for x in range(SIDE):
        parts = [turn(G4[x], -32 * i) for i in range(4)]
        store_colours(4, 4 + 2 * x, parts[0], parts[1])
        store_colours(4, 5 + 2 * x, parts[2], parts[3])
    for l in (4, 5):
        black_sweep(l, BLACK_DOWN, True)
        residual(l)
        restrict_to(l, N[l + 1], 0, 0)
        lv = LEV[l + 1]
        for p in range(lv.p0, lv.p0 + lv.np):
            store_colours(l + 1, p, N[l + 1][2 * (p - 1)], N[l + 1][2 * (p - 1) + 1])
    black_sweep(6, BLACK_UP, False)
    for _ in range(COARSE_SWEEPS - 1):
        red_sweep(6)
        black_sweep(6, BLACK_UP, False)

    def expand(l):
        lf, lc = LEV[l], LEV[l + 1]
        c0, cn, r0, rn = GIVE[l]
        fine0 = lf.oy + 2 * (r0 - lc.oy)
        if l == 3:
            c0, r0 = 2 * gx + 1, 4 * gy + 4
            fine0 = 8
        zf = lane_index(rn)
        z = (jnp.where(zf < 100, zf, zf - 128) >> 1) + (8 * gz if l == 2 else 0)
        at, beside = z & 127, (z + 2 * (zf & 1) - 1) & 127

        def body(i):
            rows = pl.ds(r0, rn)
            r, b = R[l + 1][c0 + i, rows, :], B[l + 1][c0 + i, rows, :]
            if rn % 8:
                mm = ((iota((rn, 128), 0) + iota((rn, 128), 1)) & 1) == 1
                both = jnp.where(mm, b, r), jnp.where(mm, r, b)
            else:
                both = pick(m, b, r), pick(m, r, b)
            for a, e in enumerate(both):
                here, there = take(e, at), take(e, beside)
                for k in (0, 1):
                    EX[l][2 * i + a, pl.ds(fine0 + k, rn, stride=2), :] = here
                    EZ[l][2 * i + a, pl.ds(fine0 + k, rn, stride=2), :] = there

        sweep_loop(0, cn, 20, body)

    def correct(l):
        lv = LEV[l]
        second_row = (iota((8, 128), 0) & 1) == 1
        p0, count, r0, nr = CORRECTED[l]
        rows, table = pl.ds(r0, nr), pl.ds(r0 - lv.r0, nr)

        def body(p):
            e = p - EDGE[l]
            t = kind(l, p)
            sides = pick(m, EX[l][e - 1, rows, :], EX[l][e + 1, rows, :])
            sides = sides + pick(second_row, EX[l][e, pl.ds(r0 + 1, nr), :], EX[l][e, pl.ds(r0 - 1, nr), :])
            add = EX[l][e, rows, :] * A[l][t, table, :] + (EZ[l][e, rows, :] + sides) * Q[l][t, table, :]
            return add

        start = B[l] if l else H

        def plain(p):
            B[l][p, rows, :] = start[p, rows, :] + body(p)

        sweep_loop(p0, count, 36, plain)

    for l in (5, 4):
        expand(l)
        correct(l)
        red_sweep(l)
        black_sweep(l, BLACK_UP, False)
    expand(3)
    correct(3)
    red_sweep(3)
    black_sweep(3, BLACK_UP, False)
    expand(2)
    correct(2)
    red_sweep(2)
    black_sweep(2, BLACK_UP, False)
    expand(1)
    correct(1)
    red_sweep(1)
    black_sweep(1, BLACK_UP, False)
    expand(0)
    correct(0)
    red_sweep(0)
    for what in (beside1, second, beside2, third, (k3, blocks), plane):
        settle(what, False, True)


def results(R, FR, FB, C, D, u_hbm, r_hbm, B, T, u_out, r_out, sem):
    lv = LEV[0]
    m = odd()
    not_m = jnp.logical_not(m)

    def kind(p):
        x = lax.axis_index("gx") * lv.n + 2 * (p - lv.po)
        return jnp.where(x == 0, 1, jnp.where(x == lv.total - 2, 2, jnp.where((x < 0) | (x >= lv.total), 3, 0)))

    def black(p):
        t = kind(p)
        fs = FB[p, 4:76, :] + around(R, p, 4, 72, not_m)
        b = fs * C[t, 1]
        B[p, 4:76, :] = b
        T[p, 4:76, :] = fs - D[t, 1] * b

    def finish(p):
        x = 2 * (p - lv.po)
        r, b = R[p, 8:72, :], B[p, 8:72, :]
        u_out[x] = pick(m, b, r)[:, 0:64]
        u_out[x + 1] = pick(m, r, b)[:, 0:64]
        left = FR[p, 8:72, :] + around(B, p, lv.oy, lv.n, m) - D[kind(p), 0, 4:68, :] * r
        b = T[p, 8:72, :]
        r_out[x] = pick(m, b, left)[:, 0:64]
        r_out[x + 1] = pick(m, left, b)[:, 0:64]

    done, first, copies = 2, 3, []
    for part in PARTS:
        ready = min(first + part + (PARTS[0] if first == 3 else part), 35)
        for p in range(done, ready + 1):
            black(p)
        done = ready + 1
        for p in range(first, first + part):
            finish(p)
        cut = pl.ds(2 * (first - 3), 2 * part)
        for src, dst in ((u_out, u_hbm), (r_out, r_hbm)):
            copy = pltpu.make_async_copy(src.at[cut], dst.at[cut], sem.at[len(copies)])
            copy.start()
            copies.append(copy)
        first += part
    for copy in copies:
        copy.wait()


PARTS = (4, 4, 4, 4, 4, 4, 4, 4)
LANE_FACES = ((0, 0, 3, 64), (1, 3, 2, 61), (2, 5, 1, 59))
FETCHED = (0, 8, 16, 24, 32)
EDGES = tuple(itertools.product((False, True), repeat=3))
AROUND = sorted((d for d in itertools.product((-1, 0, 1), repeat=3) if any(d)), key=lambda d: -sum(map(abs, d)))
FLAT = [d for d in AROUND if d[2] == 0]
ACROSS = [d for d in AROUND if d[2]]
FAR = [d for d in ACROSS if d not in BESIDE]
EDGE = {0: -1, 1: -1, 2: -1, 3: -1, 4: 2, 5: -1}


def inside(d, me, far=1):
    ok = None
    for step, at in zip(d, me):
        if step:
            here = (at >= far) if step < 0 else (at < SIDE - far)
            ok = here if ok is None else ok & here
    return True if ok is None else ok


def vmem(*shape):
    return pltpu.VMEM(shape, F32)


def per_device(right_side, guess):
    whole = vmem(64, 64, 64)
    scratch = [whole, whole]
    scratch += [vmem(*lv.shape()) for lv in LEV[1:]]
    scratch += [vmem(*lv.shape()) for lv in LEV]
    for _ in range(2):
        scratch += [vmem(*lv.shape()) for lv in LEV[1:]]
    for _ in range(2):
        scratch += [vmem(4, 2, lv.nr, 128) for lv in LEV[1:]]
    for _ in range(2):
        scratch += [vmem(4, lv.nr, 128) for lv in LEV[:6]]
    for _ in range(2):
        scratch += [vmem(2 * GIVE[l][1], LEV[l].rows, 128) for l in range(6)]
    scratch += [vmem(*LEV[0].shape())] * 2
    scratch += [vmem(2, 64, 128)] * 2 + [vmem(2, 80, 128)] * 2 + [vmem(32, 8, 128)] * 4
    scratch += [vmem(32, 32, 128), vmem(16, 16, 128)]
    scratch += [vmem(8, 32, 128), vmem(2, 16, 128), vmem(12, 64, 128), vmem(4, 48, 128)]
    scratch += [vmem(16, 16, 128), vmem(8, 8, 128)]
    packed = ((2, 64, 80), (2, 64, 80), (2, 32, 64), (1, 16, 48))
    for groups, n, _ in packed:
        scratch += [vmem(groups, n, 128)] * 2
    for groups, _, rows in packed:
        scratch += [vmem(groups + 2, rows, 128)] * 2
    scratch += [vmem(16, 128), vmem(3, 3, 32, 128), vmem(8, 128), vmem(8, 32, 128), vmem(2048, 128)]
    dma = pltpu.SemaphoreType.DMA((len(PHASES),))
    scratch += [dma, dma, pltpu.SemaphoreType.DMA((8,)), pltpu.SemaphoreType.REGULAR((2,))]
    level0, table = pltpu.VMEM(LEV[0].shape(), F32), pltpu.VMEM((4, 2, LEV[0].nr, 128), F32)
    parts = pl.pallas_call(
        kernel,
        out_shape=(level0,) * 3 + (table, table),
        in_specs=[pl.BlockSpec(memory_space=pl.ANY)] * 2,
        out_specs=(pl.BlockSpec(memory_space=pltpu.VMEM),) * 5,
        scratch_shapes=scratch,
        compiler_params=pltpu.CompilerParams(collective_id=0, has_side_effects=True, vmem_limit_bytes=48 * 2**20),
    )(right_side, guess)
    block = jax.ShapeDtypeStruct(right_side.shape, F32)
    return pl.pallas_call(
        results,
        out_shape=(block, block),
        in_specs=[pl.BlockSpec(memory_space=pltpu.VMEM)] * 5,
        out_specs=(pl.BlockSpec(memory_space=pl.ANY),) * 2,
        scratch_shapes=[vmem(*LEV[0].shape())] * 2 + [vmem(64, 64, 64)] * 2 + [pltpu.SemaphoreType.DMA((2 * len(PARTS),))],
        compiler_params=pltpu.CompilerParams(vmem_limit_bytes=12 * 2**20),
    )(*parts)


def solution(mesh):
    spec = P("gx", "gy", "gz")
    return jax.shard_map(per_device, mesh=mesh, in_specs=(spec, spec), out_specs=(spec, spec), check_vma=False)
```

```python
import itertools

import jax
import jax.numpy as jnp
from jax import lax
from jax.experimental import pallas as pl
from jax.experimental.pallas import tpu as pltpu
from jax.sharding import PartitionSpec as P

COARSE_SWEEPS = 4
MESH = pl.DeviceIdType.MESH
SIDE = 8
F32 = jnp.float32


class Level:
    def __init__(self, n, total, po, oy, p0, np_, r0, nr, pairs, rows, whole_z):
        self.n, self.total, self.po, self.oy = n, total, po, oy
        self.p0, self.np, self.r0, self.nr = p0, np_, r0, nr
        self.pairs, self.rows, self.whole_z = pairs, rows, whole_z

    def shape(self):
        return (self.pairs, self.rows, 128)


LEV = [
    Level(64, 512, 3, 8, 1, 36, 4, 72, 38, 80, False),
    Level(32, 256, 5, 16, 1, 24, 8, 48, 26, 64, False),
    Level(16, 128, 5, 16, 1, 16, 8, 32, 18, 48, False),
    Level(8, 64, 5, 16, 1, 12, 8, 24, 14, 40, True),
    Level(32, 32, 4, 8, 4, 16, 8, 32, 24, 48, True),
    Level(16, 16, 1, 8, 1, 8, 8, 16, 10, 32, True),
    Level(8, 8, 1, 8, 1, 4, 8, 8, 6, 24, True),
]
GIVE = {0: (3, 20, 12, 40), 1: (2, 14, 12, 24), 2: (2, 10, 12, 16), 3: (0, 8, 0, 12), 4: (0, 10, 8, 16), 5: (0, 6, 8, 8)}
ALL = {4: (4, 16, 8, 32), 5: (1, 8, 8, 16), 6: (1, 4, 8, 8)}
RED = {0: (2, 34, 4, 72), 1: (3, 20, 12, 40), 2: (2, 14, 8, 32), 3: (2, 10, 8, 24), **ALL}
BLACK_DOWN = {0: (2, 34, 4, 72), 1: (2, 22, 8, 48), 2: (2, 14, 8, 32), 3: (2, 10, 8, 24), **ALL}
BLACK_UP = {1: (3, 20, 12, 40), 2: (3, 12, 12, 24), 3: (3, 8, 12, 16), **ALL}
CORRECTED = {0: (1, 36, 4, 72), 1: (2, 22, 8, 48), 2: (2, 14, 8, 32), 3: (2, 10, 8, 24), **ALL}
PHASES = ("f", "v", 1, 2, "3", "4", "fz", "1z", "2z")
BESIDE = [(0, 0, -1), (0, 0, 1)]
WIDTH = {1: 6, 2: 7}


def iota(shape, axis):
    return lax.broadcasted_iota(jnp.int32, shape, axis)


def odd():
    return ((iota((8, 128), 0) + iota((8, 128), 1)) & 1) == 1


def lanes():
    return iota((8, 128), 1)


def pick(mask, a, b):
    shape = a.shape
    if shape[0] <= 8:
        return jnp.where(mask[: shape[0]], a, b)
    tiles = (shape[0] // 8, 8, 128)
    return jnp.where(mask[None], a.reshape(tiles), b.reshape(tiles)).reshape(shape)


def within(start, width):
    return ((lanes() - start) & 127) < width


def turn(a, shift):
    return pltpu.roll(a, shift % 128, axis=1) if shift % 128 else a


def take(a, index):
    return jnp.take_along_axis(a, index, axis=1, mode="promise_in_bounds")


def lane_index(rows):
    return iota((rows, 128), 1)


def sweep_loop(start, count, step, body):
    step = max(k for k in range(1, step + 1) if count % k == 0)
    if count == step:
        for i in range(count):
            body(start + i)
        return

    def some(j, carry):
        for i in range(step):
            body(start + j * step + i)
        return carry

    lax.fori_loop(0, count // step, some, 0)


def emit(*stages):
    start = min(first + lag for first, _, lag, _ in stages)
    end = max(first + count + lag for first, count, lag, _ in stages)
    for t in range(start, end):
        for first, count, lag, body in stages:
            if first <= t - lag < first + count:
                body(t - lag)


def around(src, p, r0, nr, up):
    here = src[p, pl.ds(r0, nr), :]
    side = pick(up, src[p + 1, pl.ds(r0, nr), :], src[p - 1, pl.ds(r0, nr), :])
    rows = src[p, pl.ds(r0 - 1, nr), :] + src[p, pl.ds(r0 + 1, nr), :]
    return (here + side) + rows + (pltpu.roll(here, 1, axis=1) + pltpu.roll(here, 127, axis=1))


def kernel(*refs):
    it = iter(refs)
    f_hbm, u_hbm, R0, FR0, FB0, C0, D0 = (next(it) for _ in range(7))
    f_in, u_in = next(it), next(it)
    R = [R0] + [next(it) for _ in range(6)]
    B = [next(it) for _ in range(7)]
    FR = [FR0] + [next(it) for _ in range(6)]
    FB = [FB0] + [next(it) for _ in range(6)]
    C = [C0] + [next(it) for _ in range(6)]
    D = [D0] + [next(it) for _ in range(6)]
    A = [next(it) for _ in range(6)]
    Q = [next(it) for _ in range(6)]
    EX = [next(it) for _ in range(6)]
    EZ = [next(it) for _ in range(6)]
    T, H = next(it), next(it)
    xs, xr = (next(it), next(it)), (next(it), next(it))
    ys, yr = (next(it), next(it)), (next(it), next(it))
    G = {1: next(it), 2: next(it)}
    PS = {1: next(it), 2: next(it)}
    PR = {1: next(it), 2: next(it)}
    N = {5: next(it), 6: next(it)}
    zs = {k: (next(it), next(it)) for k in ("f", "v", 1, 2)}
    zr = {k: (next(it), next(it)) for k in ("f", "v", 1, 2)}
    pack3, Z3, pack4, G4, tally = (next(it) for _ in range(5))
    send_sem, recv_sem, in_sem, token = (next(it) for _ in range(4))

    gx, gy, gz = lax.axis_index("gx"), lax.axis_index("gy"), lax.axis_index("gz")
    me = (gx, gy, gz)

    def fetch(c):
        cut = pl.ds(2 * FETCHED[c], 2 * (FETCHED[c + 1] - FETCHED[c]))
        return [
            pltpu.make_async_copy(src.at[cut], dst.at[cut], in_sem.at[2 * c + i])
            for i, (src, dst) in enumerate(((u_hbm, u_in), (f_hbm, f_in)))
        ]

    for c in range(len(FETCHED) - 1):
        for copy in fetch(c):
            copy.start()

    barrier = pltpu.get_barrier_semaphore()
    rooms = [jnp.where((at > 0) & (at < SIDE - 1), 3, 2) for at in me]
    for d in itertools.product((-1, 0, 1), repeat=3):
        if d != (0, 0, 0):

            @pl.when(inside(d, me))
            def _(d=d):
                pl.semaphore_signal(barrier, inc=1, device_id=tuple(at + step for at, step in zip(me, d)), device_id_type=MESH)

    def tokens(k, far, act):
        count = jnp.int32(0)
        for d in itertools.product((-1, 0, 1), repeat=3):
            if d == (0, 0, 0) or (d[2] and (d[0] or d[1])):
                continue
            there = inside(d, me, far)
            count = count + jnp.where(there, 1, 0)
            if act:

                @pl.when(there)
                def _(d=d):
                    device = tuple(at + far * step for at, step in zip(me, d))
                    pl.semaphore_signal(token.at[k], inc=1, device_id=device, device_id_type=MESH)

        if not act:
            pl.semaphore_wait(token.at[k], count)

    lv = LEV[0]
    m64 = ((iota((64, 64), 0) + iota((64, 64), 1)) & 1) == 1
    lane, m = lanes(), odd()
    not_m = jnp.logical_not(m)
    at_fb = within(5, 1) | within(68, 1)
    at_fr = within(3, 2) | within(65, 2)
    third_row = iota((8, 128), 0) == 2

    def apart(p):
        a, b = u_in[2 * (p - lv.po)], u_in[2 * (p - lv.po) + 1]
        B[0][p, 8:72, 0:64] = jnp.where(m64, a, b)
        a, b = f_in[2 * (p - lv.po)], f_in[2 * (p - lv.po) + 1]
        FR[0][p, 8:72, 0:64] = jnp.where(m64, b, a)
        FB[0][p, 8:72, 0:64] = jnp.where(m64, a, b)

    def faces_of(p):
        for side, (rb, rr, rk) in enumerate(((8, 8, 6), (69, 70, 69))):
            t = turn(jnp.where(third_row, FB[0][p, rk : rk + 8, :], FR[0][p, rr : rr + 8, :]), 64)
            ys[side][p - 3] = jnp.where(lane < 64, B[0][p, rb : rb + 8, :], t)
        t = pick(at_fb, turn(FB[0][p, 8:72, :], 5), B[0][p, 8:72, :])
        T[p, 8:72, :] = pick(at_fr, turn(FR[0][p, 8:72, :], 3), t)

    def pack_faces(get, out, count, low, high, width, apart, start=0):
        for i0 in range(start, start + count, 16):
            half = i0 % 16
            lo = hi = None
            for i in range(i0, min(i0 + 16 - half, start + count)):
                j = i % 16
                t = get(i)
                a = turn(t, 8 * j)
                b = turn(t, 8 * j + apart) if apart else a
                if lo is None:
                    lo, hi = a, b
                else:
                    lo = pick(within(low + 8 * j, width), a, lo)
                    hi = pick(within(high + apart + 8 * j, width), b, hi)
            if half:
                lo = pick(within(low + 64, 64), lo, out[0][i0 // 16])
                hi = pick(within(high + apart + 64, 64), hi, out[1][i0 // 16])
            out[0][i0 // 16] = lo
            out[1][i0 // 16] = hi

    for c, (start, end) in enumerate(zip(FETCHED, FETCHED[1:])):
        for copy in fetch(c):
            copy.wait()
        for p in range(3 + start, 3 + end):
            apart(p)
        for p in range(3 + start, 3 + end):
            faces_of(p)
        pack_faces(lambda i: T[3 + i, 8:72, :], zs["f"], end - start, 0, 61, 8, 0, start)
    for side, (near, next_) in enumerate(((3, 4), (34, 33))):
        for k, (a, other) in enumerate(((near, FR[0]), (next_, FB[0]))):
            xs[side][k] = pick(lane < 64, B[0][a, 8:72, :], turn(other[near, 8:72, :], 64))
    pl.semaphore_wait(barrier, rooms[0] * rooms[1] * rooms[2] - 1)

    at_edge = [(at == 0) | (at == SIDE - 1) for at in me]

    def halo(key, directions, pieces):
        k = PHASES.index(key)
        total = dict.fromkeys(EDGES, 0)
        for d in directions:
            copies = pieces(d)

            @pl.when(inside(d, me))
            def _(d=d, copies=copies):
                device = tuple(at + step for at, step in zip(me, d))
                for src, dst, _ in copies:
                    pltpu.make_async_remote_copy(
                        src, dst, send_sem.at[k], recv_sem.at[k], device_id=device, device_id_type=MESH
                    ).start()

            for edge in total:
                if not any(e and step > 0 for e, step in zip(edge, d)):
                    total[edge] += sum(rows for _, _, rows in copies)
        return k, total

    def both(a, b):
        return a[0], {edge: a[1][edge] + b[1][edge] for edge in EDGES}

    def sides(arrays, oy, n):
        def pieces(d):
            out = []
            for src, ps, dst, pd, own, hp, hr in arrays:
                s0, d0, w = {-1: (ps, pd + own, hp), 0: (ps, pd, own), 1: (ps + own - hp, pd - hp, hp)}[d[0]]
                rs, rd, rw = {-1: (0, oy + n, hr), 0: (0, oy, n), 1: (n - hr, oy - hr, hr)}[d[1]]
                rs = rs + (oy if src.shape[1] > n else 0)
                out.append((src.at[pl.ds(s0, w), pl.ds(rs, rw), :], dst.at[pl.ds(d0, w), pl.ds(rd, rw), :], w * rw))
            return out

        return pieces

    def faces(key, oy, n, hz):
        groups = zs[key][0].shape[0]

        def pieces(d):
            s0, d0, w = {-1: (0, groups + 1, 1), 0: (0, 1, groups), 1: (groups - 1, 0, 1)}[d[0]]
            rs, rd, rw = {-1: (0, oy + n, hz), 0: (0, oy, n), 1: (n - hz, oy - hz, hz)}[d[1]]
            src, dst = (zs[key][0], zr[key][1]) if d[2] < 0 else (zs[key][1], zr[key][0])
            return [(src.at[pl.ds(s0, w), pl.ds(rs, rw), :], dst.at[pl.ds(d0, w), pl.ds(rd, rw), :], w * rw)]

        return pieces

    def exchange(key, arrays, oy, n, hz, directions):
        packed = halo(key, directions, faces(key, oy, n, hz))
        return both(packed, halo(key, FLAT, sides(arrays, oy, n)))

    def settle(what, arrived, left):
        k, total = what
        other = tuple(jnp.where(at == 0, at + 1, at - 1) for at in me)
        for edge, rows in total.items():
            same = None
            for e, here in zip(edge, at_edge):
                t = here if e else jnp.logical_not(here)
                same = t if same is None else same & t

            @pl.when(same)
            def _(rows=rows):
                cut = tally.at[pl.ds(0, rows), :]
                copy = pltpu.make_async_remote_copy(cut, cut, send_sem.at[k], recv_sem.at[k], device_id=other, device_id_type=MESH)
                if arrived:
                    copy.wait_recv()
                if left:
                    copy.wait_send()

    def first_sides(d):
        side = 0 if d[0] < 0 else 1
        rs, rd, rw = {-1: (0, 72, 3), 0: (0, 8, 64), 1: (61, 5, 3)}[d[1]]
        return [(xs[side].at[:, pl.ds(rs, rw), :], xr[1 - side].at[:, pl.ds(rd, rw), :], 2 * rw)]

    def first_rows(d):
        side = 0 if d[1] < 0 else 1
        return [(ys[side].at[:, pl.ds(0, 3), :], yr[1 - side].at[:, pl.ds(0, 3), :], 96)]

    beside0 = halo("fz", BESIDE, faces("f", 8, 64, 3))
    first = halo("f", FAR, faces("f", 8, 64, 3))
    first = both(first, halo("f", FLAT, lambda d: first_sides(d) if d[0] else first_rows(d)))
    def outside(ref, po, own, hp, oy, n, hr):
        planes, rows = ref.shape[0], ref.shape[1]
        for cond, cut in (
            (gx == 0, (slice(po - hp, po), slice(0, rows))),
            (gx == SIDE - 1, (slice(po + own, po + own + hp), slice(0, rows))),
            (gy == 0, (slice(0, planes), slice(oy - hr, oy))),
            (gy == SIDE - 1, (slice(0, planes), slice(oy + n, oy + n + hr))),
        ):

            @pl.when(cond)
            def _(cut=cut):
                shape = (cut[1].stop - cut[1].start, 128)
                for p in range(cut[0].start, cut[0].stop):
                    ref[p, cut[1], :] = jnp.zeros(shape, F32)

    def outside_z(key):
        for side, cond in ((0, gz == 0), (1, gz == SIDE - 1)):

            @pl.when(cond)
            def _(side=side):
                ref = zr[key][side]
                ref[...] = jnp.zeros(ref.shape, F32)

    def edges_z(key, po, n, hz, oy, groups):
        for side in (0, 1):
            ref = zr[key][side]
            rows = ref.shape[1]
            for cond, cut in (
                (gx == 0, (0, 1, 0, rows)),
                (gx == SIDE - 1, (groups + 1, 1, 0, rows)),
                (gy == 0, (0, groups + 2, oy - hz, hz)),
                (gy == SIDE - 1, (0, groups + 2, oy + n, hz)),
            ):

                @pl.when(cond)
                def _(cut=cut, ref=ref):
                    ref[pl.ds(cut[0], cut[1]), pl.ds(cut[2], cut[3]), :] = jnp.zeros((cut[1], cut[3], 128), F32)

    outside(H, 3, 32, 2, 8, 64, 3)
    for i in range(2):
        for cond, refs0 in ((gx == (0, SIDE - 1)[i], (xr[i],)), (gy == (0, SIDE - 1)[i], (yr[i],))):

            @pl.when(cond)
            def _(refs0=refs0):
                for ref in refs0:
                    ref[...] = jnp.zeros(ref.shape, F32)

        @pl.when(gy == (0, SIDE - 1)[i])
        def _(i=i):
            for ref in xr:
                for k in range(2):
                    ref[k, pl.ds((5, 72)[i], 3), :] = jnp.zeros((3, 128), F32)

    for key, n, oy, groups, hz in (("f", 64, 8, 2, 3), ("v", 64, 8, 2, 3), (1, 32, 16, 2, 6), (2, 16, 16, 1, 7)):
        outside_z(key)
        edges_z(key, 3, n, hz, oy, groups)
    outside(PR[1], 2, 8, 2, 16, 32, 8)
    outside(PR[2], 1, 2, 1, 16, 16, 8)
    for dx, dy in itertools.product((-1, 0, 1), repeat=2):
        if (dx, dy) != (0, 0):

            @pl.when(jnp.logical_not(inside((dx, dy, 0), me)))
            def _(dx=dx, dy=dy):
                Z3[dx + 1, dy + 1] = jnp.zeros((4 * SIDE, 128), F32)

    for l in (4, 5, 6):
        R[l][...] = jnp.zeros(LEV[l].shape(), F32)
        B[l][...] = jnp.zeros(LEV[l].shape(), F32)
    for l in (4, 5):
        EX[l][...] = jnp.zeros(EX[l].shape, F32)

    def tables(l):
        lv = LEV[l]
        shape = (lv.nr, 128)
        row, lane = iota(shape, 0) + lv.r0, iota(shape, 1)
        y = row - lv.oy
        z = jnp.where(lane < 100, lane, lane - 128)
        if l < 4:
            y = y + gy * lv.n
        if l < 3:
            z = z + gz * lv.n
        last = lv.total - 1
        within = (y >= 0) & (y <= last) & (z >= 0) & (z <= last)
        one = lambda c: jnp.where(c, 1, 0)
        w = one(y == 0) + one(y == last) + one(z == 0) + one(z == last)
        high = one(((row + lane) & 1) == 1)
        for kind, colour in itertools.product(range(3), range(2)):
            a = high if colour == 0 else 1 - high
            d = w if kind == 0 else (w + 1 - a if kind == 1 else w + a)
            inv = jnp.where(d == 0, 1 / 6, jnp.where(d == 1, 1 / 7, jnp.where(d == 2, 1 / 8, 1 / 9)))
            C[l][kind, colour] = jnp.where(within, inv, 0.0)
            D[l][kind, colour] = 6.0 + d.astype(F32)
            if colour == 1 and l < 6:
                q = jnp.where(within, 0.25, 0.0)
                Q[l][kind] = q
                A[l][kind] = (1.0 - d.astype(F32)) * q
        for colour in range(2):
            C[l][3, colour] = jnp.zeros(shape, F32)
            D[l][3, colour] = jnp.full(shape, 6.0, F32)
        if l < 6:
            Q[l][3] = jnp.zeros(shape, F32)
            A[l][3] = jnp.zeros(shape, F32)

    for l in range(7):
        tables(l)

    def kind(l, p):
        lv = LEV[l]
        x = 2 * (p - lv.po) + (gx * lv.n if l < 4 else 0)
        if l >= 4:
            return jnp.where(x == 0, 1, jnp.where(x == lv.total - 2, 2, 0))
        return jnp.where(x == 0, 1, jnp.where(x == lv.total - 2, 2, jnp.where((x < 0) | (x >= lv.total), 3, 0)))

    def slot_of(i, n):
        groups = n // 16
        if i < 0:
            return 0, 16 + i
        if i >= n:
            return groups + 1, i - n
        return 1 + i // 16, i % 16

    def unpack_first(i, r0, nr, which):
        g, j = slot_of(i, 32)
        rows = pl.ds(r0, nr)
        low, high = zr["f"][0][g, rows, :], zr["f"][1][g, rows, :]
        for k, at, width, shift in which:
            ref = (B, FR, FB)[k][0]
            w = turn(pick(within(8 * j + at, width), high, low), shift - 8 * j)
            ref[3 + i, rows, :] = pick(lane < 64, ref[3 + i, rows, :], w)

    settle(beside0, True, False)
    for i in range(32):
        unpack_first(i, 8, 64, LANE_FACES)

    settle(first, True, True)
    settle(beside0, False, True)
    tokens(0, 2, True)

    for side, (near, next_) in enumerate(((2, 1), (35, 36))):
        rows = pl.ds(4, 72)
        a, b = xr[side][0, rows, :], xr[side][1, rows, :]
        B[0][near, rows, :] = a
        B[0][next_, rows, :] = b
        FR[0][near, rows, :] = turn(a, 64)
        FB[0][near, rows, :] = turn(b, 64)
    for i in (-2, -1, 32, 33):
        unpack_first(i, 4, 72, LANE_FACES[: 3 if -1 <= i < 33 else 1])
    for i in range(32):
        for side, (rb, rr, rk) in enumerate(((5, 6, 7), (72, 72, 72))):
            t = yr[side][i]
            f = turn(t, 64)
            B[0][3 + i, rb : rb + 3, :] = t[0:3]
            FR[0][3 + i, rr : rr + 2, :] = f[0:2]
            FB[0][3 + i, rk : rk + 1, :] = f[2:3]
            unpack_first(i, (0, 72)[side], 8, LANE_FACES)

    def red(l, lag):
        lv = LEV[l]
        p0, count, r0, nr = RED[l]
        rows, table = pl.ds(r0, nr), pl.ds(r0 - lv.r0, nr)

        def body(p):
            R[l][p, rows, :] = (FR[l][p, rows, :] + around(B[l], p, r0, nr, m)) * C[l][kind(l, p), 0, table, :]

        return p0, count, lag, body

    def black(l, region, keep, lag):
        lv = LEV[l]
        p0, count, r0, nr = region[l]
        rows, table = pl.ds(r0, nr), pl.ds(r0 - lv.r0, nr)

        def body(p):
            t = kind(l, p)
            fs = FB[l][p, rows, :] + around(R[l], p, r0, nr, not_m)
            b = fs * C[l][t, 1, table, :]
            B[l][p, rows, :] = b
            if keep:
                T[p, rows, :] = fs - D[l][t, 1, table, :] * b

        return p0, count, lag, body

    def red_sweep(l):
        emit(red(l, 0))

    def black_sweep(l, region, keep):
        emit(black(l, region, keep, 0))

    def red_residual(l, p):
        lv = LEV[l]
        s = around(B[l], p, lv.oy, lv.n, m)
        at = lv.oy - lv.r0
        return FR[l][p, pl.ds(lv.oy, lv.n), :] + s - D[l][kind(l, p), 0, pl.ds(at, lv.n), :] * R[l][p, pl.ds(lv.oy, lv.n), :]

    def residue(l, lag):
        lv = LEV[l]

        def body(p):
            T[p, pl.ds(lv.oy, lv.n), :] = T[p, pl.ds(lv.oy, lv.n), :] + red_residual(l, p)

        return lv.po, lv.n // 2, lag, body

    def residual(l):
        emit(residue(l, 0))

    def coarse_side(l, p):
        lv = LEV[l]
        half = lv.n // 2
        u = T[p, pl.ds(lv.oy, half, stride=2), :] + T[p, pl.ds(lv.oy + 1, half, stride=2), :]
        z = 2 * lane_index(half)
        return 0.5 * (take(u, z & 127) + take(u, (z + 1) & 127))

    def restrict(l, dst, lag):
        lv = LEV[l]

        def body(p):
            dst[p - lv.po, pl.ds(0, lv.n // 2), :] = coarse_side(l, p)

        return lv.po, lv.n // 2, lag, body


    def send_right_side(l):
        n, w = LEV[l].n, WIDTH[l]
        per = 128 // n
        for q in range(n // per):
            t = G[l][per * q]
            for j in range(1, per):
                t = pick(within(n * j, n), turn(G[l][per * q + j], n * j), t)
            PS[l][q] = t
        pack_faces(lambda i: G[l][i], zs[l], n, 0, n - 8, 8, 128 - 2 * n)
        wide = 8 // per
        beside = halo(f"{l}z", BESIDE, faces(l, 16, n, w))
        return beside, exchange(l, [(PS[l], 0, PR[l], wide, n // per, wide, w)], 16, n, w, FAR)

    def side_lanes(l, i, rows):
        g, j = slot_of(i, LEV[l].n)
        return turn(pick(within(8 * j, 8), zr[l][1][g, rows, :], zr[l][0][g, rows, :]), LEV[l].n - 8 * j)

    def own_side_lanes(l):
        n = LEV[l].n
        for i in range(n):
            G[l][i] = pick(lane < n, G[l][i], side_lanes(l, i, pl.ds(16, n)))

    def split_right_side(l):
        lv = LEV[l]
        n = lv.n
        per = 128 // n

        def natural(i):
            q, k = (i + 8) // per, (i + 8) % per

            def tile(r, nr):
                rows = pl.ds(r, nr)
                return pick(lane < n, turn(PR[l][q, rows, :], -n * k), side_lanes(l, i, rows))

            if 0 <= i < n:
                return jnp.concatenate([tile(8, 8), G[l][i], tile(16 + n, 8)], axis=0)
            return tile(lv.r0, lv.nr)

        p0, count, _, _ = BLACK_DOWN[l] if l == 1 else (lv.p0, lv.np, 0, 0)
        for p in range(p0, p0 + count):
            a, b = natural(2 * (p - lv.po)), natural(2 * (p - lv.po) + 1)
            store_colours(l, p, a, b)

    def store_colours(l, p, a, b):
        lv = LEV[l]
        rows = pl.ds(lv.r0, lv.nr)
        red = pick(m, b, a)
        FR[l][p, rows, :] = red
        FB[l][p, rows, :] = pick(m, a, b)
        R[l][p, rows, :] = red * C[l][kind(l, p), 0]

    emit(red(0, 0), black(0, BLACK_DOWN, True, 8), residue(0, 16), restrict(0, G[1], 22))
    beside1, second = send_right_side(1)
    def keep_black(p):
        H[p, 8:72, :] = B[0][p, 8:72, :]

    sweep_loop(3, 32, 8, keep_black)

    tokens(0, 2, False)
    tokens(1, 4, True)
    settle(beside1, True, False)
    own_side_lanes(1)
    settle(second, True, False)
    split_right_side(1)
    black_sweep(1, BLACK_DOWN, True)
    residual(1)
    emit(restrict(1, G[2], 0))
    beside2, third = send_right_side(2)
    pack_faces(lambda i: B[0][3 + i, 8:72, :], zs["v"], 32, 0, 61, 3, 0)
    kept = exchange("v", [(B[0], 3, H, 3, 32, 2, 3)], 8, 64, 3, ACROSS)
    settle(beside2, True, False)
    own_side_lanes(2)
    settle(third, True, False)
    split_right_side(2)
    black_sweep(2, BLACK_DOWN, True)
    residual(2)

    own3 = None
    for i in range(8):
        g = jnp.where(lane < 8, coarse_side(2, LEV[2].po + i), 0.0)
        g = pltpu.roll(g, 8 * lax.rem(gz + i, 8), axis=1)
        own3 = g if own3 is None else own3 + g
    pack3[0:8, :] = own3
    own3 = jnp.where(lane[0:4] < 64, pack3[0:4, :], turn(pack3[4:8, :], 64))
    pack3[8:12, :] = own3
    Z3[1, 1, pl.ds(4 * gz, 4), :] = own3
    tokens(1, 4, False)

    k3 = PHASES.index("3")
    for dx, dy in sorted(itertools.product((-1, 0, 1), repeat=2), key=lambda d: -abs(d[0]) - abs(d[1])):

        @pl.when(inside((dx, dy, 0), me))
        def _(dx=dx, dy=dy):
            for far in (4, 3, 5, 2, 6, 1, 7, 0):
                if (dx, dy, far) != (0, 0, 0):
                    pltpu.make_async_remote_copy(
                        pack3.at[pl.ds(8, 4), :],
                        Z3.at[1 - dx, 1 - dy, pl.ds(4 * gz, 4), :],
                        send_sem.at[k3],
                        recv_sem.at[k3],
                        device_id=(gx + dx, gy + dy, (gz + far) & (SIDE - 1)),
                        device_id_type=MESH,
                    ).start()

    blocks = {edge: 4 * ((2 if edge[0] else 3) * (2 if edge[1] else 3) * SIDE - 1) for edge in EDGES}
    settle((k3, blocks), True, False)

    for p in range(1, 13):
        ab = []
        for i in (2 * (p - 1), 2 * (p - 1) + 1):
            x = i % 8
            tiles = []
            for cy in range(3):
                t = None
                for k in range(SIDE):
                    block = Z3[i // 8, cy, 4 * k : 4 * k + 4, :]
                    s = 8 * ((x + k) % 8)
                    t = block if t is None else jnp.where((within(s, 8) | within(s + 64, 8))[0:4], block, t)
                other = turn(t, 64)
                low = lane[0:4] < 64
                t = jnp.concatenate([jnp.where(low, t, other), jnp.where(low, other, t)], axis=0)
                tiles.append(turn(t, -8 * x))
            ab.append(jnp.concatenate(tiles, axis=0))
        store_colours(3, p, ab[0], ab[1])
    black_sweep(3, BLACK_DOWN, True)

    residual(3)
    own4 = None
    for i in range(4):
        g = turn(pick(lane < 32, coarse_side(3, LEV[3].po + i), jnp.zeros((4, 128), F32)), 32 * i)
        own4 = g if own4 is None else own4 + g
    pack4[0:4, :] = own4
    G4[gx, pl.ds(4 * gy, 4), :] = own4

    k4 = PHASES.index("4")

    ring = lambda k: min(k, SIDE - k)
    for dx, dy in sorted(itertools.product(range(SIDE), repeat=2), key=lambda d: -ring(d[0]) - ring(d[1])):
        if (dx, dy) != (0, 0):
            pltpu.make_async_remote_copy(
                pack4.at[pl.ds(0, 4), :],
                G4.at[gx, pl.ds(4 * gy, 4), :],
                send_sem.at[k4],
                recv_sem.at[k4],
                device_id=((gx + dx) & (SIDE - 1), (gy + dy) & (SIDE - 1), gz),
                device_id_type=MESH,
            ).start()
    plane = (k4, dict.fromkeys(EDGES, 4 * (SIDE * SIDE - 1)))
    settle(kept, True, True)
    for i in range(-2, 34):
        g, j = slot_of(i, 32)
        w = turn(pick(within(8 * j, 3), zr["v"][1][g, 4:76, :], zr["v"][0][g, 4:76, :]), 64 - 8 * j)
        H[3 + i, 4:76, :] = pick(lane < 64, H[3 + i, 4:76, :], w)
    settle(plane, True, False)
    for x in range(SIDE):
        parts = [turn(G4[x], -32 * i) for i in range(4)]
        store_colours(4, 4 + 2 * x, parts[0], parts[1])
        store_colours(4, 5 + 2 * x, parts[2], parts[3])
    for l in (4, 5):
        black_sweep(l, BLACK_DOWN, True)
        residual(l)
        emit(restrict(l, N[l + 1], 0))
        lv = LEV[l + 1]
        for p in range(lv.p0, lv.p0 + lv.np):
            store_colours(l + 1, p, N[l + 1][2 * (p - 1)], N[l + 1][2 * (p - 1) + 1])
    black_sweep(6, BLACK_UP, False)
    for _ in range(COARSE_SWEEPS - 1):
        red_sweep(6)
        black_sweep(6, BLACK_UP, False)

    def expanding(l, lag):
        lf, lc = LEV[l], LEV[l + 1]
        c0, cn, r0, rn = GIVE[l]
        fine0 = lf.oy + 2 * (r0 - lc.oy)
        if l == 3:
            c0, r0 = 2 * gx + 1, 4 * gy + 4
            fine0 = 8
        zf = lane_index(rn)
        z = (jnp.where(zf < 100, zf, zf - 128) >> 1) + (8 * gz if l == 2 else 0)
        at, beside = z & 127, (z + 2 * (zf & 1) - 1) & 127

        def body(i):
            rows = pl.ds(r0, rn)
            r, b = R[l + 1][c0 + i, rows, :], B[l + 1][c0 + i, rows, :]
            if rn % 8:
                mm = ((iota((rn, 128), 0) + iota((rn, 128), 1)) & 1) == 1
                both = jnp.where(mm, b, r), jnp.where(mm, r, b)
            else:
                both = pick(m, b, r), pick(m, r, b)
            for a, e in enumerate(both):
                here, there = take(e, at), take(e, beside)
                for k in (0, 1):
                    EX[l][2 * i + a, pl.ds(fine0 + k, rn, stride=2), :] = here
                    EZ[l][2 * i + a, pl.ds(fine0 + k, rn, stride=2), :] = there

        return EDGE[l], 2 * cn, lag, lambda p: body((p - EDGE[l]) // 2) if (p - EDGE[l]) % 2 == 0 else None

    def expand(l):
        emit(expanding(l, 0))

    def correcting(l, lag):
        lv = LEV[l]
        second_row = (iota((8, 128), 0) & 1) == 1
        p0, count, r0, nr = CORRECTED[l]
        rows, table = pl.ds(r0, nr), pl.ds(r0 - lv.r0, nr)

        def body(p):
            e = p - EDGE[l]
            t = kind(l, p)
            sides = pick(m, EX[l][e - 1, rows, :], EX[l][e + 1, rows, :])
            sides = sides + pick(second_row, EX[l][e, pl.ds(r0 + 1, nr), :], EX[l][e, pl.ds(r0 - 1, nr), :])
            add = EX[l][e, rows, :] * A[l][t, table, :] + (EZ[l][e, rows, :] + sides) * Q[l][t, table, :]
            return add

        start = B[l] if l else H

        def plain(p):
            B[l][p, rows, :] = start[p, rows, :] + body(p)

        return p0, count, lag, plain

    def correct(l):
        emit(correcting(l, 0))

    for l in (5, 4):
        expand(l)
        correct(l)
        red_sweep(l)
        black_sweep(l, BLACK_UP, False)
    expand(3)
    correct(3)
    red_sweep(3)
    black_sweep(3, BLACK_UP, False)
    expand(2)
    correct(2)
    red_sweep(2)
    black_sweep(2, BLACK_UP, False)
    emit(expanding(1, 0), correcting(1, 8), red(1, 12), black(1, BLACK_UP, False, 18))
    emit(expanding(0, 0), correcting(0, 12), red(0, 16))
    for what in (beside1, second, beside2, third, (k3, blocks), plane):
        settle(what, False, True)


def results(R, FR, FB, C, D, u_hbm, r_hbm, B, T, u_out, r_out, sem):
    lv = LEV[0]
    m = odd()
    not_m = jnp.logical_not(m)

    def kind(p):
        x = lax.axis_index("gx") * lv.n + 2 * (p - lv.po)
        return jnp.where(x == 0, 1, jnp.where(x == lv.total - 2, 2, jnp.where((x < 0) | (x >= lv.total), 3, 0)))

    def black(p):
        t = kind(p)
        fs = FB[p, 4:76, :] + around(R, p, 4, 72, not_m)
        b = fs * C[t, 1]
        B[p, 4:76, :] = b
        T[p, 4:76, :] = fs - D[t, 1] * b

    copies = []

    def out(src, dst, k):
        cut = pl.ds(2 * (STARTS[k] - 3), 2 * PARTS[k])
        copy = pltpu.make_async_copy(src.at[cut], dst.at[cut], sem.at[len(copies)])
        copy.start()
        copies.append(copy)

    def solve(k):
        for p in range(STARTS[k] + (1 if k else -1), STARTS[k] + PARTS[k] + 1):
            black(p)
        for p in range(STARTS[k], STARTS[k] + PARTS[k]):
            x = 2 * (p - lv.po)
            r, b = R[p, 8:72, :], B[p, 8:72, :]
            u_out[x] = pick(m, b, r)[:, 0:64]
            u_out[x + 1] = pick(m, r, b)[:, 0:64]
        out(u_out, u_hbm, k)

    def remain(k):
        for p in range(STARTS[k], STARTS[k] + PARTS[k]):
            x = 2 * (p - lv.po)
            left = FR[p, 8:72, :] + around(B, p, lv.oy, lv.n, m) - D[kind(p), 0, 4:68, :] * R[p, 8:72, :]
            b = T[p, 8:72, :]
            r_out[x] = pick(m, b, left)[:, 0:64]
            r_out[x + 1] = pick(m, left, b)[:, 0:64]
        out(r_out, r_hbm, k)

    solve(0)
    for k in range(1, len(PARTS)):
        solve(k)
        remain(k - 1)
    remain(len(PARTS) - 1)
    for copy in copies:
        copy.wait()


PARTS = (4, 4, 4, 4, 4, 4, 4, 4)
STARTS = tuple(3 + sum(PARTS[:k]) for k in range(len(PARTS)))
LANE_FACES = ((0, 0, 3, 64), (1, 3, 2, 61), (2, 5, 1, 59))
FETCHED = (0, 8, 16, 24, 32)
EDGES = tuple(itertools.product((False, True), repeat=3))
AROUND = sorted((d for d in itertools.product((-1, 0, 1), repeat=3) if any(d)), key=lambda d: -sum(map(abs, d)))
FLAT = [d for d in AROUND if d[2] == 0]
ACROSS = [d for d in AROUND if d[2]]
FAR = [d for d in ACROSS if d not in BESIDE]
EDGE = {0: -1, 1: -1, 2: -1, 3: -1, 4: 2, 5: -1}


def inside(d, me, far=1):
    ok = None
    for step, at in zip(d, me):
        if step:
            here = (at >= far) if step < 0 else (at < SIDE - far)
            ok = here if ok is None else ok & here
    return True if ok is None else ok


def vmem(*shape):
    return pltpu.VMEM(shape, F32)


def per_device(right_side, guess):
    whole = vmem(64, 64, 64)
    scratch = [whole, whole]
    scratch += [vmem(*lv.shape()) for lv in LEV[1:]]
    scratch += [vmem(*lv.shape()) for lv in LEV]
    for _ in range(2):
        scratch += [vmem(*lv.shape()) for lv in LEV[1:]]
    for _ in range(2):
        scratch += [vmem(4, 2, lv.nr, 128) for lv in LEV[1:]]
    for _ in range(2):
        scratch += [vmem(4, lv.nr, 128) for lv in LEV[:6]]
    for _ in range(2):
        scratch += [vmem(2 * GIVE[l][1], LEV[l].rows, 128) for l in range(6)]
    scratch += [vmem(*LEV[0].shape())] * 2
    scratch += [vmem(2, 64, 128)] * 2 + [vmem(2, 80, 128)] * 2 + [vmem(32, 8, 128)] * 4
    scratch += [vmem(32, 32, 128), vmem(16, 16, 128)]
    scratch += [vmem(8, 32, 128), vmem(2, 16, 128), vmem(12, 64, 128), vmem(4, 48, 128)]
    scratch += [vmem(16, 16, 128), vmem(8, 8, 128)]
    packed = ((2, 64, 80), (2, 64, 80), (2, 32, 64), (1, 16, 48))
    for groups, n, _ in packed:
        scratch += [vmem(groups, n, 128)] * 2
    for groups, _, rows in packed:
        scratch += [vmem(groups + 2, rows, 128)] * 2
    scratch += [vmem(16, 128), vmem(3, 3, 32, 128), vmem(8, 128), vmem(8, 32, 128), vmem(2048, 128)]
    dma = pltpu.SemaphoreType.DMA((len(PHASES),))
    scratch += [dma, dma, pltpu.SemaphoreType.DMA((8,)), pltpu.SemaphoreType.REGULAR((2,))]
    level0, table = pltpu.VMEM(LEV[0].shape(), F32), pltpu.VMEM((4, 2, LEV[0].nr, 128), F32)
    parts = pl.pallas_call(
        kernel,
        out_shape=(level0,) * 3 + (table, table),
        in_specs=[pl.BlockSpec(memory_space=pl.ANY)] * 2,
        out_specs=(pl.BlockSpec(memory_space=pltpu.VMEM),) * 5,
        scratch_shapes=scratch,
        compiler_params=pltpu.CompilerParams(collective_id=0, has_side_effects=True, vmem_limit_bytes=48 * 2**20),
    )(right_side, guess)
    block = jax.ShapeDtypeStruct(right_side.shape, F32)
    return pl.pallas_call(
        results,
        out_shape=(block, block),
        in_specs=[pl.BlockSpec(memory_space=pltpu.VMEM)] * 5,
        out_specs=(pl.BlockSpec(memory_space=pl.ANY),) * 2,
        scratch_shapes=[vmem(*LEV[0].shape())] * 2 + [vmem(64, 64, 64)] * 2 + [pltpu.SemaphoreType.DMA((2 * len(PARTS),))],
        compiler_params=pltpu.CompilerParams(vmem_limit_bytes=12 * 2**20),
    )(*parts)


def solution(mesh):
    spec = P("gx", "gy", "gz")
    return jax.shard_map(per_device, mesh=mesh, in_specs=(spec, spec), out_specs=(spec, spec), check_vma=False)
```

```python
import itertools

import jax
import jax.numpy as jnp
from jax import lax
from jax.experimental import pallas as pl
from jax.experimental.pallas import tpu as pltpu
from jax.sharding import PartitionSpec as P

COARSE_SWEEPS = 4
MESH = pl.DeviceIdType.MESH
SIDE = 8
F32 = jnp.float32


class Level:
    def __init__(self, n, total, po, oy, p0, np_, r0, nr, pairs, rows, whole_z):
        self.n, self.total, self.po, self.oy = n, total, po, oy
        self.p0, self.np, self.r0, self.nr = p0, np_, r0, nr
        self.pairs, self.rows, self.whole_z = pairs, rows, whole_z

    def shape(self):
        return (self.pairs, self.rows, 128)


LEV = [
    Level(64, 512, 3, 8, 1, 36, 4, 72, 38, 80, False),
    Level(32, 256, 5, 16, 1, 24, 8, 48, 26, 64, False),
    Level(16, 128, 5, 16, 1, 16, 8, 32, 18, 48, False),
    Level(8, 64, 5, 16, 1, 12, 8, 24, 14, 40, True),
    Level(32, 32, 4, 8, 4, 16, 8, 32, 24, 48, True),
    Level(16, 16, 1, 8, 1, 8, 8, 16, 10, 32, True),
    Level(8, 8, 1, 8, 1, 4, 8, 8, 6, 24, True),
]
GIVE = {0: (3, 20, 12, 40), 1: (2, 14, 12, 24), 2: (2, 10, 12, 16), 3: (0, 8, 0, 12), 4: (0, 10, 8, 16), 5: (0, 6, 8, 8)}
ALL = {4: (4, 16, 8, 32), 5: (1, 8, 8, 16), 6: (1, 4, 8, 8)}
RED = {0: (2, 34, 4, 72), 1: (3, 20, 12, 40), 2: (2, 14, 8, 32), 3: (2, 10, 8, 24), **ALL}
BLACK_DOWN = {0: (2, 34, 4, 72), 1: (2, 22, 8, 48), 2: (2, 14, 8, 32), 3: (2, 10, 8, 24), **ALL}
BLACK_UP = {1: (3, 20, 12, 40), 2: (3, 12, 12, 24), 3: (3, 8, 12, 16), **ALL}
CORRECTED = {0: (1, 36, 4, 72), 1: (2, 22, 8, 48), 2: (2, 14, 8, 32), 3: (2, 10, 8, 24), **ALL}
PHASES = ("f", "v", 1, 2, "3", "4", "fz", "1z", "2z")
BESIDE = [(0, 0, -1), (0, 0, 1)]
WIDTH = {1: 6, 2: 7}


def iota(shape, axis):
    return lax.broadcasted_iota(jnp.int32, shape, axis)


def odd():
    return ((iota((8, 128), 0) + iota((8, 128), 1)) & 1) == 1


def lanes():
    return iota((8, 128), 1)


def pick(mask, a, b):
    shape = a.shape
    if shape[0] <= 8:
        return jnp.where(mask[: shape[0]], a, b)
    tiles = (shape[0] // 8, 8, 128)
    return jnp.where(mask[None], a.reshape(tiles), b.reshape(tiles)).reshape(shape)


def within(start, width):
    return ((lanes() - start) & 127) < width


def turn(a, shift):
    return pltpu.roll(a, shift % 128, axis=1) if shift % 128 else a


def take(a, index):
    return jnp.take_along_axis(a, index, axis=1, mode="promise_in_bounds")


def lane_index(rows):
    return iota((rows, 128), 1)


def sweep_loop(start, count, step, body):
    step = max(k for k in range(1, step + 1) if count % k == 0)
    if count == step:
        for i in range(count):
            body(start + i)
        return

    def some(j, carry):
        for i in range(step):
            body(start + j * step + i)
        return carry

    lax.fori_loop(0, count // step, some, 0)


def around(src, p, r0, nr, up):
    here = src[p, pl.ds(r0, nr), :]
    side = pick(up, src[p + 1, pl.ds(r0, nr), :], src[p - 1, pl.ds(r0, nr), :])
    rows = src[p, pl.ds(r0 - 1, nr), :] + src[p, pl.ds(r0 + 1, nr), :]
    return (here + side) + rows + (pltpu.roll(here, 1, axis=1) + pltpu.roll(here, 127, axis=1))


def kernel(*refs):
    it = iter(refs)
    f_hbm, u_hbm, R0, FR0, FB0, C0, D0 = (next(it) for _ in range(7))
    f_in, u_in = next(it), next(it)
    R = [R0] + [next(it) for _ in range(6)]
    B = [next(it) for _ in range(7)]
    FR = [FR0] + [next(it) for _ in range(6)]
    FB = [FB0] + [next(it) for _ in range(6)]
    C = [C0] + [next(it) for _ in range(6)]
    D = [D0] + [next(it) for _ in range(6)]
    A = [next(it) for _ in range(6)]
    Q = [next(it) for _ in range(6)]
    EX = [next(it) for _ in range(6)]
    EZ = [next(it) for _ in range(6)]
    T, H = next(it), next(it)
    xs, xr = (next(it), next(it)), (next(it), next(it))
    ys, yr = (next(it), next(it)), (next(it), next(it))
    G = {1: next(it), 2: next(it)}
    PS = {1: next(it), 2: next(it)}
    PR = {1: next(it), 2: next(it)}
    N = {5: next(it), 6: next(it)}
    zs = {k: (next(it), next(it)) for k in ("f", "v", 1, 2)}
    zr = {k: (next(it), next(it)) for k in ("f", "v", 1, 2)}
    pack3, Z3, pack4, G4, tally = (next(it) for _ in range(5))
    send_sem, recv_sem, in_sem, token = (next(it) for _ in range(4))

    gx, gy, gz = lax.axis_index("gx"), lax.axis_index("gy"), lax.axis_index("gz")
    me = (gx, gy, gz)

    def fetch(c):
        cut = pl.ds(2 * FETCHED[c], 2 * (FETCHED[c + 1] - FETCHED[c]))
        return [
            pltpu.make_async_copy(src.at[cut], dst.at[cut], in_sem.at[2 * c + i])
            for i, (src, dst) in enumerate(((u_hbm, u_in), (f_hbm, f_in)))
        ]

    for c in range(len(FETCHED) - 1):
        for copy in fetch(c):
            copy.start()

    barrier = pltpu.get_barrier_semaphore()
    rooms = [jnp.where((at > 0) & (at < SIDE - 1), 3, 2) for at in me]
    for d in itertools.product((-1, 0, 1), repeat=3):
        if d != (0, 0, 0):

            @pl.when(inside(d, me))
            def _(d=d):
                pl.semaphore_signal(barrier, inc=1, device_id=tuple(at + step for at, step in zip(me, d)), device_id_type=MESH)

    def tokens(k, far, act):
        count = jnp.int32(0)
        for d in itertools.product((-1, 0, 1), repeat=3):
            if d == (0, 0, 0) or (d[2] and (d[0] or d[1])):
                continue
            there = inside(d, me, far)
            count = count + jnp.where(there, 1, 0)
            if act:

                @pl.when(there)
                def _(d=d):
                    device = tuple(at + far * step for at, step in zip(me, d))
                    pl.semaphore_signal(token.at[k], inc=1, device_id=device, device_id_type=MESH)

        if not act:
            pl.semaphore_wait(token.at[k], count)

    lv = LEV[0]
    m64 = ((iota((64, 64), 0) + iota((64, 64), 1)) & 1) == 1
    lane, m = lanes(), odd()
    not_m = jnp.logical_not(m)
    at_fb = within(5, 1) | within(68, 1)
    at_fr = within(3, 2) | within(65, 2)
    third_row = iota((8, 128), 0) == 2

    def apart(p):
        a, b = u_in[2 * (p - lv.po)], u_in[2 * (p - lv.po) + 1]
        B[0][p, 8:72, 0:64] = jnp.where(m64, a, b)
        a, b = f_in[2 * (p - lv.po)], f_in[2 * (p - lv.po) + 1]
        FR[0][p, 8:72, 0:64] = jnp.where(m64, b, a)
        FB[0][p, 8:72, 0:64] = jnp.where(m64, a, b)

    def faces_of(p):
        for side, (rb, rr, rk) in enumerate(((8, 8, 6), (69, 70, 69))):
            t = turn(jnp.where(third_row, FB[0][p, rk : rk + 8, :], FR[0][p, rr : rr + 8, :]), 64)
            ys[side][p - 3] = jnp.where(lane < 64, B[0][p, rb : rb + 8, :], t)
        t = pick(at_fb, turn(FB[0][p, 8:72, :], 5), B[0][p, 8:72, :])
        T[p, 8:72, :] = pick(at_fr, turn(FR[0][p, 8:72, :], 3), t)

    def pack_faces(get, out, count, low, high, width, apart, start=0):
        for i0 in range(start, start + count, 16):
            half = i0 % 16
            lo = hi = None
            for i in range(i0, min(i0 + 16 - half, start + count)):
                j = i % 16
                t = get(i)
                a = turn(t, 8 * j)
                b = turn(t, 8 * j + apart) if apart else a
                if lo is None:
                    lo, hi = a, b
                else:
                    lo = pick(within(low + 8 * j, width), a, lo)
                    hi = pick(within(high + apart + 8 * j, width), b, hi)
            if half:
                lo = pick(within(low + 64, 64), lo, out[0][i0 // 16])
                hi = pick(within(high + apart + 64, 64), hi, out[1][i0 // 16])
            out[0][i0 // 16] = lo
            out[1][i0 // 16] = hi

    for c, (start, end) in enumerate(zip(FETCHED, FETCHED[1:])):
        for copy in fetch(c):
            copy.wait()
        for p in range(3 + start, 3 + end):
            apart(p)
        for p in range(3 + start, 3 + end):
            faces_of(p)
        pack_faces(lambda i: T[3 + i, 8:72, :], zs["f"], end - start, 0, 61, 8, 0, start)
    for side, (near, next_) in enumerate(((3, 4), (34, 33))):
        for k, (a, other) in enumerate(((near, FR[0]), (next_, FB[0]))):
            xs[side][k] = pick(lane < 64, B[0][a, 8:72, :], turn(other[near, 8:72, :], 64))
    pl.semaphore_wait(barrier, rooms[0] * rooms[1] * rooms[2] - 1)

    at_edge = [(at == 0) | (at == SIDE - 1) for at in me]

    def halo(key, directions, pieces):
        k = PHASES.index(key)
        total = dict.fromkeys(EDGES, 0)
        for d in directions:
            copies = pieces(d)

            @pl.when(inside(d, me))
            def _(d=d, copies=copies):
                device = tuple(at + step for at, step in zip(me, d))
                for src, dst, _ in copies:
                    pltpu.make_async_remote_copy(
                        src, dst, send_sem.at[k], recv_sem.at[k], device_id=device, device_id_type=MESH
                    ).start()

            for edge in total:
                if not any(e and step > 0 for e, step in zip(edge, d)):
                    total[edge] += sum(rows for _, _, rows in copies)
        return k, total

    def both(a, b):
        return a[0], {edge: a[1][edge] + b[1][edge] for edge in EDGES}

    def sides(arrays, oy, n):
        def pieces(d):
            out = []
            for src, ps, dst, pd, own, hp, hr in arrays:
                s0, d0, w = {-1: (ps, pd + own, hp), 0: (ps, pd, own), 1: (ps + own - hp, pd - hp, hp)}[d[0]]
                rs, rd, rw = {-1: (0, oy + n, hr), 0: (0, oy, n), 1: (n - hr, oy - hr, hr)}[d[1]]
                rs = rs + (oy if src.shape[1] > n else 0)
                out.append((src.at[pl.ds(s0, w), pl.ds(rs, rw), :], dst.at[pl.ds(d0, w), pl.ds(rd, rw), :], w * rw))
            return out

        return pieces

    def faces(key, oy, n, hz):
        groups = zs[key][0].shape[0]

        def pieces(d):
            s0, d0, w = {-1: (0, groups + 1, 1), 0: (0, 1, groups), 1: (groups - 1, 0, 1)}[d[0]]
            rs, rd, rw = {-1: (0, oy + n, hz), 0: (0, oy, n), 1: (n - hz, oy - hz, hz)}[d[1]]
            src, dst = (zs[key][0], zr[key][1]) if d[2] < 0 else (zs[key][1], zr[key][0])
            return [(src.at[pl.ds(s0, w), pl.ds(rs, rw), :], dst.at[pl.ds(d0, w), pl.ds(rd, rw), :], w * rw)]

        return pieces

    def exchange(key, arrays, oy, n, hz, directions):
        packed = halo(key, directions, faces(key, oy, n, hz))
        return both(packed, halo(key, FLAT, sides(arrays, oy, n)))

    def settle(what, arrived, left):
        k, total = what
        other = tuple(jnp.where(at == 0, at + 1, at - 1) for at in me)
        for edge, rows in total.items():
            same = None
            for e, here in zip(edge, at_edge):
                t = here if e else jnp.logical_not(here)
                same = t if same is None else same & t

            @pl.when(same)
            def _(rows=rows):
                cut = tally.at[pl.ds(0, rows), :]
                copy = pltpu.make_async_remote_copy(cut, cut, send_sem.at[k], recv_sem.at[k], device_id=other, device_id_type=MESH)
                if arrived:
                    copy.wait_recv()
                if left:
                    copy.wait_send()

    def first_sides(d):
        side = 0 if d[0] < 0 else 1
        rs, rd, rw = {-1: (0, 72, 3), 0: (0, 8, 64), 1: (61, 5, 3)}[d[1]]
        return [(xs[side].at[:, pl.ds(rs, rw), :], xr[1 - side].at[:, pl.ds(rd, rw), :], 2 * rw)]

    def first_rows(d):
        side = 0 if d[1] < 0 else 1
        return [(ys[side].at[:, pl.ds(0, 3), :], yr[1 - side].at[:, pl.ds(0, 3), :], 96)]

    beside0 = halo("fz", BESIDE, faces("f", 8, 64, 3))
    first = halo("f", FAR, faces("f", 8, 64, 3))
    first = both(first, halo("f", FLAT, lambda d: first_sides(d) if d[0] else first_rows(d)))
    def outside(ref, po, own, hp, oy, n, hr):
        planes, rows = ref.shape[0], ref.shape[1]
        for cond, cut in (
            (gx == 0, (slice(po - hp, po), slice(0, rows))),
            (gx == SIDE - 1, (slice(po + own, po + own + hp), slice(0, rows))),
            (gy == 0, (slice(0, planes), slice(oy - hr, oy))),
            (gy == SIDE - 1, (slice(0, planes), slice(oy + n, oy + n + hr))),
        ):

            @pl.when(cond)
            def _(cut=cut):
                shape = (cut[1].stop - cut[1].start, 128)
                for p in range(cut[0].start, cut[0].stop):
                    ref[p, cut[1], :] = jnp.zeros(shape, F32)

    def outside_z(key):
        for side, cond in ((0, gz == 0), (1, gz == SIDE - 1)):

            @pl.when(cond)
            def _(side=side):
                ref = zr[key][side]
                ref[...] = jnp.zeros(ref.shape, F32)

    def edges_z(key, po, n, hz, oy, groups):
        for side in (0, 1):
            ref = zr[key][side]
            rows = ref.shape[1]
            for cond, cut in (
                (gx == 0, (0, 1, 0, rows)),
                (gx == SIDE - 1, (groups + 1, 1, 0, rows)),
                (gy == 0, (0, groups + 2, oy - hz, hz)),
                (gy == SIDE - 1, (0, groups + 2, oy + n, hz)),
            ):

                @pl.when(cond)
                def _(cut=cut, ref=ref):
                    ref[pl.ds(cut[0], cut[1]), pl.ds(cut[2], cut[3]), :] = jnp.zeros((cut[1], cut[3], 128), F32)

    outside(H, 3, 32, 2, 8, 64, 3)
    for i in range(2):
        for cond, refs0 in ((gx == (0, SIDE - 1)[i], (xr[i],)), (gy == (0, SIDE - 1)[i], (yr[i],))):

            @pl.when(cond)
            def _(refs0=refs0):
                for ref in refs0:
                    ref[...] = jnp.zeros(ref.shape, F32)

        @pl.when(gy == (0, SIDE - 1)[i])
        def _(i=i):
            for ref in xr:
                for k in range(2):
                    ref[k, pl.ds((5, 72)[i], 3), :] = jnp.zeros((3, 128), F32)

    for key, n, oy, groups, hz in (("f", 64, 8, 2, 3), ("v", 64, 8, 2, 3), (1, 32, 16, 2, 6), (2, 16, 16, 1, 7)):
        outside_z(key)
        edges_z(key, 3, n, hz, oy, groups)
    outside(PR[1], 2, 8, 2, 16, 32, 8)
    outside(PR[2], 1, 2, 1, 16, 16, 8)
    for dx, dy in itertools.product((-1, 0, 1), repeat=2):
        if (dx, dy) != (0, 0):

            @pl.when(jnp.logical_not(inside((dx, dy, 0), me)))
            def _(dx=dx, dy=dy):
                Z3[dx + 1, dy + 1] = jnp.zeros((4 * SIDE, 128), F32)

    for l in (4, 5, 6):
        R[l][...] = jnp.zeros(LEV[l].shape(), F32)
        B[l][...] = jnp.zeros(LEV[l].shape(), F32)
    for l in (4, 5):
        EX[l][...] = jnp.zeros(EX[l].shape, F32)

    def tables(l):
        lv = LEV[l]
        shape = (lv.nr, 128)
        row, lane = iota(shape, 0) + lv.r0, iota(shape, 1)
        y = row - lv.oy
        z = jnp.where(lane < 100, lane, lane - 128)
        if l < 4:
            y = y + gy * lv.n
        if l < 3:
            z = z + gz * lv.n
        last = lv.total - 1
        within = (y >= 0) & (y <= last) & (z >= 0) & (z <= last)
        one = lambda c: jnp.where(c, 1, 0)
        w = one(y == 0) + one(y == last) + one(z == 0) + one(z == last)
        high = one(((row + lane) & 1) == 1)
        for kind, colour in itertools.product(range(3), range(2)):
            a = high if colour == 0 else 1 - high
            d = w if kind == 0 else (w + 1 - a if kind == 1 else w + a)
            inv = jnp.where(d == 0, 1 / 6, jnp.where(d == 1, 1 / 7, jnp.where(d == 2, 1 / 8, 1 / 9)))
            C[l][kind, colour] = jnp.where(within, inv, 0.0)
            D[l][kind, colour] = 6.0 + d.astype(F32)
            if colour == 1 and l < 6:
                q = jnp.where(within, 0.25, 0.0)
                Q[l][kind] = q
                A[l][kind] = (1.0 - d.astype(F32)) * q
        for colour in range(2):
            C[l][3, colour] = jnp.zeros(shape, F32)
            D[l][3, colour] = jnp.full(shape, 6.0, F32)
        if l < 6:
            Q[l][3] = jnp.zeros(shape, F32)
            A[l][3] = jnp.zeros(shape, F32)

    for l in range(7):
        tables(l)

    def kind(l, p):
        lv = LEV[l]
        x = 2 * (p - lv.po) + (gx * lv.n if l < 4 else 0)
        if l >= 4:
            return jnp.where(x == 0, 1, jnp.where(x == lv.total - 2, 2, 0))
        return jnp.where(x == 0, 1, jnp.where(x == lv.total - 2, 2, jnp.where((x < 0) | (x >= lv.total), 3, 0)))

    def slot_of(i, n):
        groups = n // 16
        if i < 0:
            return 0, 16 + i
        if i >= n:
            return groups + 1, i - n
        return 1 + i // 16, i % 16

    def unpack_first(i, r0, nr, which):
        g, j = slot_of(i, 32)
        rows = pl.ds(r0, nr)
        low, high = zr["f"][0][g, rows, :], zr["f"][1][g, rows, :]
        for k, at, width, shift in which:
            ref = (B, FR, FB)[k][0]
            w = turn(pick(within(8 * j + at, width), high, low), shift - 8 * j)
            ref[3 + i, rows, :] = pick(lane < 64, ref[3 + i, rows, :], w)

    settle(beside0, True, False)
    for i in range(32):
        unpack_first(i, 8, 64, LANE_FACES)

    settle(first, True, True)
    settle(beside0, False, True)
    tokens(0, 2, True)

    for side, (near, next_) in enumerate(((2, 1), (35, 36))):
        rows = pl.ds(4, 72)
        a, b = xr[side][0, rows, :], xr[side][1, rows, :]
        B[0][near, rows, :] = a
        B[0][next_, rows, :] = b
        FR[0][near, rows, :] = turn(a, 64)
        FB[0][near, rows, :] = turn(b, 64)
    for i in (-2, -1, 32, 33):
        unpack_first(i, 4, 72, LANE_FACES[: 3 if -1 <= i < 33 else 1])
    for i in range(32):
        for side, (rb, rr, rk) in enumerate(((5, 6, 7), (72, 72, 72))):
            t = yr[side][i]
            f = turn(t, 64)
            B[0][3 + i, rb : rb + 3, :] = t[0:3]
            FR[0][3 + i, rr : rr + 2, :] = f[0:2]
            FB[0][3 + i, rk : rk + 1, :] = f[2:3]
            unpack_first(i, (0, 72)[side], 8, LANE_FACES)

    def red_sweep(l):
        lv = LEV[l]
        p0, count, r0, nr = RED[l]
        rows, table = pl.ds(r0, nr), pl.ds(r0 - lv.r0, nr)

        def body(p):
            R[l][p, rows, :] = (FR[l][p, rows, :] + around(B[l], p, r0, nr, m)) * C[l][kind(l, p), 0, table, :]

        sweep_loop(p0, count, 36, body)

    def black_sweep(l, region, keep):
        lv = LEV[l]
        p0, count, r0, nr = region[l]
        rows, table = pl.ds(r0, nr), pl.ds(r0 - lv.r0, nr)

        def body(p):
            t = kind(l, p)
            fs = FB[l][p, rows, :] + around(R[l], p, r0, nr, not_m)
            b = fs * C[l][t, 1, table, :]
            B[l][p, rows, :] = b
            if keep:
                T[p, rows, :] = fs - D[l][t, 1, table, :] * b

        sweep_loop(p0, count, 36, body)

    def red_residual(l, p):
        lv = LEV[l]
        s = around(B[l], p, lv.oy, lv.n, m)
        at = lv.oy - lv.r0
        return FR[l][p, pl.ds(lv.oy, lv.n), :] + s - D[l][kind(l, p), 0, pl.ds(at, lv.n), :] * R[l][p, pl.ds(lv.oy, lv.n), :]

    def residual(l):
        lv = LEV[l]

        def body(p):
            T[p, pl.ds(lv.oy, lv.n), :] = T[p, pl.ds(lv.oy, lv.n), :] + red_residual(l, p)

        sweep_loop(lv.po, lv.n // 2, 32, body)

    def coarse_side(l, p):
        lv = LEV[l]
        half = lv.n // 2
        u = T[p, pl.ds(lv.oy, half, stride=2), :] + T[p, pl.ds(lv.oy + 1, half, stride=2), :]
        z = 2 * lane_index(half)
        return 0.5 * (take(u, z & 127) + take(u, (z + 1) & 127))

    red_sweep(0)
    black_sweep(0, BLACK_DOWN, True)

    def restrict_to(l, dst, first_plane, first_row):
        lv = LEV[l]

        def body(p):
            dst[p - lv.po + first_plane, pl.ds(first_row, lv.n // 2), :] = coarse_side(l, p)

        sweep_loop(lv.po, lv.n // 2, 32, body)

    residual(0)
    restrict_to(0, G[1], 0, 0)

    def send_right_side(l):
        n, w = LEV[l].n, WIDTH[l]
        per = 128 // n
        for q in range(n // per):
            t = G[l][per * q]
            for j in range(1, per):
                t = pick(within(n * j, n), turn(G[l][per * q + j], n * j), t)
            PS[l][q] = t
        pack_faces(lambda i: G[l][i], zs[l], n, 0, n - 8, 8, 128 - 2 * n)
        wide = 8 // per
        beside = halo(f"{l}z", BESIDE, faces(l, 16, n, w))
        return beside, exchange(l, [(PS[l], 0, PR[l], wide, n // per, wide, w)], 16, n, w, FAR)

    def side_lanes(l, i, rows):
        g, j = slot_of(i, LEV[l].n)
        return turn(pick(within(8 * j, 8), zr[l][1][g, rows, :], zr[l][0][g, rows, :]), LEV[l].n - 8 * j)

    def own_side_lanes(l):
        n = LEV[l].n
        for i in range(n):
            G[l][i] = pick(lane < n, G[l][i], side_lanes(l, i, pl.ds(16, n)))

    def split_right_side(l):
        lv = LEV[l]
        n = lv.n
        per = 128 // n

        def natural(i):
            q, k = (i + 8) // per, (i + 8) % per

            def tile(r, nr):
                rows = pl.ds(r, nr)
                return pick(lane < n, turn(PR[l][q, rows, :], -n * k), side_lanes(l, i, rows))

            if 0 <= i < n:
                return jnp.concatenate([tile(8, 8), G[l][i], tile(16 + n, 8)], axis=0)
            return tile(lv.r0, lv.nr)

        p0, count, _, _ = BLACK_DOWN[l] if l == 1 else (lv.p0, lv.np, 0, 0)
        for p in range(p0, p0 + count):
            a, b = natural(2 * (p - lv.po)), natural(2 * (p - lv.po) + 1)
            store_colours(l, p, a, b)

    def store_colours(l, p, a, b):
        lv = LEV[l]
        rows = pl.ds(lv.r0, lv.nr)
        red = pick(m, b, a)
        FR[l][p, rows, :] = red
        FB[l][p, rows, :] = pick(m, a, b)
        R[l][p, rows, :] = red * C[l][kind(l, p), 0]

    beside1, second = send_right_side(1)
    def keep_black(p):
        H[p, 8:72, :] = B[0][p, 8:72, :]

    sweep_loop(3, 32, 8, keep_black)

    tokens(0, 2, False)
    tokens(1, 4, True)
    settle(beside1, True, False)
    own_side_lanes(1)
    settle(second, True, False)
    split_right_side(1)
    black_sweep(1, BLACK_DOWN, True)
    residual(1)
    restrict_to(1, G[2], 0, 0)
    beside2, third = send_right_side(2)
    pack_faces(lambda i: B[0][3 + i, 8:72, :], zs["v"], 32, 0, 61, 3, 0)
    kept = exchange("v", [(B[0], 3, H, 3, 32, 2, 3)], 8, 64, 3, ACROSS)
    settle(beside2, True, False)
    own_side_lanes(2)
    settle(third, True, False)
    split_right_side(2)
    black_sweep(2, BLACK_DOWN, True)
    residual(2)

    own3 = None
    for i in range(8):
        g = jnp.where(lane < 8, coarse_side(2, LEV[2].po + i), 0.0)
        g = pltpu.roll(g, 8 * lax.rem(gz + i, 8), axis=1)
        own3 = g if own3 is None else own3 + g
    pack3[0:8, :] = own3
    own3 = jnp.where(lane[0:4] < 64, pack3[0:4, :], turn(pack3[4:8, :], 64))
    pack3[8:12, :] = own3
    Z3[1, 1, pl.ds(4 * gz, 4), :] = own3
    tokens(1, 4, False)

    k3 = PHASES.index("3")
    for dx, dy in sorted(itertools.product((-1, 0, 1), repeat=2), key=lambda d: -abs(d[0]) - abs(d[1])):

        @pl.when(inside((dx, dy, 0), me))
        def _(dx=dx, dy=dy):
            for far in (4, 3, 5, 2, 6, 1, 7, 0):
                if (dx, dy, far) != (0, 0, 0):
                    pltpu.make_async_remote_copy(
                        pack3.at[pl.ds(8, 4), :],
                        Z3.at[1 - dx, 1 - dy, pl.ds(4 * gz, 4), :],
                        send_sem.at[k3],
                        recv_sem.at[k3],
                        device_id=(gx + dx, gy + dy, (gz + far) & (SIDE - 1)),
                        device_id_type=MESH,
                    ).start()

    blocks = {edge: 4 * ((2 if edge[0] else 3) * (2 if edge[1] else 3) * SIDE - 1) for edge in EDGES}
    settle((k3, blocks), True, False)

    for p in range(1, 13):
        ab = []
        for i in (2 * (p - 1), 2 * (p - 1) + 1):
            x = i % 8
            tiles = []
            for cy in range(3):
                t = None
                for k in range(SIDE):
                    block = Z3[i // 8, cy, 4 * k : 4 * k + 4, :]
                    s = 8 * ((x + k) % 8)
                    t = block if t is None else jnp.where((within(s, 8) | within(s + 64, 8))[0:4], block, t)
                other = turn(t, 64)
                low = lane[0:4] < 64
                t = jnp.concatenate([jnp.where(low, t, other), jnp.where(low, other, t)], axis=0)
                tiles.append(turn(t, -8 * x))
            ab.append(jnp.concatenate(tiles, axis=0))
        store_colours(3, p, ab[0], ab[1])
    black_sweep(3, BLACK_DOWN, True)

    residual(3)
    own4 = None
    for i in range(4):
        g = turn(pick(lane < 32, coarse_side(3, LEV[3].po + i), jnp.zeros((4, 128), F32)), 32 * i)
        own4 = g if own4 is None else own4 + g
    pack4[0:4, :] = own4
    G4[gx, pl.ds(4 * gy, 4), :] = own4

    k4 = PHASES.index("4")

    ring = lambda k: min(k, SIDE - k)
    for dx, dy in sorted(itertools.product(range(SIDE), repeat=2), key=lambda d: -ring(d[0]) - ring(d[1])):
        if (dx, dy) != (0, 0):
            pltpu.make_async_remote_copy(
                pack4.at[pl.ds(0, 4), :],
                G4.at[gx, pl.ds(4 * gy, 4), :],
                send_sem.at[k4],
                recv_sem.at[k4],
                device_id=((gx + dx) & (SIDE - 1), (gy + dy) & (SIDE - 1), gz),
                device_id_type=MESH,
            ).start()
    plane = (k4, dict.fromkeys(EDGES, 4 * (SIDE * SIDE - 1)))
    settle(kept, True, True)
    for i in range(-2, 34):
        g, j = slot_of(i, 32)
        w = turn(pick(within(8 * j, 3), zr["v"][1][g, 4:76, :], zr["v"][0][g, 4:76, :]), 64 - 8 * j)
        H[3 + i, 4:76, :] = pick(lane < 64, H[3 + i, 4:76, :], w)
    settle(plane, True, False)
    for x in range(SIDE):
        parts = [turn(G4[x], -32 * i) for i in range(4)]
        store_colours(4, 4 + 2 * x, parts[0], parts[1])
        store_colours(4, 5 + 2 * x, parts[2], parts[3])
    for l in (4, 5):
        black_sweep(l, BLACK_DOWN, True)
        residual(l)
        restrict_to(l, N[l + 1], 0, 0)
        lv = LEV[l + 1]
        for p in range(lv.p0, lv.p0 + lv.np):
            store_colours(l + 1, p, N[l + 1][2 * (p - 1)], N[l + 1][2 * (p - 1) + 1])
    black_sweep(6, BLACK_UP, False)
    for _ in range(COARSE_SWEEPS - 1):
        red_sweep(6)
        black_sweep(6, BLACK_UP, False)

    def expand(l):
        lf, lc = LEV[l], LEV[l + 1]
        c0, cn, r0, rn = GIVE[l]
        fine0 = lf.oy + 2 * (r0 - lc.oy)
        if l == 3:
            c0, r0 = 2 * gx + 1, 4 * gy + 4
            fine0 = 8
        zf = lane_index(rn)
        z = (jnp.where(zf < 100, zf, zf - 128) >> 1) + (8 * gz if l == 2 else 0)
        at, beside = z & 127, (z + 2 * (zf & 1) - 1) & 127

        def body(i):
            rows = pl.ds(r0, rn)
            r, b = R[l + 1][c0 + i, rows, :], B[l + 1][c0 + i, rows, :]
            if rn % 8:
                mm = ((iota((rn, 128), 0) + iota((rn, 128), 1)) & 1) == 1
                both = jnp.where(mm, b, r), jnp.where(mm, r, b)
            else:
                both = pick(m, b, r), pick(m, r, b)
            for a, e in enumerate(both):
                here, there = take(e, at), take(e, beside)
                for k in (0, 1):
                    EX[l][2 * i + a, pl.ds(fine0 + k, rn, stride=2), :] = here
                    EZ[l][2 * i + a, pl.ds(fine0 + k, rn, stride=2), :] = there

        sweep_loop(0, cn, 20, body)

    def correct(l):
        lv = LEV[l]
        second_row = (iota((8, 128), 0) & 1) == 1
        p0, count, r0, nr = CORRECTED[l]
        rows, table = pl.ds(r0, nr), pl.ds(r0 - lv.r0, nr)

        def body(p):
            e = p - EDGE[l]
            t = kind(l, p)
            sides = pick(m, EX[l][e - 1, rows, :], EX[l][e + 1, rows, :])
            sides = sides + pick(second_row, EX[l][e, pl.ds(r0 + 1, nr), :], EX[l][e, pl.ds(r0 - 1, nr), :])
            add = EX[l][e, rows, :] * A[l][t, table, :] + (EZ[l][e, rows, :] + sides) * Q[l][t, table, :]
            return add

        start = B[l] if l else H

        def plain(p):
            B[l][p, rows, :] = start[p, rows, :] + body(p)

        sweep_loop(p0, count, 36, plain)

    for l in (5, 4):
        expand(l)
        correct(l)
        red_sweep(l)
        black_sweep(l, BLACK_UP, False)
    expand(3)
    correct(3)
    red_sweep(3)
    black_sweep(3, BLACK_UP, False)
    expand(2)
    correct(2)
    red_sweep(2)
    black_sweep(2, BLACK_UP, False)
    expand(1)
    correct(1)
    red_sweep(1)
    black_sweep(1, BLACK_UP, False)
    expand(0)
    correct(0)
    red_sweep(0)
    for what in (beside1, second, beside2, third, (k3, blocks), plane):
        settle(what, False, True)


def results(R, FR, FB, C, D, u_hbm, r_hbm, B, T, u_out, r_out, sem):
    lv = LEV[0]
    m = odd()
    not_m = jnp.logical_not(m)

    def kind(p):
        x = lax.axis_index("gx") * lv.n + 2 * (p - lv.po)
        return jnp.where(x == 0, 1, jnp.where(x == lv.total - 2, 2, jnp.where((x < 0) | (x >= lv.total), 3, 0)))

    def black(p):
        t = kind(p)
        fs = FB[p, 4:76, :] + around(R, p, 4, 72, not_m)
        b = fs * C[t, 1]
        B[p, 4:76, :] = b
        T[p, 4:76, :] = fs - D[t, 1] * b

    copies = []

    def out(src, dst, k):
        cut = pl.ds(2 * (STARTS[k] - 3), 2 * PARTS[k])
        copy = pltpu.make_async_copy(src.at[cut], dst.at[cut], sem.at[len(copies)])
        copy.start()
        copies.append(copy)

    def solve(k):
        for p in range(STARTS[k] + (1 if k else -1), STARTS[k] + PARTS[k] + 1):
            black(p)
        for p in range(STARTS[k], STARTS[k] + PARTS[k]):
            x = 2 * (p - lv.po)
            r, b = R[p, 8:72, :], B[p, 8:72, :]
            u_out[x] = pick(m, b, r)[:, 0:64]
            u_out[x + 1] = pick(m, r, b)[:, 0:64]
        out(u_out, u_hbm, k)

    def remain(k):
        for p in range(STARTS[k], STARTS[k] + PARTS[k]):
            x = 2 * (p - lv.po)
            left = FR[p, 8:72, :] + around(B, p, lv.oy, lv.n, m) - D[kind(p), 0, 4:68, :] * R[p, 8:72, :]
            b = T[p, 8:72, :]
            r_out[x] = pick(m, b, left)[:, 0:64]
            r_out[x + 1] = pick(m, left, b)[:, 0:64]
        out(r_out, r_hbm, k)

    solve(0)
    for k in range(1, len(PARTS)):
        solve(k)
        remain(k - 1)
    remain(len(PARTS) - 1)
    for copy in copies:
        copy.wait()


PARTS = (4, 4, 4, 4, 4, 4, 4, 4)
STARTS = tuple(3 + sum(PARTS[:k]) for k in range(len(PARTS)))
LANE_FACES = ((0, 0, 3, 64), (1, 3, 2, 61), (2, 5, 1, 59))
FETCHED = (0, 8, 16, 24, 32)
EDGES = tuple(itertools.product((False, True), repeat=3))
AROUND = sorted((d for d in itertools.product((-1, 0, 1), repeat=3) if any(d)), key=lambda d: -sum(map(abs, d)))
FLAT = [d for d in AROUND if d[2] == 0]
ACROSS = [d for d in AROUND if d[2]]
FAR = [d for d in ACROSS if d not in BESIDE]
EDGE = {0: -1, 1: -1, 2: -1, 3: -1, 4: 2, 5: -1}


def inside(d, me, far=1):
    ok = None
    for step, at in zip(d, me):
        if step:
            here = (at >= far) if step < 0 else (at < SIDE - far)
            ok = here if ok is None else ok & here
    return True if ok is None else ok


def vmem(*shape):
    return pltpu.VMEM(shape, F32)


def per_device(right_side, guess):
    whole = vmem(64, 64, 64)
    scratch = [whole, whole]
    scratch += [vmem(*lv.shape()) for lv in LEV[1:]]
    scratch += [vmem(*lv.shape()) for lv in LEV]
    for _ in range(2):
        scratch += [vmem(*lv.shape()) for lv in LEV[1:]]
    for _ in range(2):
        scratch += [vmem(4, 2, lv.nr, 128) for lv in LEV[1:]]
    for _ in range(2):
        scratch += [vmem(4, lv.nr, 128) for lv in LEV[:6]]
    for _ in range(2):
        scratch += [vmem(2 * GIVE[l][1], LEV[l].rows, 128) for l in range(6)]
    scratch += [vmem(*LEV[0].shape())] * 2
    scratch += [vmem(2, 64, 128)] * 2 + [vmem(2, 80, 128)] * 2 + [vmem(32, 8, 128)] * 4
    scratch += [vmem(32, 32, 128), vmem(16, 16, 128)]
    scratch += [vmem(8, 32, 128), vmem(2, 16, 128), vmem(12, 64, 128), vmem(4, 48, 128)]
    scratch += [vmem(16, 16, 128), vmem(8, 8, 128)]
    packed = ((2, 64, 80), (2, 64, 80), (2, 32, 64), (1, 16, 48))
    for groups, n, _ in packed:
        scratch += [vmem(groups, n, 128)] * 2
    for groups, _, rows in packed:
        scratch += [vmem(groups + 2, rows, 128)] * 2
    scratch += [vmem(16, 128), vmem(3, 3, 32, 128), vmem(8, 128), vmem(8, 32, 128), vmem(2048, 128)]
    dma = pltpu.SemaphoreType.DMA((len(PHASES),))
    scratch += [dma, dma, pltpu.SemaphoreType.DMA((8,)), pltpu.SemaphoreType.REGULAR((2,))]
    level0, table = pltpu.VMEM(LEV[0].shape(), F32), pltpu.VMEM((4, 2, LEV[0].nr, 128), F32)
    parts = pl.pallas_call(
        kernel,
        out_shape=(level0,) * 3 + (table, table),
        in_specs=[pl.BlockSpec(memory_space=pl.ANY)] * 2,
        out_specs=(pl.BlockSpec(memory_space=pltpu.VMEM),) * 5,
        scratch_shapes=scratch,
        compiler_params=pltpu.CompilerParams(collective_id=0, has_side_effects=True, vmem_limit_bytes=48 * 2**20),
    )(right_side, guess)
    block = jax.ShapeDtypeStruct(right_side.shape, F32)
    return pl.pallas_call(
        results,
        out_shape=(block, block),
        in_specs=[pl.BlockSpec(memory_space=pltpu.VMEM)] * 5,
        out_specs=(pl.BlockSpec(memory_space=pl.ANY),) * 2,
        scratch_shapes=[vmem(*LEV[0].shape())] * 2 + [vmem(64, 64, 64)] * 2 + [pltpu.SemaphoreType.DMA((2 * len(PARTS),))],
        compiler_params=pltpu.CompilerParams(vmem_limit_bytes=12 * 2**20),
    )(*parts)


def solution(mesh):
    spec = P("gx", "gy", "gz")
    return jax.shard_map(per_device, mesh=mesh, in_specs=(spec, spec), out_specs=(spec, spec), check_vma=False)
```
